256 devices in a mesh: dp: 128 (over y, z, x), mp: 2 (over core).
Axes of the slice: x: 4, y: 4, z: 8, core: 2. Of those that a mesh axis runs over, the one named last changes fastest.
Arguments:
- hidden_state: bfloat16 [256, 19, 19, 256], P('dp'), may hold values from -6 to 6
- actions: int32 [256, 2], P('dp'), may hold values from 0 to 361
- value_target: int32 [256, 2], P('dp'), may hold values from 0 to 600
- reward_target: int32 [256, 2], P('dp'), may hold values from 0 to 600
- kernel_first: float32 [3, 3, 256, 256], P(None, None, 'dp', 'mp'), may hold values from -6 to 6
- kernel_second: float32 [3, 3, 256, 256], P(None, None, 'dp', 'mp'), may hold values from -6 to 6
- head_weight: float32 [2, 256, 601], P('mp', 'dp'), may hold values from -6 to 6
- action_embed: float32 [2, 256], P('mp', 'dp'), may hold values from -6 to 6
- first_mean: float32 [3, 3, 256, 256], P(None, None, 'dp', 'mp'), may hold values from -0.00061035156 to 0.00061035156
- first_square: float32 [3, 3, 256, 256], P(None, None, 'dp', 'mp'), may hold values from 1e-09 to 1e-06
- second_mean: float32 [3, 3, 256, 256], P(None, None, 'dp', 'mp'), may hold values from -0.00061035156 to 0.00061035156
- second_square: float32 [3, 3, 256, 256], P(None, None, 'dp', 'mp'), may hold values from 1e-09 to 1e-06
- head_mean: float32 [2, 256, 601], P('mp', 'dp'), may hold values from -0.0029296875 to 0.0029296875
- head_square: float32 [2, 256, 601], P('mp', 'dp'), may hold values from 1e-08 to 1e-06
- embed_mean: float32 [2, 256], P('mp', 'dp'), may hold values from -0.0017089844 to 0.0017089844
- embed_square: float32 [2, 256], P('mp', 'dp'), may hold values from 1e-09 to 1e-06
Outputs:
- kernel_first_new: float32 [3, 3, 256, 256], P(None, None, 'dp', 'mp')
- kernel_second_new: float32 [3, 3, 256, 256], P(None, None, 'dp', 'mp')
- head_weight_new: float32 [2, 256, 601], P('mp', 'dp')
- action_embed_new: float32 [2, 256], P('mp', 'dp')
- first_mean_new: float32 [3, 3, 256, 256], P(None, None, 'dp', 'mp')
- first_square_new: float32 [3, 3, 256, 256], P(None, None, 'dp', 'mp')
- second_mean_new: float32 [3, 3, 256, 256], P(None, None, 'dp', 'mp')
- second_square_new: float32 [3, 3, 256, 256], P(None, None, 'dp', 'mp')
- head_mean_new: float32 [2, 256, 601], P('mp', 'dp')
- head_square_new: float32 [2, 256, 601], P('mp', 'dp')
- embed_mean_new: float32 [2, 256], P('mp', 'dp')
- embed_square_new: float32 [2, 256], P('mp', 'dp')
- first_grad: float32 [3, 3, 256, 256], P(None, None, 'dp', 'mp')
- second_grad: float32 [3, 3, 256, 256], P(None, None, 'dp', 'mp')
- head_grad: float32 [2, 256, 601], P('mp', 'dp')
- embed_grad: float32 [2, 256], P('mp', 'dp')
The draws below stay inside these ranges and needn't reach their ends.
Inputs may be any that keep to these rules, and one draw needn't show every extreme that they name: `actions`: the value 361 stands for a pass.
All inputs are finite; a program needn't handle non-finite values.
Results may differ from the reference program's by a relative error of at most 0.02.
Values may be sent and summed in bfloat16 or wider, within the bound.
A program may use at most 64 MiB of HBM per device.

```python
import math
import jax
import jax.numpy as jnp
from jax import lax

CHANNELS = 256
BOARD = 19
CELLS = 361
BUCKETS = 601
UNROLL = 2
TOTAL_POS = 256


def touch_ends(entries, stream_key, least, top_value):
    extent = entries.shape
    spot = [jax.random.randint(jax.random.fold_in(stream_key, axis), (), 0, extent[axis]) for axis in range(len(extent))]
    entries = entries.at[tuple(spot)].set(least)
    longest = extent.index(max(extent))
    spot[longest] = (spot[longest] + 1) % extent[longest]
    return entries.at[tuple(spot)].set(top_value)


def shard_levels(rng, shape, split, smallest, high):
    loudness, own = 1.0, jax.random.fold_in(rng, 6)
    for axis_at, shards_of in split:
        draws = jnp.exp(jax.random.uniform(jax.random.fold_in(own, axis_at), (shards_of,), jnp.float32, smallest / len(split), high / len(split)))
        loudness = loudness * jnp.repeat(draws, shape[axis_at] // shards_of).reshape([-1 if axis == axis_at else 1 for axis in range(len(shape))])
    return loudness


def noise(key, extent, scale, most, cuts=(), held_as=jnp.bfloat16):
    loudness = shard_levels(key, extent, cuts, -0.22, 0.18) if cuts else 1.0
    drawn = jax.random.normal(key, extent, jnp.float32) * scale * loudness
    return jnp.minimum(jnp.maximum(drawn, -most), most).astype(held_as)


def setup_inputs(seed: int = 0) -> dict:
    keys = jax.random.split(jax.random.key(seed), 17)
    return {
        "hidden_state": noise(keys[0], (TOTAL_POS, BOARD, BOARD, CHANNELS), 1.0, 6.0, ((0, 128),)),
        "actions": touch_ends(jax.random.randint(keys[1], (TOTAL_POS, UNROLL), 0, CELLS + 1), jax.random.fold_in(keys[1], 1), 0, CELLS).astype(jnp.int32),
        "value_target": touch_ends(jax.random.randint(keys[2], (TOTAL_POS, UNROLL), 0, BUCKETS), jax.random.fold_in(keys[2], 1), 0, BUCKETS - 1).astype(jnp.int32),
        "reward_target": touch_ends(jax.random.randint(keys[3], (TOTAL_POS, UNROLL), 0, BUCKETS), jax.random.fold_in(keys[3], 1), 0, BUCKETS - 1).astype(jnp.int32),
        "kernel_first": noise(keys[4], (3, 3, CHANNELS, CHANNELS), 1.0, 6.0, ((2, 128), (3, 2)), jnp.float32),
        "kernel_second": noise(keys[5], (3, 3, CHANNELS, CHANNELS), 1.0, 6.0, ((2, 128), (3, 2)), jnp.float32),
        "head_weight": noise(keys[6], (2, CHANNELS, BUCKETS), 1.0, 6.0, ((0, 2), (1, 128)), jnp.float32),
        "action_embed": noise(keys[7], (2, CHANNELS), 1.0, 6.0, ((0, 2), (1, 128)), jnp.float32),
        "first_mean": noise(keys[8], (3, 3, CHANNELS, CHANNELS), (1e-4), 0.00061035156, ((2, 128), (3, 2)), jnp.float32),
        "first_square": jnp.clip(jnp.exp(math.log(9.999999974752427e-07) - 6.9077553 * jax.random.uniform(keys[9], (3, 3, CHANNELS, CHANNELS), jnp.float32) ** shard_levels(keys[9], (3, 3, CHANNELS, CHANNELS), ((2, 128), (3, 2)), -0.2, 0.2)), 9.999999717180685e-10, 9.999999974752427e-07),
        "second_mean": noise(keys[10], (3, 3, CHANNELS, CHANNELS), (1e-4), 0.00061035156, ((2, 128), (3, 2)), jnp.float32),
        "second_square": jnp.clip(jnp.exp(math.log(9.999999974752427e-07) - 6.9077553 * jax.random.uniform(keys[11], (3, 3, CHANNELS, CHANNELS), jnp.float32) ** shard_levels(keys[11], (3, 3, CHANNELS, CHANNELS), ((2, 128), (3, 2)), -0.2, 0.2)), 9.999999717180685e-10, 9.999999974752427e-07),
        "head_mean": noise(keys[12], (2, CHANNELS, BUCKETS), (5e-4), 0.0029296875, ((0, 2), (1, 128)), jnp.float32),
        "head_square": jnp.clip(jnp.exp(math.log(9.999999974752427e-07) - 4.6051702 * jax.random.uniform(keys[13], (2, CHANNELS, BUCKETS), jnp.float32) ** shard_levels(keys[13], (2, CHANNELS, BUCKETS), ((0, 2), (1, 128)), -0.2, 0.2)), 9.99999993922529e-09, 9.999999974752427e-07),
        "embed_mean": noise(keys[14], (2, CHANNELS), (3e-4), 0.0017089844, ((0, 2), (1, 128)), jnp.float32),
        "embed_square": jnp.clip(jnp.exp(math.log(9.999999974752427e-07) - 6.9077553 * jax.random.uniform(keys[15], (2, CHANNELS), jnp.float32) ** shard_levels(keys[15], (2, CHANNELS), ((0, 2), (1, 128)), -0.2, 0.2)), 9.999999717180685e-10, 9.999999974752427e-07),
    }


head_scale = 4.0
soft_cap = 15.0
eps_norm = 1e-05
beta_one = 0.9
beta_two = 0.999
step_size = 0.1
eps_adam = 1e-08

def conv_apply(field, kernel, layout):
    return lax.conv_general_dilated(field, kernel, (1, 1), 'SAME', dimension_numbers=('NHWC', layout, 'NHWC'), preferred_element_type=jnp.float32)

def gate_slope(pre):
    sig = jax.nn.sigmoid(pre)
    return sig * (1.0 + pre * (1.0 - sig))

def tap_products(field, grad, field_rows):
    side = field.shape[1]
    padded = jnp.pad(field, ((0, 0), (1, 1), (1, 1), (0, 0)))
    flat_grad = grad.reshape(-1, grad.shape[3])
    blocks = []
    for offset in range(9):
        row_start = offset // 3
        col_start = offset % 3
        window = padded[:, row_start:row_start + side, col_start:col_start + side, :].reshape(-1, field.shape[3])
        if field_rows:
            blocks.append(lax.dot_general(window, flat_grad, (((0,), (0,)), ((), ())), preferred_element_type=jnp.float32))
        else:
            blocks.append(lax.dot_general(flat_grad, window, (((0,), (0,)), ((), ())), preferred_element_type=jnp.float32))
    stacked = jnp.stack(blocks)
    return stacked.reshape(3, 3, stacked.shape[1], stacked.shape[2])

def action_planes(move, board):
    cells = board * board
    plane = (lax.broadcasted_iota(jnp.int32, (move.shape[0], cells), 1) == move[:, None]).astype(jnp.float32)
    passed = (move == cells).astype(jnp.float32)
    return (plane.reshape(move.shape[0], board, board, 1), passed[:, None, None, None])

def head_backward(state, head_used, value_now, reward_now, total):
    pooled = lax.optimization_barrier(jnp.mean(state, axis=(1, 2))).astype(jnp.bfloat16)
    raw = head_scale * jnp.stack([jnp.dot(pooled, head_used[0], preferred_element_type=jnp.float32), jnp.dot(pooled, head_used[1], preferred_element_type=jnp.float32)])
    squashed = jnp.tanh(raw / soft_cap)
    raised = jnp.exp(soft_cap * squashed)
    chances = raised / lax.optimization_barrier(jnp.sum(raised, axis=2, keepdims=True))
    targets = jnp.stack([value_now, reward_now])
    picked = (lax.broadcasted_iota(jnp.int32, raw.shape, 2) == targets[:, :, None]).astype(jnp.float32)
    logit_grad = ((chances - picked) * (1.0 - squashed * squashed) / total).astype(jnp.bfloat16)
    pooled_grad = head_scale * (jnp.dot(logit_grad[0], head_used[0].T, preferred_element_type=jnp.float32) + jnp.dot(logit_grad[1], head_used[1].T, preferred_element_type=jnp.float32))
    return (pooled, logit_grad, pooled_grad)

def adam_update(param, grad, mean, square):
    mean_new = beta_one * mean + (1.0 - beta_one) * grad
    square_new = beta_two * square + (1.0 - beta_two) * grad * grad
    param_new = param - step_size * mean_new / (jnp.sqrt(square_new) + eps_adam)
    return (param_new, mean_new, square_new)

def reference(hidden_state, actions, value_target, reward_target, kernel_first, kernel_second, head_weight, action_embed, first_mean, first_square, second_mean, second_square, head_mean, head_square, embed_mean, embed_square):
    first_used = kernel_first.astype(jnp.bfloat16)
    second_used = kernel_second.astype(jnp.bfloat16)
    head_used = head_weight.astype(jnp.bfloat16)
    embed_used = action_embed.astype(jnp.bfloat16)
    board = hidden_state.shape[1]
    cells = board * board
    scale = (9.0 * CHANNELS) ** (-0.5)
    embed = embed_used.astype(jnp.float32)
    state = hidden_state.astype(jnp.float32)
    saved = []
    for position in range(UNROLL):
        plane, passed = action_planes(actions[:, position], board)
        mixed = state + plane * embed[0] + passed * embed[1]
        conv_input = mixed.astype(jnp.bfloat16)
        pre = scale * conv_apply(conv_input, first_used, 'HWIO')
        hidden = jax.nn.silu(pre).astype(jnp.bfloat16)
        summed = mixed + scale * conv_apply(hidden, second_used, 'HWOI')
        factor = lax.rsqrt(lax.optimization_barrier(jnp.mean(summed * summed, axis=(1, 2, 3), keepdims=True)) + eps_norm)
        state = summed * factor
        pooled, logit_grad, pooled_grad = head_backward(state, head_used, value_target[:, position], reward_target[:, position], TOTAL_POS)
        saved.append((plane, passed, conv_input, pre, hidden, summed, factor, pooled, logit_grad, pooled_grad))
    first_grad = jnp.zeros(kernel_first.shape, jnp.float32)
    second_grad = jnp.zeros(kernel_second.shape, jnp.float32)
    head_grad = jnp.zeros(head_weight.shape, jnp.float32)
    embed_grad = jnp.zeros(action_embed.shape, jnp.float32)
    carry = jnp.zeros(hidden_state.shape, jnp.float32)
    for position in range(UNROLL - 1, -1, -1):
        plane, passed, conv_input, pre, hidden, summed, factor, pooled, logit_grad, pooled_grad = saved[position]
        state_grad = carry + pooled_grad[:, None, None, :] / cells
        summed_grad = factor * state_grad - factor * factor * factor * summed * lax.optimization_barrier(jnp.mean(state_grad * summed, axis=(1, 2, 3), keepdims=True))
        branch_grad = summed_grad.astype(jnp.bfloat16)
        hidden_grad = scale * conv_apply(branch_grad, second_used[::-1, ::-1], 'HWIO')
        inner_grad = (hidden_grad * gate_slope(pre)).astype(jnp.bfloat16)
        carry = summed_grad + scale * conv_apply(inner_grad, first_used[::-1, ::-1], 'HWOI')
        first_grad = first_grad + scale * tap_products(conv_input, inner_grad, True)
        second_grad = second_grad + scale * tap_products(hidden, branch_grad, False)
        head_grad = head_grad + head_scale * jnp.stack([lax.dot_general(pooled, logit_grad[0], (((0,), (0,)), ((), ())), preferred_element_type=jnp.float32), lax.dot_general(pooled, logit_grad[1], (((0,), (0,)), ((), ())), preferred_element_type=jnp.float32)])
        embed_grad = embed_grad + jnp.stack([lax.optimization_barrier(jnp.sum(plane * carry, axis=(0, 1, 2))), lax.optimization_barrier(jnp.sum(passed * carry, axis=(0, 1, 2)))])
    first_new, first_mean_new, first_square_new = adam_update(kernel_first, first_grad, first_mean, first_square)
    second_new, second_mean_new, second_square_new = adam_update(kernel_second, second_grad, second_mean, second_square)
    head_new, head_mean_new, head_square_new = adam_update(head_weight, head_grad, head_mean, head_square)
    embed_new, embed_mean_new, embed_square_new = adam_update(action_embed, embed_grad, embed_mean, embed_square)
    return (first_new, second_new, head_new, embed_new, first_mean_new, first_square_new, second_mean_new, second_square_new, head_mean_new, head_square_new, embed_mean_new, embed_square_new, first_grad, second_grad, head_grad, embed_grad)
```

```python
import functools

import jax
import jax.numpy as jnp
from jax import lax
from jax.experimental import pallas as pl
from jax.experimental.pallas import tpu as pltpu
from jax.sharding import Mesh
from jax.sharding import PartitionSpec as P

MESH = pl.DeviceIdType.MESH
CHANNELS = 256
DP = ("dp_0", "dp_1", "dp_2")
SIDE = 19
CELLS = 361
BUCKETS = 601
PITCH = 32
ROWS = SIDE * PITCH
TALL = 640
DEPTH = 704
ITEMS = 24
SCALE = (9.0 * CHANNELS) ** (-0.5)

head_scale = 4.0
soft_cap = 15.0
eps_norm = 1e-05
beta_one = 0.9
beta_two = 0.999
step_size = 0.1
eps_adam = 1e-08

F32 = jnp.float32
BF16 = jnp.bfloat16


def seats():
    return (
        lax.axis_index("dp_0"),
        lax.axis_index("dp_1"),
        lax.axis_index("dp_2"),
        lax.axis_index("mp"),
    )


def greet_all(y, z, x, c):
    barrier = pltpu.get_barrier_semaphore()
    for step in range(1, 8):
        pl.semaphore_signal(
            barrier, inc=1, device_id={"dp_1": lax.rem(z + step, 8)}, device_id_type=MESH
        )
    for step in range(1, 4):
        for name, here in (("dp_0", y), ("dp_2", x)):
            pl.semaphore_signal(
                barrier, inc=1, device_id={name: lax.rem(here + step, 4)}, device_id_type=MESH
            )
    pl.semaphore_signal(barrier, inc=1, device_id={"mp": 1 - c}, device_id_type=MESH)
    return barrier


def remote(src, dst, send, recv, peer):
    return pltpu.make_async_remote_copy(
        src_ref=src, dst_ref=dst, send_sem=send, recv_sem=recv, device_id=peer, device_id_type=MESH
    )


HALVES = (("dp_2", "dp_0"), ("dp_0", "dp_2"))
ORDER = (1, 3, 2)


def gather_kernel(
    first, second, head, embed, out, rows, stage, wide, z_send, z_recv, p_send, p_recv, q_send, q_recv,
    m_send, m_recv,
):
    y, z, x, c = seats()
    here = {"dp_0": y, "dp_2": x}
    barrier = greet_all(y, z, x, c)

    for tap in range(9):
        rows[2 * tap : 2 * tap + 2, :] = first[tap // 3, tap % 3]
        rows[18 + 2 * tap : 20 + 2 * tap, :] = second[tap // 3, tap % 3]
    rows[36:48, :] = jnp.zeros((12, 128), F32)
    for block in range(5):
        width = min(128, BUCKETS - 128 * block)
        rows[36 + 2 * block : 38 + 2 * block, 0:width] = head[0, :, 128 * block : 128 * block + width]
    for r in range(2):
        rows[46 + r : 47 + r, :] = jnp.broadcast_to(embed[:, r : r + 1], (1, 128))
    stage[z] = rows[...].astype(BF16)
    pl.semaphore_wait(barrier, 14)

    started = []
    for step in range(1, 8):
        copy = remote(
            stage.at[z], stage.at[z], z_send.at[step], z_recv.at[z], {"dp_1": lax.rem(z + step, 8)}
        )
        copy.start()
        started.append(copy)
    for step in range(1, 8):
        peer = lax.rem(z + step, 8)
        remote(stage.at[peer], stage.at[peer], z_send.at[0], z_recv.at[peer], {"dp_1": peer}).wait_recv()
    for piece in range(8):
        wide[56 * piece : 56 * piece + 48, :] = stage[piece].astype(F32)
    for item in range(ITEMS):
        low = wide[pl.ds(2 * item, 8, stride=56), :]
        high = wide[pl.ds(2 * item + 1, 8, stride=56), :]
        out[c, item, y, x] = jnp.concatenate([low, high], axis=0).astype(BF16)

    def part(half, near, far):
        items = pl.ds(12 * half, 12)
        if half == 0:
            return out.at[c, items, far, near]
        return out.at[c, items, near, far]

    def slab(half, far):
        items = pl.ds(12 * half, 12)
        if half == 0:
            return out.at[c, items, far]
        return out.at[c, items, :, far]

    for step in ORDER:
        for half, (near, far) in enumerate(HALVES):
            ref = part(half, here[near], here[far])
            copy = remote(
                ref, ref, p_send.at[half, step], p_recv.at[half, here[near]],
                {near: lax.rem(here[near] + step, 4)},
            )
            copy.start()
            started.append(copy)
    partner = {"mp": 1 - c}
    for half, (near, far) in enumerate(HALVES):
        for step in ORDER:
            peer = lax.rem(here[near] + step, 4)
            ref = part(half, peer, here[far])
            remote(ref, ref, p_send.at[half, 0], p_recv.at[half, peer], {near: peer}).wait_recv()
        ref = slab(half, here[far])
        for step in ORDER:
            copy = remote(
                ref, ref, q_send.at[half, step], q_recv.at[half, here[far]],
                {far: lax.rem(here[far] + step, 4)},
            )
            copy.start()
            started.append(copy)
        copy = remote(ref, ref, m_send.at[half, 0], m_recv.at[half, here[far], c], partner)
        copy.start()
        started.append(copy)
    for step in ORDER:
        for half, (near, far) in enumerate(HALVES):
            peer = lax.rem(here[far] + step, 4)
            ref = slab(half, peer)
            remote(ref, ref, q_send.at[half, 0], q_recv.at[half, peer], {far: peer}).wait_recv()
            copy = remote(ref, ref, m_send.at[half, step], m_recv.at[half, peer, c], partner)
            copy.start()
            started.append(copy)
    for half in range(2):
        for spot in range(4):
            items = pl.ds(12 * half, 12)
            ref = out.at[1 - c, items, spot] if half == 0 else out.at[1 - c, items, :, spot]
            remote(ref, ref, m_send.at[half, 0], m_recv.at[half, spot, 1 - c], partner).wait_recv()
    for copy in started:
        copy.wait_send()


def gather(first, second, head, embed):
    vmem = pl.BlockSpec(memory_space=pltpu.VMEM)
    dma = pltpu.SemaphoreType.DMA
    return pl.pallas_call(
        gather_kernel,
        out_shape=jax.ShapeDtypeStruct((2, ITEMS, 4, 4, 16, 128), BF16),
        in_specs=[vmem] * 4,
        out_specs=vmem,
        scratch_shapes=[
            pltpu.VMEM((48, 128), F32),
            pltpu.VMEM((8, 48, 128), BF16),
            pltpu.VMEM((448, 128), F32),
            dma((8,)),
            dma((8,)),
            dma((2, 4)),
            dma((2, 4)),
            dma((2, 4)),
            dma((2, 4)),
            dma((2, 4)),
            dma((2, 4, 2)),
        ],
        compiler_params=pltpu.CompilerParams(
            collective_id=0, has_side_effects=True, vmem_limit_bytes=16 << 20
        ),
        name="gather",
    )(first, second, head, embed)


def scatter_kernel(
    g, out, inbox, sums, a_in, b_in, a_sum, b_sum, a_last, b_last, flat, letters, m_send, m_recv, p_send, p_recv,
    q_send, q_recv, z_send, z_recv,
):
    y, z, x, c = seats()
    here = {"dp_0": y, "dp_2": x}
    barrier = greet_all(y, z, x, c)
    pl.semaphore_wait(barrier, 14)
    started = []

    def launch(copy):
        copy.start()
        started.append(copy)

    partner = {"mp": 1 - c}
    for half in range(2):
        items = pl.ds(12 * half, 12)
        launch(remote(g.at[1 - c, items], inbox.at[items], m_send.at[half], m_recv.at[half], partner))
    arrivals, folded, last = (a_in, b_in), (a_sum, b_sum), (a_last, b_last)
    for half, (near, far) in enumerate(HALVES):
        items = pl.ds(12 * half, 12)
        remote(g.at[1 - c, items], inbox.at[items], m_send.at[half], m_recv.at[half], partner).wait_recv()

        def join(item, carry):
            total = g[c, item].astype(F32) + inbox[item].astype(F32)
            sums[item] = total.astype(BF16)
            return carry

        lax.fori_loop(12 * half, 12 * half + 12, join, 0)
        for step in ORDER:
            peer = lax.rem(here[near] + step, 4)
            ref = sums.at[items, :, peer] if half == 0 else sums.at[items, peer]
            launch(
                remote(
                    ref, arrivals[half].at[here[near]], p_send.at[half, step], p_recv.at[half, here[near]],
                    {near: peer},
                )
            )
    for half, (near, far) in enumerate(HALVES):
        peers = [lax.rem(here[near] + step, 4) for step in (1, 2, 3)]
        for peer in peers:
            ref = arrivals[half].at[peer]
            remote(ref, ref, p_send.at[half, 0], p_recv.at[half, peer], {near: peer}).wait_recv()

        def fold(item, carry):
            own = sums[item, :, x] if half == 0 else sums[12 + item, y]
            total = own.astype(F32)
            for peer in peers:
                total = total + arrivals[half][peer, item].astype(F32)
            folded[half][item] = total.astype(BF16)
            return carry

        lax.fori_loop(0, 12, fold, 0)
        for step in ORDER:
            peer = lax.rem(here[far] + step, 4)
            launch(
                remote(
                    folded[half].at[:, peer], last[half].at[here[far]], q_send.at[half, step],
                    q_recv.at[half, here[far]], {far: peer},
                )
            )
    for half, (near, far) in enumerate(HALVES):
        peers = [lax.rem(here[far] + step, 4) for step in (1, 2, 3)]
        for peer in peers:
            ref = last[half].at[peer]
            remote(ref, ref, q_send.at[half, 0], q_recv.at[half, peer], {far: peer}).wait_recv()

        def settle(item, carry):
            total = folded[half][item, here[far]].astype(F32)
            for peer in peers:
                total = total + last[half][peer, item].astype(F32)
            flat[pl.ds(pl.multiple_of((12 * half + item) * 16, 16), 16), :] = total
            return carry

        lax.fori_loop(0, 12, settle, 0)
    for spot in range(8):
        letters[spot] = flat[pl.ds(spot, 48, stride=8), :].astype(BF16)
    for step in range(1, 8):
        peer = lax.rem(z + step, 8)
        launch(remote(letters.at[peer], out.at[z], z_send.at[step], z_recv.at[z], {"dp_1": peer}))
    out[z] = letters[z]
    for step in range(1, 8):
        peer = lax.rem(z + step, 8)
        remote(letters.at[peer], out.at[peer], z_send.at[0], z_recv.at[peer], {"dp_1": peer}).wait_recv()
    for copy in started:
        copy.wait_send()


def scatter(grads):
    vmem = pl.BlockSpec(memory_space=pltpu.VMEM)
    dma = pltpu.SemaphoreType.DMA
    return pl.pallas_call(
        scatter_kernel,
        out_shape=jax.ShapeDtypeStruct((8, 48, 128), BF16),
        in_specs=[vmem],
        out_specs=vmem,
        scratch_shapes=[
            pltpu.VMEM((ITEMS, 4, 4, 16, 128), BF16),
            pltpu.VMEM((ITEMS, 4, 4, 16, 128), BF16),
            pltpu.VMEM((4, 12, 4, 16, 128), BF16),
            pltpu.VMEM((4, 12, 4, 16, 128), BF16),
            pltpu.VMEM((12, 4, 16, 128), BF16),
            pltpu.VMEM((12, 4, 16, 128), BF16),
            pltpu.VMEM((4, 12, 16, 128), BF16),
            pltpu.VMEM((4, 12, 16, 128), BF16),
            pltpu.VMEM((384, 128), F32),
            pltpu.VMEM((8, 48, 128), BF16),
            dma((2,)),
            dma((2,)),
            dma((2, 4)),
            dma((2, 4)),
            dma((2, 4)),
            dma((2, 4)),
            dma((8,)),
            dma((8,)),
        ],
        compiler_params=pltpu.CompilerParams(
            collective_id=1, has_side_effects=True, vmem_limit_bytes=24 << 20
        ),
        name="scatter",
    )(grads)


NN = (((1,), (0,)), ((), ()))
NT = (((1,), (1,)), ((), ()))
TN = (((0,), (0,)), ((), ()))


def dot(a, b, dims=NN):
    return lax.dot_general(a, b, dims, preferred_element_type=F32)


def compute_kernel(
    moves, values, rewards, hidden_in, w, out, xs, hs, bs, zs, xt, bt, state, mixed, pre, summed, saved
):
    c = lax.axis_index("mp")
    row = lax.broadcasted_iota(jnp.int32, (ROWS, CHANNELS), 0)
    valid = lax.rem(row, PITCH) < SIDE

    def first(tap):
        return jnp.concatenate([w[0, tap], w[1, tap]], axis=1)

    def second(tap):
        return jnp.concatenate([w[0, 9 + tap], w[1, 9 + tap]], axis=1)

    def head(h):
        return jnp.concatenate([w[h, 18 + k] for k in range(5)], axis=1)

    def conv(field, kernel, flip):
        taps = [8 - t if flip else t for t in range(9)]
        lhs = jnp.concatenate(
            [field[t % 3, PITCH * (t // 3) : PITCH * (t // 3) + ROWS] for t in range(9)], axis=1
        )
        return lhs, [kernel(t) for t in taps]

    def conv_plain(field, kernel, flip):
        lhs, parts = conv(field, kernel, flip)
        return dot(lhs, jnp.concatenate(parts, axis=0))

    def conv_swapped(field, kernel, flip):
        lhs, parts = conv(field, kernel, flip)
        return dot(lhs, jnp.concatenate(parts, axis=1), NT)

    def spread(value, dest):
        dest[1, PITCH : PITCH + ROWS] = value.astype(BF16)
        dest[0, PITCH : PITCH + ROWS] = pltpu.roll(value, 1, 0).astype(BF16)
        dest[2, PITCH : PITCH + ROWS] = pltpu.roll(value, ROWS - 1, 0).astype(BF16)

    def turned(value):
        tall = jnp.concatenate([value, jnp.zeros((TALL - ROWS, CHANNELS), F32)], axis=0)
        return tall.T.astype(BF16)

    def total(value):
        return jnp.sum(jnp.sum(value, axis=0, keepdims=True), axis=1, keepdims=True)

    for field in (xs, hs, bs, zs):
        for k in range(2):
            for b in range(3):
                field[k, b, 0:PITCH] = jnp.zeros((PITCH, CHANNELS), BF16)
                field[k, b, PITCH + ROWS : DEPTH] = jnp.zeros((DEPTH - PITCH - ROWS, CHANNELS), BF16)

    lane = lax.broadcasted_iota(jnp.int32, (CHANNELS, CHANNELS), 1)
    natural = 64 * (lane // 64) + 8 * (lane % 8) + 2 * ((lane // 16) % 4) + (lane // 8) % 2
    source = lax.broadcasted_iota(jnp.int32, (CHANNELS, CHANNELS), 0)
    permute = (source == natural).astype(BF16)
    state[...] = jnp.zeros((ROWS, CHANNELS), F32)
    for line in range(SIDE):
        state[PITCH * line : PITCH * line + SIDE, :] = hidden_in[c, line].astype(F32)
    state[...] = dot(state[...].astype(BF16), permute)

    ones = jnp.ones((16, 128), BF16)
    pick = lax.broadcasted_iota(jnp.int32, (16, 128), 1) == 0
    pick = jnp.where(pick, ones, jnp.zeros_like(ones))
    embed = [dot(pick, w[e, 23], NT)[0:1, :] for e in range(2)]

    bucket = lax.broadcasted_iota(jnp.int32, (16, 640), 1)
    kept = []
    pooled_rows = jnp.zeros((16, CHANNELS), F32)
    grad_rows = [jnp.zeros((16, 640), F32) for _ in range(2)]
    for k in range(2):
        move = moves[c, k]
        spot = PITCH * lax.div(move, SIDE) + lax.rem(move, SIDE)
        passed = move == CELLS
        added = jnp.where(row == spot, embed[0], 0.0) + jnp.where(passed, 1.0, 0.0) * embed[1]
        now = jnp.where(valid, state[...] + added, 0.0)
        mixed[...] = now
        spread(now, xs.at[k])
        xt[:, TALL * k : TALL * k + TALL] = turned(now)
        value = SCALE * conv_plain(xs.at[k], first, False)
        pre[k] = value
        spread(jnp.where(valid, value * jax.nn.sigmoid(value), 0.0), hs.at[k])
        branch = conv_swapped(hs.at[k], second, False)
        value = jnp.where(valid, mixed[...] + SCALE * branch, 0.0)
        summed[k] = value
        factor = lax.rsqrt(total(value * value) / (CELLS * CHANNELS) + eps_norm)
        value = value * factor
        state[...] = value
        pooled = (jnp.sum(value, axis=0, keepdims=True) / CELLS).astype(BF16)
        pooled = jnp.broadcast_to(pooled.astype(F32), (16, CHANNELS))
        own_row = lax.broadcasted_iota(jnp.int32, (16, CHANNELS), 0) == k
        pooled_rows = jnp.where(own_row, pooled, pooled_rows)
        pooled = pooled.astype(BF16)
        pooled_grad = jnp.zeros((16, CHANNELS), F32)
        for h, targets in enumerate((values, rewards)):
            raw = head_scale * dot(pooled, head(h))
            squashed = jnp.tanh(raw / soft_cap)
            raised = jnp.where(bucket < BUCKETS, jnp.exp(soft_cap * squashed), 0.0)
            chances = raised / jnp.sum(raised, axis=1, keepdims=True)
            picked = jnp.where(bucket == targets[c, k], 1.0, 0.0)
            logit = (chances - picked) * (1.0 - squashed * squashed) / 256.0
            logit = jnp.where(bucket < BUCKETS, logit, 0.0).astype(BF16)
            pooled_grad = pooled_grad + dot(logit, head(h), NT)
            logit = logit.astype(F32)
            own_row = lax.broadcasted_iota(jnp.int32, (16, 640), 0) == k
            grad_rows[h] = jnp.where(own_row, logit, grad_rows[h])
        kept.append((spot, passed, factor, head_scale * pooled_grad[0:1, :] / CELLS))

    for h in range(2):
        grad = head_scale * dot(pooled_rows.astype(BF16), grad_rows[h].astype(BF16), TN)
        for block in range(5):
            out[h, 18 + block] = grad[:, 128 * block : 128 * block + 128].astype(BF16)

    embed_grad = [jnp.zeros((1, CHANNELS), F32) for _ in range(2)]
    for k in (1, 0):
        spot, passed, factor, pooled_grad = kept[k]
        grad = pooled_grad if k == 1 else saved[...] + pooled_grad
        grad = jnp.where(valid, grad, 0.0)
        value = summed[k]
        slope = total(grad * value) / (CELLS * CHANNELS)
        summed_grad = factor * grad - factor * factor * factor * value * slope
        saved[...] = summed_grad
        spread(summed_grad, bs.at[k])
        bt[:, TALL * k : TALL * k + TALL] = turned(summed_grad)
        hidden_grad = SCALE * conv_plain(bs.at[k], second, True)
        value = pre[k]
        sig = jax.nn.sigmoid(value)
        inner = hidden_grad * (sig * (1.0 + value * (1.0 - sig)))
        spread(jnp.where(valid, inner, 0.0), zs.at[k])
        carry = saved[...] + SCALE * conv_swapped(zs.at[k], first, True)
        carry = jnp.where(valid, carry, 0.0)
        saved[...] = carry
        embed_grad[0] = embed_grad[0] + jnp.sum(jnp.where(row == spot, carry, 0.0), axis=0, keepdims=True)
        embed_grad[1] = embed_grad[1] + jnp.where(passed, 1.0, 0.0) * jnp.sum(carry, axis=0, keepdims=True)

    for e in range(2):
        rows = jnp.broadcast_to(embed_grad[e], (16, CHANNELS)).astype(BF16)
        top = lax.broadcasted_iota(jnp.int32, (16, 128), 0) == 0
        out[e, 23] = dot(rows, jnp.where(top, ones, jnp.zeros_like(ones)), TN).astype(BF16)

    def window(field, tap):
        start = PITCH * (tap // 3)
        return jnp.concatenate([field[k, tap % 3, start : start + TALL] for k in range(2)], axis=0)

    for tap in range(9):
        grad = SCALE * dot(bt[...], window(hs, tap))
        out[0, 9 + tap] = grad[:, 0:128].astype(BF16)
        out[1, 9 + tap] = grad[:, 128:256].astype(BF16)
    for tap in range(9):
        grad = SCALE * dot(xt[...], window(zs, 8 - tap))
        out[0, tap] = grad[:, 0:128].astype(BF16)
        out[1, tap] = grad[:, 128:256].astype(BF16)


def compute(moves, values, rewards, hidden_state, weights):
    vmem = pl.BlockSpec(memory_space=pltpu.VMEM)
    smem = pl.BlockSpec(memory_space=pltpu.SMEM)
    copies = pltpu.VMEM((2, 3, DEPTH, CHANNELS), BF16)
    field = pltpu.VMEM((ROWS, CHANNELS), F32)
    fields = pltpu.VMEM((2, ROWS, CHANNELS), F32)
    return pl.pallas_call(
        compute_kernel,
        out_shape=jax.ShapeDtypeStruct((2, ITEMS, CHANNELS, 128), BF16),
        in_specs=[smem, smem, smem, vmem, vmem],
        out_specs=vmem,
        scratch_shapes=[
            copies,
            copies,
            copies,
            copies,
            pltpu.VMEM((CHANNELS, 2 * TALL), BF16),
            pltpu.VMEM((CHANNELS, 2 * TALL), BF16),
            field,
            field,
            fields,
            fields,
            field,
        ],
        compiler_params=pltpu.CompilerParams(vmem_limit_bytes=56 << 20),
        name="compute",
    )(moves, values, rewards, hidden_state, weights)


def adam(param, grad, mean, square):
    mean_new = beta_one * mean + (1.0 - beta_one) * grad
    square_new = beta_two * square + (1.0 - beta_two) * grad * grad
    param_new = param - step_size * mean_new / (jnp.sqrt(square_new) + eps_adam)
    return param_new, mean_new, square_new, grad


def adam_kernel(parts, *refs):
    params, means, squares, outs = refs[0:4], refs[4:8], refs[8:12], refs[12:]
    new, mean_new, square_new, grads = outs[0:4], outs[4:8], outs[8:12], outs[12:16]
    total = parts[0].astype(F32)
    for piece in range(1, 8):
        total = total + parts[piece].astype(F32)
    for which in range(2):
        for tap in range(9):
            a, b, at = tap // 3, tap % 3, 18 * which + 2 * tap
            results = adam(
                params[which][a, b], total[at : at + 2], means[which][a, b], squares[which][a, b]
            )
            for ref, result in zip((new, mean_new, square_new, grads), results):
                ref[which][a, b] = result
    head = jnp.concatenate([total[36 + 2 * k : 38 + 2 * k] for k in range(5)], axis=1)[:, 0:BUCKETS]
    results = adam(params[2][0], head, means[2][0], squares[2][0])
    for ref, result in zip((new, mean_new, square_new, grads), results):
        ref[2][0] = result
    embed = jnp.concatenate([total[46:47, 0:1], total[47:48, 0:1]], axis=1)
    results = adam(params[3][...], embed, means[3][...], squares[3][...])
    for ref, result in zip((new, mean_new, square_new, grads), results):
        ref[3][...] = result


def updates(parts, params, means, squares):
    vmem = pl.BlockSpec(memory_space=pltpu.VMEM)
    shapes = [jax.ShapeDtypeStruct(p.shape, F32) for p in params]
    return pl.pallas_call(
        adam_kernel,
        out_shape=shapes * 4,
        in_specs=[vmem] * 13,
        out_specs=[vmem] * 16,
        compiler_params=pltpu.CompilerParams(vmem_limit_bytes=8 << 20),
        name="adam",
    )(parts, *params, *means, *squares)


def local(
    hidden_state,
    actions,
    value_target,
    reward_target,
    kernel_first,
    kernel_second,
    head_weight,
    action_embed,
    first_mean,
    first_square,
    second_mean,
    second_square,
    head_mean,
    head_square,
    embed_mean,
    embed_square,
):
    params = (kernel_first, kernel_second, head_weight, action_embed)
    weights = gather(*params).reshape(2, ITEMS, CHANNELS, 128)
    grads = compute(actions, value_target, reward_target, hidden_state, weights)
    parts = scatter(grads.reshape(2, ITEMS, 4, 4, 16, 128))
    outs = updates(
        parts,
        params,
        (first_mean, second_mean, head_mean, embed_mean),
        (first_square, second_square, head_square, embed_square),
    )
    new, means, squares, sums = outs[0:4], outs[4:8], outs[8:12], outs[12:16]
    moments = [moment for pair in zip(means, squares) for moment in pair]
    return (*new, *moments, *sums)


def solution(mesh):
    torus = Mesh(mesh.devices.reshape(4, 8, 4, mesh.shape["mp"]), ("dp_0", "dp_1", "dp_2", "mp"))
    kernel = P(None, None, DP, "mp")
    head = P("mp", DP, None)
    embed = P("mp", DP)
    rows = P(DP, None)
    placed = (P(DP, None, None, None), rows, rows, rows, kernel, kernel, head, embed)
    moments = (kernel, kernel, kernel, kernel, head, head, embed, embed)
    return jax.shard_map(
        local,
        mesh=torus,
        in_specs=placed + moments,
        out_specs=(kernel, kernel, head, embed) + moments + (kernel, kernel, head, embed),
        check_vma=False,
    )
```

```python
import functools

import jax
import jax.numpy as jnp
from jax import lax
from jax.experimental import pallas as pl
from jax.experimental.pallas import tpu as pltpu
from jax.sharding import Mesh
from jax.sharding import PartitionSpec as P

MESH = pl.DeviceIdType.MESH
CHANNELS = 256
DP = ("dp_0", "dp_1", "dp_2")
SIDE = 19
CELLS = 361
BUCKETS = 601
PITCH = 32
ROWS = SIDE * PITCH
TALL = 640
DEPTH = 704
ITEMS = 24
HEAD, SECOND, FIRST, EMBED = 0, 5, 14, 23
CHUNKS = (((0, 2, 0), (2, 3, 0)), ((5, 5, 2), (10, 4, 3)), ((14, 5, 7), (19, 5, 7)))
HALVES = (("dp_2", "dp_0"), ("dp_0", "dp_2"))
ORDER = (1, 3, 2)
SCALE = (9.0 * CHANNELS) ** (-0.5)

head_scale = 4.0
soft_cap = 15.0
eps_norm = 1e-05
beta_one = 0.9
beta_two = 0.999
step_size = 0.1
eps_adam = 1e-08

F32 = jnp.float32
BF16 = jnp.bfloat16


def seats():
    return (
        lax.axis_index("dp_0"),
        lax.axis_index("dp_1"),
        lax.axis_index("dp_2"),
        lax.axis_index("mp"),
    )


def greet_all(y, z, x, c):
    barrier = pltpu.get_barrier_semaphore()
    for step in range(1, 8):
        pl.semaphore_signal(
            barrier, inc=1, device_id={"dp_1": lax.rem(z + step, 8)}, device_id_type=MESH
        )
    for step in range(1, 4):
        for name, here in (("dp_0", y), ("dp_2", x)):
            pl.semaphore_signal(
                barrier, inc=1, device_id={name: lax.rem(here + step, 4)}, device_id_type=MESH
            )
    pl.semaphore_signal(barrier, inc=1, device_id={"mp": 1 - c}, device_id_type=MESH)
    return barrier


def remote(src, dst, send, recv, peer):
    return pltpu.make_async_remote_copy(
        src_ref=src, dst_ref=dst, send_sem=send, recv_sem=recv, device_id=peer, device_id_type=MESH
    )


def arrived(ref, recv, send, peer):
    remote(ref, ref, send, recv, peer).wait_recv()


class Gather:
    def __init__(self, seat, w, stage, wide, sems, started):
        self.y, self.z, self.x, self.c = seat
        self.here = {"dp_0": self.y, "dp_2": self.x}
        self.w, self.stage, self.wide, self.started = w, stage, wide, started
        self.z_send, self.z_recv, self.p_send, self.p_recv = sems[0:4]
        self.q_send, self.q_recv, self.r_send, self.r_recv, self.m_send, self.m_recv = sems[4:10]
        self.partner = {"mp": 1 - self.c}

    def launch(self, copy):
        copy.start()
        self.started.append(copy)

    def tile(self, chunk, half, near, far):
        start, count, _ = CHUNKS[chunk][half]
        items = pl.ds(start, count)
        if half == 0:
            return self.w.at[self.c, items, far, near]
        return self.w.at[self.c, items, near, far]

    def slab(self, chunk, half, far, core, part=None):
        start, count, _ = CHUNKS[chunk][half]
        items = pl.ds(start, count)
        span = pl.ds(0, 4) if part is None else pl.ds(2 * part, 2)
        if half == 0:
            return self.w.at[core, items, far, span]
        return self.w.at[core, items, span, far]

    def along_z(self):
        z = self.z
        for step in range(1, 8):
            peer = {"dp_1": lax.rem(z + step, 8)}
            ref = self.stage.at[z]
            self.launch(remote(ref, ref, self.z_send.at[step], self.z_recv.at[z], peer))

    def near_sends(self):
        z = self.z
        for step in range(1, 8):
            peer = lax.rem(z + step, 8)
            arrived(self.stage.at[peer], self.z_recv.at[peer], self.z_send.at[0], {"dp_1": peer})
        for piece in range(8):
            self.wide[56 * piece : 56 * piece + 48, :] = self.stage[piece].astype(F32)
        for chunk in (2, 1, 0):
            for half, (near, far) in enumerate(HALVES):
                start, count, _ = CHUNKS[chunk][half]
                for item in range(start, start + count):
                    low = self.wide[pl.ds(2 * item, 8, stride=56), :]
                    high = self.wide[pl.ds(2 * item + 1, 8, stride=56), :]
                    block = jnp.concatenate([low, high], axis=0).astype(BF16)
                    self.w[self.c, item, self.y, self.x] = block
            for step in ORDER:
                for half, (near, far) in enumerate(HALVES):
                    at = self.here[near]
                    ref = self.tile(chunk, half, at, self.here[far])
                    self.launch(
                        remote(
                            ref, ref, self.p_send.at[chunk, half, step], self.p_recv.at[chunk, half, at],
                            {near: lax.rem(at + step, 4)},
                        )
                    )

    def to_partner(self, chunk, half, piece, ref):
        self.launch(
            remote(
                ref, ref, self.m_send.at[chunk, half, piece], self.m_recv.at[chunk, half, piece], self.partner
            )
        )

    def far_sends(self, chunk):
        for half, (near, far) in enumerate(HALVES):
            for step in ORDER:
                peer = lax.rem(self.here[near] + step, 4)
                ref = self.tile(chunk, half, peer, self.here[far])
                arrived(ref, self.p_recv.at[chunk, half, peer], self.p_send.at[chunk, half, 0], {near: peer})
            at = self.here[far]
            ref = self.slab(chunk, half, at, self.c)
            for way, step in enumerate((1, 3)):
                self.launch(
                    remote(
                        ref, ref, self.q_send.at[chunk, half, way], self.q_recv.at[chunk, half, way],
                        {far: lax.rem(at + step, 4)},
                    )
                )
            self.to_partner(chunk, half, 0, ref)

    def relays(self, chunk):
        for half, (near, far) in enumerate(HALVES):
            at = self.here[far]
            for way, (step, back) in enumerate(((1, 3), (3, 1))):
                peer = lax.rem(at + back, 4)
                ref = self.slab(chunk, half, peer, self.c)
                arrived(ref, self.q_recv.at[chunk, half, way], self.q_send.at[chunk, half, way], {far: peer})
                part = self.slab(chunk, half, peer, self.c, way)
                self.launch(
                    remote(
                        part, part, self.r_send.at[chunk, half, way], self.r_recv.at[chunk, half, way],
                        {far: lax.rem(at + step, 4)},
                    )
                )
                self.to_partner(chunk, half, 1 + way, ref)

    def finish(self, chunk):
        for half, (near, far) in enumerate(HALVES):
            peer = lax.rem(self.here[far] + 2, 4)
            for way in range(2):
                part = self.slab(chunk, half, peer, self.c, way)
                arrived(part, self.r_recv.at[chunk, half, way], self.r_send.at[chunk, half, way], {far: peer})
                self.to_partner(chunk, half, 3 + way, part)
        for half, (near, far) in enumerate(HALVES):
            at, other = self.here[far], 1 - self.c
            refs = [self.slab(chunk, half, lax.rem(at + step, 4), other) for step in (0, 3, 1)]
            refs += [self.slab(chunk, half, lax.rem(at + 2, 4), other, way) for way in range(2)]
            for piece, ref in enumerate(refs):
                sems = self.m_recv.at[chunk, half, piece], self.m_send.at[chunk, half, piece]
                arrived(ref, *sems, self.partner)


class Scatter:
    def __init__(self, seat, g, buffers, sems, started):
        self.y, self.z, self.x, self.c = seat
        self.here = {"dp_0": self.y, "dp_2": self.x}
        self.g, self.started = g, started
        self.inbox, self.sums, a_in, b_in, a_sum, b_sum, a_last, b_last, self.flat = buffers
        self.arrivals, self.folded, self.last = (a_in, b_in), (a_sum, b_sum), (a_last, b_last)
        self.m_send, self.m_recv, self.p_send, self.p_recv = sems[0:4]
        self.q_send, self.q_recv, self.z_send, self.z_recv = sems[4:8]
        self.partner = {"mp": 1 - self.c}

    def launch(self, copy):
        copy.start()
        self.started.append(copy)

    def across(self, chunk, half):
        start, count, _ = CHUNKS[chunk][half]
        items = pl.ds(start, count)
        return remote(
            self.g.at[1 - self.c, items], self.inbox.at[items], self.m_send.at[chunk, half],
            self.m_recv.at[chunk, half], self.partner,
        )

    def to_partner(self, chunk, half):
        self.launch(self.across(chunk, half))

    def near_sends(self, chunk, half):
        near, far = HALVES[half]
        start, count, at = CHUNKS[chunk][half]
        self.across(chunk, half).wait_recv()

        def join(item, carry):
            total = self.g[self.c, item].astype(F32) + self.inbox[item].astype(F32)
            self.sums[item] = total.astype(BF16)
            return carry

        lax.fori_loop(start, start + count, join, 0)
        items = pl.ds(start, count)
        for step in ORDER:
            peer = lax.rem(self.here[near] + step, 4)
            ref = self.sums.at[items, :, peer] if half == 0 else self.sums.at[items, peer]
            self.launch(
                remote(
                    ref, self.arrivals[half].at[self.here[near], pl.ds(at, count)],
                    self.p_send.at[chunk, half, step], self.p_recv.at[chunk, half, self.here[near]], {near: peer},
                )
            )

    def far_sends(self, chunk, half):
        near, far = HALVES[half]
        start, count, at = CHUNKS[chunk][half]
        peers = [lax.rem(self.here[near] + step, 4) for step in (1, 2, 3)]
        box, total_of = self.arrivals[half], self.folded[half]
        for peer in peers:
            ref = box.at[peer, pl.ds(at, count)]
            arrived(ref, self.p_recv.at[chunk, half, peer], self.p_send.at[chunk, half, 0], {near: peer})

        def fold(item, carry):
            own = self.sums[start + item, :, self.x] if half == 0 else self.sums[start + item, self.y]
            total = own.astype(F32)
            for peer in peers:
                total = total + box[peer, at + item].astype(F32)
            total_of[at + item] = total.astype(BF16)
            return carry

        lax.fori_loop(0, count, fold, 0)
        for step in ORDER:
            peer = lax.rem(self.here[far] + step, 4)
            self.launch(
                remote(
                    total_of.at[pl.ds(at, count), peer], self.last[half].at[self.here[far], pl.ds(at, count)],
                    self.q_send.at[chunk, half, step], self.q_recv.at[chunk, half, self.here[far]], {far: peer},
                )
            )

    def settle(self, chunk, half):
        near, far = HALVES[half]
        start, count, at = CHUNKS[chunk][half]
        peers = [lax.rem(self.here[far] + step, 4) for step in (1, 2, 3)]
        box, total_of = self.last[half], self.folded[half]
        for peer in peers:
            ref = box.at[peer, pl.ds(at, count)]
            arrived(ref, self.q_recv.at[chunk, half, peer], self.q_send.at[chunk, half, 0], {far: peer})

        def close(item, carry):
            total = total_of[at + item, self.here[far]].astype(F32)
            for peer in peers:
                total = total + box[peer, at + item].astype(F32)
            self.flat[pl.ds(pl.multiple_of((start + item) * 16, 16), 16), :] = total
            return carry

        lax.fori_loop(0, count, close, 0)

    def along_z(self, turn, item, letters, out):
        rows = letters.shape[1]
        for spot in range(8):
            letters[spot] = self.flat[pl.ds(16 * item + spot, rows, stride=8), :].astype(BF16)
        for step in range(1, 8):
            peer = lax.rem(self.z + step, 8)
            self.launch(
                remote(
                    letters.at[peer], out.at[self.z], self.z_send.at[turn, step], self.z_recv.at[turn, self.z],
                    {"dp_1": peer},
                )
            )
        out[self.z] = letters[self.z]

    def collect(self, turn, out):
        for step in range(1, 8):
            peer = lax.rem(self.z + step, 8)
            arrived(out.at[peer], self.z_recv.at[turn, peer], self.z_send.at[turn, 0], {"dp_1": peer})


NN = (((1,), (0,)), ((), ()))
NT = (((1,), (1,)), ((), ()))
TN = (((0,), (0,)), ((), ()))


def dot(a, b, dims=NN):
    return lax.dot_general(a, b, dims, preferred_element_type=F32)


def window_kernel(
    moves, values, rewards, hidden_in, first_in, second_in, head_in, embed_in, early, late,
    first_v, second_v, head_v, embed_v, hidden_v, rows, stage, wide, w, g,
    inbox, sums, a_in, b_in, a_sum, b_sum, a_last, b_last, flat, early_out, late_out,
    xs, hs, bs, zs, xt, bt, state, mixed, pre, summed, saved, local_sem, *sems,
):
    seat = y, z, x, c = seats()
    barrier = greet_all(y, z, x, c)
    pairs = (
        (first_in, first_v), (second_in, second_v), (head_in, head_v), (embed_in, embed_v), (hidden_in, hidden_v)
    )
    loads = [pltpu.make_async_copy(src, dst, local_sem.at[k]) for k, (src, dst) in enumerate(pairs)]
    for load in loads:
        load.start()
    started = []
    gather = Gather(seat, w, stage, wide, sems[0:10], started)
    scatter = Scatter(
        seat, g, (inbox, sums, a_in, b_in, a_sum, b_sum, a_last, b_last, flat), sems[10:18], started
    )
    rows[2 * HEAD : 2 * SECOND, :] = jnp.zeros((10, 128), F32)
    for load in loads[0:4]:
        load.wait()
    for tap in range(9):
        at = 2 * (SECOND + tap)
        rows[at : at + 2, :] = second_v[tap // 3, tap % 3]
        at = 2 * (FIRST + tap)
        rows[at : at + 2, :] = first_v[tap // 3, tap % 3]
    for block in range(5):
        width = min(128, BUCKETS - 128 * block)
        at = 2 * (HEAD + block)
        rows[at : at + 2, 0:width] = head_v[0, :, 128 * block : 128 * block + width]
    for r in range(2):
        at = 2 * EMBED + r
        rows[at : at + 1, :] = jnp.broadcast_to(embed_v[:, r : r + 1], (1, 128))
    stage[z] = rows[...].astype(BF16)
    pl.semaphore_wait(barrier, 14)
    gather.along_z()

    row = lax.broadcasted_iota(jnp.int32, (ROWS, CHANNELS), 0)
    valid = lax.rem(row, PITCH) < SIDE

    def whole(h, item):
        return w[h, item].reshape(CHANNELS, 128)

    def first(tap):
        return jnp.concatenate([whole(0, FIRST + tap), whole(1, FIRST + tap)], axis=1)

    def second(tap):
        return jnp.concatenate([whole(0, SECOND + tap), whole(1, SECOND + tap)], axis=1)

    def head(h):
        return jnp.concatenate([whole(h, HEAD + k) for k in range(5)], axis=1)

    def conv(field, kernel, flip):
        taps = [8 - t if flip else t for t in range(9)]
        lhs = jnp.concatenate(
            [field[t % 3, PITCH * (t // 3) : PITCH * (t // 3) + ROWS] for t in range(9)], axis=1
        )
        return lhs, [kernel(t) for t in taps]

    def conv_plain(field, kernel, flip):
        lhs, parts = conv(field, kernel, flip)
        return dot(lhs, jnp.concatenate(parts, axis=0))

    def conv_swapped(field, kernel, flip):
        lhs, parts = conv(field, kernel, flip)
        return dot(lhs, jnp.concatenate(parts, axis=1), NT)

    def spread(value, dest):
        dest[1, PITCH : PITCH + ROWS] = value.astype(BF16)
        dest[0, PITCH : PITCH + ROWS] = pltpu.roll(value, 1, 0).astype(BF16)
        dest[2, PITCH : PITCH + ROWS] = pltpu.roll(value, ROWS - 1, 0).astype(BF16)

    def turned(value):
        tall = jnp.concatenate([value, jnp.zeros((TALL - ROWS, CHANNELS), F32)], axis=0)
        return tall.T.astype(BF16)

    def total(value):
        return jnp.sum(jnp.sum(value, axis=0, keepdims=True), axis=1, keepdims=True)

    def store(h, item, value):
        g[h, item] = value.astype(BF16).reshape(4, 4, 16, 128)

    for field in (xs, hs, bs, zs):
        for k in range(2):
            for b in range(3):
                field[k, b, 0:PITCH] = jnp.zeros((PITCH, CHANNELS), BF16)
                field[k, b, PITCH + ROWS : DEPTH] = jnp.zeros((DEPTH - PITCH - ROWS, CHANNELS), BF16)
    flat[16 * FIRST : 16 * FIRST + 32, :] = jnp.zeros((32, 128), F32)

    state[...] = jnp.zeros((ROWS, CHANNELS), F32)
    loads[4].wait()

    def place(line, carry):
        cells = hidden_v[line].astype(F32)
        mine = jnp.where(c == 0, cells[:, 0, :], cells[:, 1, :])
        state[pl.ds(pl.multiple_of(PITCH * line, PITCH), SIDE), :] = mine
        return carry

    lax.fori_loop(0, SIDE, place, 0)
    lane = lax.broadcasted_iota(jnp.int32, (CHANNELS, CHANNELS), 1)
    natural = 64 * (lane // 64) + 8 * (lane % 8) + 2 * ((lane // 16) % 4) + (lane // 8) % 2
    source = lax.broadcasted_iota(jnp.int32, (CHANNELS, CHANNELS), 0)
    permute = jnp.where(source == natural, 1.0, 0.0).astype(BF16)
    state[...] = dot(state[...].astype(BF16), permute)

    gather.near_sends()
    for chunk in (2, 1, 0):
        gather.far_sends(chunk)
    for chunk in (2, 1, 0):
        gather.relays(chunk)
    gather.finish(2)

    ones = jnp.ones((16, 128), BF16)
    pick = lax.broadcasted_iota(jnp.int32, (16, 128), 1) == 0
    pick = jnp.where(pick, ones, jnp.zeros_like(ones))
    embed = [dot(pick, whole(e, EMBED), NT)[0:1, :] for e in range(2)]

    bucket = lax.broadcasted_iota(jnp.int32, (16, 640), 1)
    kept = []
    pooled_rows = jnp.zeros((16, CHANNELS), F32)
    grad_rows = [jnp.zeros((16, 640), F32) for _ in range(2)]
    for k in range(2):
        move = moves[c, k]
        spot = PITCH * lax.div(move, SIDE) + lax.rem(move, SIDE)
        passed = move == CELLS
        added = jnp.where(row == spot, embed[0], 0.0) + jnp.where(passed, 1.0, 0.0) * embed[1]
        now = jnp.where(valid, state[...] + added, 0.0)
        mixed[...] = now
        spread(now, xs.at[k])
        xt[:, TALL * k : TALL * k + TALL] = turned(now)
        value = SCALE * conv_plain(xs.at[k], first, False)
        pre[k] = value
        spread(jnp.where(valid, value * jax.nn.sigmoid(value), 0.0), hs.at[k])
        if k == 0:
            gather.finish(1)
        branch = conv_swapped(hs.at[k], second, False)
        value = jnp.where(valid, mixed[...] + SCALE * branch, 0.0)
        summed[k] = value
        factor = lax.rsqrt(total(value * value) / (CELLS * CHANNELS) + eps_norm)
        value = value * factor
        state[...] = value
        if k == 0:
            gather.finish(0)
        pooled = (jnp.sum(value, axis=0, keepdims=True) / CELLS).astype(BF16)
        pooled = jnp.broadcast_to(pooled.astype(F32), (16, CHANNELS))
        own_row = lax.broadcasted_iota(jnp.int32, (16, CHANNELS), 0) == k
        pooled_rows = jnp.where(own_row, pooled, pooled_rows)
        pooled = pooled.astype(BF16)
        pooled_grad = jnp.zeros((16, CHANNELS), F32)
        for h, targets in enumerate((values, rewards)):
            raw = head_scale * dot(pooled, head(h))
            squashed = jnp.tanh(raw / soft_cap)
            raised = jnp.where(bucket < BUCKETS, jnp.exp(soft_cap * squashed), 0.0)
            chances = raised / jnp.sum(raised, axis=1, keepdims=True)
            picked = jnp.where(bucket == targets[c, k], 1.0, 0.0)
            logit = (chances - picked) * (1.0 - squashed * squashed) / 256.0
            logit = jnp.where(bucket < BUCKETS, logit, 0.0).astype(BF16)
            pooled_grad = pooled_grad + dot(logit, head(h), NT)
            logit = logit.astype(F32)
            own_row = lax.broadcasted_iota(jnp.int32, (16, 640), 0) == k
            grad_rows[h] = jnp.where(own_row, logit, grad_rows[h])
        kept.append((spot, passed, factor, head_scale * pooled_grad[0:1, :] / CELLS))

    for h in range(2):
        grad = head_scale * dot(pooled_rows.astype(BF16), grad_rows[h].astype(BF16), TN)
        for block in range(5):
            store(h, HEAD + block, grad[:, 128 * block : 128 * block + 128])
    for half in range(2):
        scatter.to_partner(0, half)

    def window(field, tap):
        start = PITCH * (tap // 3)
        return jnp.concatenate([field[k, tap % 3, start : start + TALL] for k in range(2)], axis=0)

    embed_grad = [jnp.zeros((1, CHANNELS), F32) for _ in range(2)]
    for k in (1, 0):
        spot, passed, factor, pooled_grad = kept[k]
        grad = pooled_grad if k == 1 else saved[...] + pooled_grad
        grad = jnp.where(valid, grad, 0.0)
        value = summed[k]
        slope = total(grad * value) / (CELLS * CHANNELS)
        summed_grad = factor * grad - factor * factor * factor * value * slope
        saved[...] = summed_grad
        spread(summed_grad, bs.at[k])
        bt[:, TALL * k : TALL * k + TALL] = turned(summed_grad)
        if k == 0:
            for tap in range(9):
                grad = SCALE * dot(bt[...], window(hs, tap))
                store(0, SECOND + tap, grad[:, 0:128])
                store(1, SECOND + tap, grad[:, 128:256])
                if tap == 4:
                    scatter.to_partner(1, 0)
            scatter.to_partner(1, 1)
        hidden_grad = SCALE * conv_plain(bs.at[k], second, True)
        for half in range(2):
            scatter.near_sends(1 - k, half)
        value = pre[k]
        sig = jax.nn.sigmoid(value)
        inner = hidden_grad * (sig * (1.0 + value * (1.0 - sig)))
        spread(jnp.where(valid, inner, 0.0), zs.at[k])
        carry = saved[...] + SCALE * conv_swapped(zs.at[k], first, True)
        carry = jnp.where(valid, carry, 0.0)
        saved[...] = carry
        embed_grad[0] = embed_grad[0] + jnp.sum(jnp.where(row == spot, carry, 0.0), axis=0, keepdims=True)
        embed_grad[1] = embed_grad[1] + jnp.where(passed, 1.0, 0.0) * jnp.sum(carry, axis=0, keepdims=True)
        if k == 1:
            for half in range(2):
                scatter.far_sends(0, half)

    for e in range(2):
        lines = jnp.broadcast_to(embed_grad[e], (16, CHANNELS)).astype(BF16)
        top = lax.broadcasted_iota(jnp.int32, (16, 128), 0) == 0
        store(e, EMBED, dot(lines, jnp.where(top, ones, jnp.zeros_like(ones)), TN))

    for tap in range(9):
        grad = SCALE * dot(xt[...], window(zs, 8 - tap))
        store(0, FIRST + tap, grad[:, 0:128])
        store(1, FIRST + tap, grad[:, 128:256])
        if tap == 4:
            scatter.to_partner(2, 0)
    scatter.to_partner(2, 1)
    scatter.near_sends(2, 0)
    for half in range(2):
        scatter.settle(0, half)
        scatter.far_sends(1, half)
    scatter.near_sends(2, 1)
    for half in range(2):
        scatter.settle(1, half)
    scatter.along_z(0, 0, early_out, early)
    for half in range(2):
        scatter.far_sends(2, half)
    for half in range(2):
        scatter.settle(2, half)
    scatter.along_z(1, 12, late_out, late)
    scatter.collect(0, early)
    scatter.collect(1, late)
    for copy in started:
        copy.wait_send()


def window_grads(moves, values, rewards, hidden_state, params):
    vmem = pl.BlockSpec(memory_space=pltpu.VMEM)
    smem = pl.BlockSpec(memory_space=pltpu.SMEM)
    hbm = pl.BlockSpec(memory_space=pltpu.HBM)
    dma = pltpu.SemaphoreType.DMA
    copies = pltpu.VMEM((2, 3, DEPTH, CHANNELS), BF16)
    turned = pltpu.VMEM((CHANNELS, 2 * TALL), BF16)
    field = pltpu.VMEM((ROWS, CHANNELS), F32)
    fields = pltpu.VMEM((2, ROWS, CHANNELS), F32)
    board = pltpu.VMEM((ITEMS, 4, 4, 16, 128), BF16)
    boards = pltpu.VMEM((2, ITEMS, 4, 4, 16, 128), BF16)
    early, late = (8, 32, 128), (8, 24, 128)
    return pl.pallas_call(
        window_kernel,
        out_shape=[jax.ShapeDtypeStruct(early, BF16), jax.ShapeDtypeStruct(late, BF16)],
        in_specs=[smem] * 3 + [hbm] * 5,
        out_specs=[vmem, vmem],
        scratch_shapes=[pltpu.VMEM(p.shape, F32) for p in params]
        + [
            pltpu.VMEM(hidden_state.shape, BF16),
            pltpu.VMEM((48, 128), F32),
            pltpu.VMEM((8, 48, 128), BF16),
            pltpu.VMEM((448, 128), F32),
            boards,
            boards,
            board,
            board,
            pltpu.VMEM((4, 12, 4, 16, 128), BF16),
            pltpu.VMEM((4, 12, 4, 16, 128), BF16),
            pltpu.VMEM((12, 4, 16, 128), BF16),
            pltpu.VMEM((12, 4, 16, 128), BF16),
            pltpu.VMEM((4, 12, 16, 128), BF16),
            pltpu.VMEM((4, 12, 16, 128), BF16),
            pltpu.VMEM((384, 128), F32),
            pltpu.VMEM(early, BF16),
            pltpu.VMEM(late, BF16),
            copies,
            copies,
            copies,
            copies,
            turned,
            turned,
            field,
            field,
            fields,
            fields,
            field,
            dma((5,)),
        ]
        + [
            dma(shape)
            for shape in (
                (8,), (8,), (3, 2, 4), (3, 2, 4), (3, 2, 2), (3, 2, 2), (3, 2, 2), (3, 2, 2), (3, 2, 5), (3, 2, 5),
                (3, 2), (3, 2), (3, 2, 4), (3, 2, 4), (3, 2, 4), (3, 2, 4), (2, 8), (2, 8),
            )
        ],
        compiler_params=pltpu.CompilerParams(
            collective_id=0, has_side_effects=True, vmem_limit_bytes=58 << 20
        ),
        name="window",
    )(moves, values, rewards, hidden_state, *params)


def adam(param, grad, mean, square):
    mean_new = beta_one * mean + (1.0 - beta_one) * grad
    square_new = beta_two * square + (1.0 - beta_two) * grad * grad
    param_new = param - step_size * mean_new / (jnp.sqrt(square_new) + eps_adam)
    return param_new, mean_new, square_new, grad


def adam_kernel(early, late, *refs):
    params, means, squares, outs = refs[0:4], refs[4:8], refs[8:12], refs[12:]
    new, mean_new, square_new, grads = outs[0:4], outs[4:8], outs[8:12], outs[12:16]
    totals = []
    for parts in (early, late):
        total = parts[0].astype(F32)
        for piece in range(1, 8):
            total = total + parts[piece].astype(F32)
        totals.append(total)

    def owned(item):
        if item < FIRST:
            return totals[0][2 * item : 2 * item + 2]
        return totals[1][2 * (item - 12) : 2 * (item - 12) + 2]

    for which in range(2):
        for tap in range(9):
            a, b = tap // 3, tap % 3
            grad = owned((FIRST, SECOND)[which] + tap)
            results = adam(params[which][a, b], grad, means[which][a, b], squares[which][a, b])
            for ref, result in zip((new, mean_new, square_new, grads), results):
                ref[which][a, b] = result
    head = jnp.concatenate([owned(HEAD + k) for k in range(5)], axis=1)[:, 0:BUCKETS]
    results = adam(params[2][0], head, means[2][0], squares[2][0])
    for ref, result in zip((new, mean_new, square_new, grads), results):
        ref[2][0] = result
    embed = owned(EMBED)
    embed = jnp.concatenate([embed[0:1, 0:1], embed[1:2, 0:1]], axis=1)
    results = adam(params[3][...], embed, means[3][...], squares[3][...])
    for ref, result in zip((new, mean_new, square_new, grads), results):
        ref[3][...] = result


def updates(early, late, params, means, squares):
    vmem = pl.BlockSpec(memory_space=pltpu.VMEM)
    shapes = [jax.ShapeDtypeStruct(p.shape, F32) for p in params]
    return pl.pallas_call(
        adam_kernel,
        out_shape=shapes * 4,
        in_specs=[vmem] * 14,
        out_specs=[vmem] * 16,
        compiler_params=pltpu.CompilerParams(vmem_limit_bytes=8 << 20),
        name="adam",
    )(early, late, *params, *means, *squares)


def local(
    hidden_state,
    actions,
    value_target,
    reward_target,
    kernel_first,
    kernel_second,
    head_weight,
    action_embed,
    first_mean,
    first_square,
    second_mean,
    second_square,
    head_mean,
    head_square,
    embed_mean,
    embed_square,
):
    params = (kernel_first, kernel_second, head_weight, action_embed)
    boards = jnp.transpose(hidden_state, (1, 2, 0, 3))
    early, late = window_grads(actions, value_target, reward_target, boards, params)
    outs = updates(
        early,
        late,
        params,
        (first_mean, second_mean, head_mean, embed_mean),
        (first_square, second_square, head_square, embed_square),
    )
    new, means, squares, sums = outs[0:4], outs[4:8], outs[8:12], outs[12:16]
    moments = [moment for pair in zip(means, squares) for moment in pair]
    return (*new, *moments, *sums)


def solution(mesh):
    torus = Mesh(mesh.devices.reshape(4, 8, 4, mesh.shape["mp"]), ("dp_0", "dp_1", "dp_2", "mp"))
    kernel = P(None, None, DP, "mp")
    head = P("mp", DP, None)
    embed = P("mp", DP)
    rows = P(DP, None)
    placed = (P(DP, None, None, None), rows, rows, rows, kernel, kernel, head, embed)
    moments = (kernel, kernel, kernel, kernel, head, head, embed, embed)
    return jax.shard_map(
        local,
        mesh=torus,
        in_specs=placed + moments,
        out_specs=(kernel, kernel, head, embed) + moments + (kernel, kernel, head, embed),
        check_vma=False,
    )
```

```python
import functools

import jax
import jax.numpy as jnp
from jax import lax
from jax.experimental import pallas as pl
from jax.experimental.pallas import tpu as pltpu
from jax.sharding import Mesh
from jax.sharding import PartitionSpec as P

MESH = pl.DeviceIdType.MESH
CHANNELS = 256
DP = ("dp_0", "dp_1", "dp_2")
SIDE = 19
CELLS = 361
BUCKETS = 601
PITCH = 32
ROWS = SIDE * PITCH
TALL = 640
DEPTH = 704
ITEMS = 24
HEAD, SECOND, FIRST, EMBED = 0, 5, 14, 23
CHUNKS = (((0, 2), (2, 3)), ((5, 5), (10, 4)), ((14, 5), (19, 5)))
PIECES = (
    (0, 0, 2, 0), (1, 2, 3, 0),
    (0, 5, 3, 2), (1, 8, 2, 3), (0, 10, 2, 5), (1, 12, 2, 5),
    (0, 14, 2, 7), (1, 16, 2, 7), (0, 18, 2, 9), (1, 20, 2, 9), (0, 22, 1, 11), (1, 23, 1, 11),
)
HALVES = (("dp_2", "dp_0"), ("dp_0", "dp_2"))
ORDER = (1, 3, 2)
SCALE = (9.0 * CHANNELS) ** (-0.5)

head_scale = 4.0
soft_cap = 15.0
eps_norm = 1e-05
beta_one = 0.9
beta_two = 0.999
step_size = 0.1
eps_adam = 1e-08

F32 = jnp.float32
BF16 = jnp.bfloat16


def scoped(method):
    @functools.wraps(method)
    def inner(self, *given):
        tag = "_".join(str(v) for v in given if isinstance(v, int))
        with jax.named_scope(f"{type(self).__name__}_{method.__name__}_{tag}"):
            return method(self, *given)

    return inner


def seats():
    return (
        lax.axis_index("dp_0"),
        lax.axis_index("dp_1"),
        lax.axis_index("dp_2"),
        lax.axis_index("mp"),
    )


def greet_all(y, z, x, c):
    barrier = pltpu.get_barrier_semaphore()
    for step in range(1, 8):
        pl.semaphore_signal(
            barrier, inc=1, device_id={"dp_1": lax.rem(z + step, 8)}, device_id_type=MESH
        )
    for step in range(1, 4):
        for name, here in (("dp_0", y), ("dp_2", x)):
            pl.semaphore_signal(
                barrier, inc=1, device_id={name: lax.rem(here + step, 4)}, device_id_type=MESH
            )
    pl.semaphore_signal(barrier, inc=1, device_id={"mp": 1 - c}, device_id_type=MESH)
    return barrier


def remote(src, dst, send, recv, peer):
    return pltpu.make_async_remote_copy(
        src_ref=src, dst_ref=dst, send_sem=send, recv_sem=recv, device_id=peer, device_id_type=MESH
    )


def arrived(ref, recv, send, peer):
    remote(ref, ref, send, recv, peer).wait_recv()


class Gather:
    def __init__(self, seat, w, stage, wide, sems, started):
        self.y, self.z, self.x, self.c = seat
        self.here = {"dp_0": self.y, "dp_2": self.x}
        self.w, self.stage, self.wide, self.started = w, stage, wide, started
        self.z_send, self.z_recv, self.p_send, self.p_recv = sems[0:4]
        self.q_send, self.q_recv, self.m_send, self.m_recv = sems[4:8]
        self.partner = {"mp": 1 - self.c}

    def launch(self, copy):
        copy.start()
        self.started.append(copy)

    def tile(self, chunk, half, near, far):
        items = pl.ds(*CHUNKS[chunk][half])
        if half == 0:
            return self.w.at[self.c, items, far, near]
        return self.w.at[self.c, items, near, far]

    def slab(self, chunk, half, far, core):
        items = pl.ds(*CHUNKS[chunk][half])
        if half == 0:
            return self.w.at[core, items, far]
        return self.w.at[core, items, :, far]

    @scoped
    def along_z(self):
        z = self.z
        for group in (1, 0):
            ref = self.stage.at[group, z]
            for step in range(1, 8):
                peer = {"dp_1": lax.rem(z + step, 8)}
                self.launch(remote(ref, ref, self.z_send.at[group, step], self.z_recv.at[group, z], peer))

    @scoped
    def unpack(self, group):
        for step in range(1, 8):
            peer = lax.rem(self.z + step, 8)
            sems = self.z_recv.at[group, peer], self.z_send.at[group, 0]
            arrived(self.stage.at[group, peer], *sems, {"dp_1": peer})
        for piece in range(8):
            self.wide[group, 24 * piece : 24 * piece + 24, :] = self.stage[group, piece].astype(F32)

    def to_far(self, chunk, half, turn, near):
        far = HALVES[half][1]
        at = self.here[far]
        ref = self.tile(chunk, half, near, at)
        for step in ORDER:
            self.launch(
                remote(
                    ref, ref, self.q_send.at[chunk, half, turn, step], self.q_recv.at[chunk, half, at],
                    {far: lax.rem(at + step, 4)},
                )
            )

    @scoped
    def near_sends(self, chunk):
        for half, (near, far) in enumerate(HALVES):
            start, count = CHUNKS[chunk][half]
            for item in range(start, start + count):
                group, line = item // 12, 2 * (item % 12)
                slab = self.wide.at[group]
                low = slab[pl.ds(line, 8, stride=24), :]
                high = slab[pl.ds(line + 1, 8, stride=24), :]
                self.w[self.c, item, self.y, self.x] = jnp.concatenate([low, high], axis=0).astype(BF16)
        for step in ORDER:
            for half, (near, far) in enumerate(HALVES):
                at = self.here[near]
                ref = self.tile(chunk, half, at, self.here[far])
                self.launch(
                    remote(
                        ref, ref, self.p_send.at[chunk, half, step], self.p_recv.at[chunk, half, at],
                        {near: lax.rem(at + step, 4)},
                    )
                )

    def own_sends(self, chunk):
        for half, (near, far) in enumerate(HALVES):
            self.to_far(chunk, half, 0, self.here[near])

    def to_partner(self, chunk, half, turn, ref):
        sems = self.m_send.at[chunk, half, turn], self.m_recv.at[chunk, half, turn]
        self.launch(remote(ref, ref, *sems, self.partner))

    @scoped
    def far_sends(self, chunk):
        for step in ORDER:
            for half, (near, far) in enumerate(HALVES):
                peer = lax.rem(self.here[near] + step, 4)
                ref = self.tile(chunk, half, peer, self.here[far])
                arrived(ref, self.p_recv.at[chunk, half, peer], self.p_send.at[chunk, half, 0], {near: peer})
                self.to_far(chunk, half, step, peer)
        for half, (near, far) in enumerate(HALVES):
            self.to_partner(chunk, half, 0, self.slab(chunk, half, self.here[far], self.c))

    @scoped
    def finish(self, chunk):
        for step in ORDER:
            for half, (near, far) in enumerate(HALVES):
                peer = lax.rem(self.here[far] + step, 4)
                ref = self.slab(chunk, half, peer, self.c)
                arrived(ref, self.q_recv.at[chunk, half, peer], self.q_send.at[chunk, half, 0, 0], {far: peer})
                self.to_partner(chunk, half, step, ref)
        for half, (near, far) in enumerate(HALVES):
            for turn in range(4):
                ref = self.slab(chunk, half, lax.rem(self.here[far] + turn, 4), 1 - self.c)
                sems = self.m_recv.at[chunk, half, turn], self.m_send.at[chunk, half, turn]
                arrived(ref, *sems, self.partner)


class Scatter:
    def __init__(self, seat, g, buffers, sems, started):
        self.y, self.z, self.x, self.c = seat
        self.here = {"dp_0": self.y, "dp_2": self.x}
        self.g, self.started = g, started
        self.inbox, self.sums, a_in, b_in, a_sum, b_sum, a_last, b_last, self.flat = buffers
        self.arrivals, self.folded, self.last = (a_in, b_in), (a_sum, b_sum), (a_last, b_last)
        self.m_send, self.m_recv, self.p_send, self.p_recv = sems[0:4]
        self.q_send, self.q_recv, self.z_send, self.z_recv = sems[4:8]
        self.partner = {"mp": 1 - self.c}

    def launch(self, copy):
        copy.start()
        self.started.append(copy)

    def across(self, piece):
        half, start, count, _ = PIECES[piece]
        items = pl.ds(start, count)
        return remote(
            self.g.at[1 - self.c, items], self.inbox.at[items], self.m_send.at[piece], self.m_recv.at[piece],
            self.partner,
        )

    def to_partner(self, piece):
        self.launch(self.across(piece))

    @scoped
    def near_sends(self, piece):
        half, start, count, at = PIECES[piece]
        near, far = HALVES[half]
        self.across(piece).wait_recv()
        for item in range(start, start + count):
            total = self.g[self.c, item].astype(F32) + self.inbox[item].astype(F32)
            self.sums[item] = total.astype(BF16)
        items = pl.ds(start, count)
        for step in ORDER:
            peer = lax.rem(self.here[near] + step, 4)
            ref = self.sums.at[items, :, peer] if half == 0 else self.sums.at[items, peer]
            self.launch(
                remote(
                    ref, self.arrivals[half].at[self.here[near], pl.ds(at, count)], self.p_send.at[piece, step],
                    self.p_recv.at[piece, self.here[near]], {near: peer},
                )
            )

    @scoped
    def far_sends(self, piece):
        half, start, count, at = PIECES[piece]
        near, far = HALVES[half]
        peers = [lax.rem(self.here[near] + step, 4) for step in ORDER]
        box, total_of = self.arrivals[half], self.folded[half]
        for peer in peers:
            ref = box.at[peer, pl.ds(at, count)]
            arrived(ref, self.p_recv.at[piece, peer], self.p_send.at[piece, 0], {near: peer})
        for item in range(count):
            own = self.sums[start + item, :, self.x] if half == 0 else self.sums[start + item, self.y]
            total = own.astype(F32)
            for peer in peers:
                total = total + box[peer, at + item].astype(F32)
            total_of[at + item] = total.astype(BF16)
        for step in ORDER:
            peer = lax.rem(self.here[far] + step, 4)
            self.launch(
                remote(
                    total_of.at[pl.ds(at, count), peer], self.last[half].at[self.here[far], pl.ds(at, count)],
                    self.q_send.at[piece, step], self.q_recv.at[piece, self.here[far]], {far: peer},
                )
            )

    @scoped
    def settle(self, piece):
        half, start, count, at = PIECES[piece]
        near, far = HALVES[half]
        peers = [lax.rem(self.here[far] + step, 4) for step in ORDER]
        box, total_of = self.last[half], self.folded[half]
        for peer in peers:
            ref = box.at[peer, pl.ds(at, count)]
            arrived(ref, self.q_recv.at[piece, peer], self.q_send.at[piece, 0], {far: peer})
        for item in range(count):
            total = total_of[at + item, self.here[far]].astype(F32)
            for peer in peers:
                total = total + box[peer, at + item].astype(F32)
            self.flat[16 * (start + item) : 16 * (start + item) + 16, :] = total

    @scoped
    def along_z(self, turn, item, letters, out):
        rows = letters.shape[1]
        for spot in range(8):
            letters[spot] = self.flat[pl.ds(16 * item + spot, rows, stride=8), :].astype(BF16)
        for step in range(1, 8):
            peer = lax.rem(self.z + step, 8)
            self.launch(
                remote(
                    letters.at[peer], out.at[self.z], self.z_send.at[turn, step], self.z_recv.at[turn, self.z],
                    {"dp_1": peer},
                )
            )
        out[self.z] = letters[self.z]

    @scoped
    def collect(self, turn, out):
        for step in range(1, 8):
            peer = lax.rem(self.z + step, 8)
            arrived(out.at[peer], self.z_recv.at[turn, peer], self.z_send.at[turn, 0], {"dp_1": peer})


NN = (((1,), (0,)), ((), ()))
NT = (((1,), (1,)), ((), ()))
TN = (((0,), (0,)), ((), ()))


def dot(a, b, dims=NN):
    return lax.dot_general(a, b, dims, preferred_element_type=F32)


def window_kernel(
    moves, values, rewards, hidden_in, first_in, second_in, head_in, embed_in, early, late,
    first_v, second_v, head_v, embed_v, hidden_v, rows, stage, wide, w, g,
    inbox, sums, a_in, b_in, a_sum, b_sum, a_last, b_last, flat, early_out, late_out,
    xs, hs, bs, zs, xt, bt, state, mixed, pre, summed, saved, local_sem, *sems,
):
    seat = y, z, x, c = seats()
    barrier = greet_all(y, z, x, c)
    pairs = (
        (first_in, first_v), (second_in, second_v), (head_in, head_v), (embed_in, embed_v), (hidden_in, hidden_v)
    )
    loads = [pltpu.make_async_copy(src, dst, local_sem.at[k]) for k, (src, dst) in enumerate(pairs)]
    for load in loads:
        load.start()
    started = []
    gather = Gather(seat, w, stage, wide, sems[0:8], started)
    scatter = Scatter(
        seat, g, (inbox, sums, a_in, b_in, a_sum, b_sum, a_last, b_last, flat), sems[8:16], started
    )
    rows[2 * HEAD : 2 * SECOND, :] = jnp.zeros((10, 128), F32)
    for load in loads[0:4]:
        load.wait()
    for tap in range(9):
        at = 2 * (SECOND + tap)
        rows[at : at + 2, :] = second_v[tap // 3, tap % 3]
        at = 2 * (FIRST + tap)
        rows[at : at + 2, :] = first_v[tap // 3, tap % 3]
    for block in range(5):
        width = min(128, BUCKETS - 128 * block)
        at = 2 * (HEAD + block)
        rows[at : at + 2, 0:width] = head_v[0, :, 128 * block : 128 * block + width]
    for r in range(2):
        at = 2 * EMBED + r
        rows[at : at + 1, :] = jnp.broadcast_to(embed_v[:, r : r + 1], (1, 128))
    for group in range(2):
        stage[group, z] = rows[24 * group : 24 * group + 24, :].astype(BF16)
    with jax.named_scope("barrier"):
        pl.semaphore_wait(barrier, 14)
    gather.along_z()

    def phase(run):
        def inner(*given):
            with jax.named_scope(run.__name__):
                return run(*given)

        return inner

    row = lax.broadcasted_iota(jnp.int32, (ROWS, CHANNELS), 0)
    valid = lax.rem(row, PITCH) < SIDE

    def whole(h, item):
        return w[h, item].reshape(CHANNELS, 128)

    def first(tap):
        return jnp.concatenate([whole(0, FIRST + tap), whole(1, FIRST + tap)], axis=1)

    def second(tap):
        return jnp.concatenate([whole(0, SECOND + tap), whole(1, SECOND + tap)], axis=1)

    def head(h):
        return jnp.concatenate([whole(h, HEAD + k) for k in range(5)], axis=1)

    def conv(field, kernel, flip):
        taps = [8 - t if flip else t for t in range(9)]
        lhs = jnp.concatenate(
            [field[t % 3, PITCH * (t // 3) : PITCH * (t // 3) + ROWS] for t in range(9)], axis=1
        )
        return lhs, [kernel(t) for t in taps]

    @phase
    def conv_plain(field, kernel, flip):
        lhs, parts = conv(field, kernel, flip)
        rhs = jnp.concatenate(parts, axis=0)
        return jnp.concatenate([dot(lhs[: ROWS // 2], rhs), dot(lhs[ROWS // 2 :], rhs)], axis=0)

    @phase
    def conv_swapped(field, kernel, flip):
        lhs, parts = conv(field, kernel, flip)
        rhs = jnp.concatenate(parts, axis=1)
        return jnp.concatenate([dot(lhs[: ROWS // 2], rhs, NT), dot(lhs[ROWS // 2 :], rhs, NT)], axis=0)

    @phase
    def spread(value, dest):
        dest[1, PITCH : PITCH + ROWS] = value.astype(BF16)
        dest[0, PITCH : PITCH + ROWS] = pltpu.roll(value, 1, 0).astype(BF16)
        dest[2, PITCH : PITCH + ROWS] = pltpu.roll(value, ROWS - 1, 0).astype(BF16)

    @phase
    def turned(value):
        tall = jnp.concatenate([value, jnp.zeros((TALL - ROWS, CHANNELS), F32)], axis=0)
        return tall.T.astype(BF16)

    def total(value):
        return jnp.sum(jnp.sum(value, axis=0, keepdims=True), axis=1, keepdims=True)

    def store(h, item, value):
        g[h, item] = value.astype(BF16).reshape(4, 4, 16, 128)

    for field in (xs, hs, bs, zs):
        for k in range(2):
            for b in range(3):
                field[k, b, 0:PITCH] = jnp.zeros((PITCH, CHANNELS), BF16)
                field[k, b, PITCH + ROWS : DEPTH] = jnp.zeros((DEPTH - PITCH - ROWS, CHANNELS), BF16)
    flat[16 * FIRST : 16 * FIRST + 32, :] = jnp.zeros((32, 128), F32)

    state[...] = jnp.zeros((ROWS, CHANNELS), F32)
    loads[4].wait()

    def place(line, carry):
        cells = hidden_v[line].astype(F32)
        mine = jnp.where(c == 0, cells[:, 0, :], cells[:, 1, :])
        state[pl.ds(pl.multiple_of(PITCH * line, PITCH), SIDE), :] = mine
        return carry

    with jax.named_scope("place"):
        lax.fori_loop(0, SIDE, place, 0)
    lane = lax.broadcasted_iota(jnp.int32, (CHANNELS, CHANNELS), 1)
    natural = 64 * (lane // 64) + 8 * (lane % 8) + 2 * ((lane // 16) % 4) + (lane // 8) % 2
    source = lax.broadcasted_iota(jnp.int32, (CHANNELS, CHANNELS), 0)
    permute = jnp.where(source == natural, 1.0, 0.0).astype(BF16)
    state[...] = dot(state[...].astype(BF16), permute)

    gather.unpack(1)
    gather.near_sends(2)
    gather.own_sends(2)
    gather.unpack(0)
    gather.near_sends(1)
    gather.near_sends(0)
    gather.far_sends(2)
    for chunk in (1, 0):
        gather.own_sends(chunk)
        gather.far_sends(chunk)
    gather.finish(2)

    ones = jnp.ones((16, 128), BF16)
    pick = lax.broadcasted_iota(jnp.int32, (16, 128), 1) == 0
    pick = jnp.where(pick, ones, jnp.zeros_like(ones))
    embed = [dot(pick, whole(e, EMBED), NT)[0:1, :] for e in range(2)]

    kept = []
    pooled_rows = jnp.zeros((16, CHANNELS), F32)
    for k in range(2):
        move = moves[c, k]
        spot = PITCH * lax.div(move, SIDE) + lax.rem(move, SIDE)
        passed = move == CELLS
        added = jnp.where(row == spot, embed[0], 0.0) + jnp.where(passed, 1.0, 0.0) * embed[1]
        now = jnp.where(valid, state[...] + added, 0.0)
        mixed[...] = now
        spread(now, xs.at[k])
        xt[:, TALL * k : TALL * k + TALL] = turned(now)
        value = SCALE * conv_plain(xs.at[k], first, False)
        pre[k] = value
        spread(jnp.where(valid, value * jax.nn.sigmoid(value), 0.0), hs.at[k])
        if k == 0:
            gather.finish(1)
        branch = conv_swapped(hs.at[k], second, False)
        value = jnp.where(valid, mixed[...] + SCALE * branch, 0.0)
        summed[k] = value
        factor = lax.rsqrt(total(value * value) / (CELLS * CHANNELS) + eps_norm)
        value = value * factor
        state[...] = value
        pooled = jnp.sum(value, axis=0, keepdims=True) / CELLS
        own_row = lax.broadcasted_iota(jnp.int32, (16, CHANNELS), 0) == k
        pooled_rows = jnp.where(own_row, pooled, pooled_rows)
        kept.append((spot, passed, factor))
    gather.finish(0)

    bucket = lax.broadcasted_iota(jnp.int32, (16, 640), 1)
    top_row = lax.broadcasted_iota(jnp.int32, (16, 640), 0) == 0
    pooled = pooled_rows.astype(BF16)
    pooled_grads = jnp.zeros((16, CHANNELS), F32)
    logits = []
    for h, targets in enumerate((values, rewards)):
        raw = head_scale * dot(pooled, head(h))
        squashed = jnp.tanh(raw / soft_cap)
        raised = jnp.where(bucket < BUCKETS, jnp.exp(soft_cap * squashed), 0.0)
        chances = raised / jnp.sum(raised, axis=1, keepdims=True)
        picked = jnp.where(bucket == jnp.where(top_row, targets[c, 0], targets[c, 1]), 1.0, 0.0)
        logit = (chances - picked) * (1.0 - squashed * squashed) / 256.0
        logit = jnp.where(bucket < BUCKETS, logit, 0.0).astype(BF16)
        pooled_grads = pooled_grads + dot(logit, head(h), NT)
        logits.append(logit)
    for h in range(2):
        grad = head_scale * dot(pooled, logits[h], TN)
        for block in range(5):
            store(h, HEAD + block, grad[:, 128 * block : 128 * block + 128])
    for piece in (0, 1):
        scatter.to_partner(piece)

    def window(field, tap):
        start = PITCH * (tap // 3)
        return jnp.concatenate([field[k, tap % 3, start : start + TALL] for k in range(2)], axis=0)

    def second_taps(*taps):
        with jax.named_scope("second_taps"):
            for tap in taps:
                grad = SCALE * dot(bt[...], window(hs, tap))
                store(0, SECOND + tap, grad[:, 0:128])
                store(1, SECOND + tap, grad[:, 128:256])

    def first_taps(*taps):
        with jax.named_scope("first_taps"):
            for tap in taps:
                grad = SCALE * dot(xt[...], window(zs, 8 - tap))
                store(0, FIRST + tap, grad[:, 0:128])
                store(1, FIRST + tap, grad[:, 128:256])

    embed_grad = [jnp.zeros((1, CHANNELS), F32) for _ in range(2)]
    for k in (1, 0):
        spot, passed, factor = kept[k]
        grad = head_scale * pooled_grads[k : k + 1, :] / CELLS
        if k == 0:
            grad = saved[...] + grad
        grad = jnp.where(valid, grad, 0.0)
        value = summed[k]
        slope = total(grad * value) / (CELLS * CHANNELS)
        summed_grad = factor * grad - factor * factor * factor * value * slope
        saved[...] = summed_grad
        spread(summed_grad, bs.at[k])
        bt[:, TALL * k : TALL * k + TALL] = turned(summed_grad)
        if k == 0:
            second_taps(0, 1, 2)
            scatter.to_partner(2)
            second_taps(3, 4)
            scatter.to_partner(3)
            second_taps(5, 6)
            scatter.to_partner(4)
            scatter.near_sends(2)
            second_taps(7, 8)
            scatter.to_partner(5)
            scatter.near_sends(3)
        hidden_grad = SCALE * conv_plain(bs.at[k], second, True)
        for piece in ((4, 5), (0, 1))[k]:
            scatter.near_sends(piece)
        value = pre[k]
        sig = jax.nn.sigmoid(value)
        inner = hidden_grad * (sig * (1.0 + value * (1.0 - sig)))
        spread(jnp.where(valid, inner, 0.0), zs.at[k])
        if k == 0:
            first_taps(0, 1)
            scatter.to_partner(6)
            first_taps(2, 3)
            scatter.to_partner(7)
            first_taps(4, 5)
            scatter.to_partner(8)
            scatter.near_sends(6)
            first_taps(6, 7)
            scatter.to_partner(9)
            scatter.near_sends(7)
            first_taps(8)
            scatter.to_partner(10)
            scatter.near_sends(8)
            scatter.near_sends(9)
        carry = saved[...] + SCALE * conv_swapped(zs.at[k], first, True)
        if k == 0:
            scatter.near_sends(10)
        carry = jnp.where(valid, carry, 0.0)
        saved[...] = carry
        embed_grad[0] = embed_grad[0] + jnp.sum(jnp.where(row == spot, carry, 0.0), axis=0, keepdims=True)
        embed_grad[1] = embed_grad[1] + jnp.where(passed, 1.0, 0.0) * jnp.sum(carry, axis=0, keepdims=True)

    for e in range(2):
        lines = jnp.broadcast_to(embed_grad[e], (16, CHANNELS)).astype(BF16)
        top = lax.broadcasted_iota(jnp.int32, (16, 128), 0) == 0
        store(e, EMBED, dot(lines, jnp.where(top, ones, jnp.zeros_like(ones)), TN))
    scatter.to_partner(11)
    for piece in (0, 1, 2, 3):
        scatter.far_sends(piece)
    scatter.near_sends(11)
    for piece in (4, 5, 6, 7, 8, 9, 10):
        scatter.far_sends(piece)
    for piece in (0, 1, 2, 3):
        scatter.settle(piece)
    scatter.far_sends(11)
    for piece in (4, 5):
        scatter.settle(piece)
    scatter.along_z(0, 0, early_out, early)
    for piece in (6, 7, 8, 9, 10, 11):
        scatter.settle(piece)
    scatter.along_z(1, 12, late_out, late)
    scatter.collect(0, early)
    scatter.collect(1, late)
    with jax.named_scope("drain"):
        for copy in started:
            copy.wait_send()


def window_grads(moves, values, rewards, hidden_state, params):
    vmem = pl.BlockSpec(memory_space=pltpu.VMEM)
    smem = pl.BlockSpec(memory_space=pltpu.SMEM)
    hbm = pl.BlockSpec(memory_space=pltpu.HBM)
    dma = pltpu.SemaphoreType.DMA
    copies = pltpu.VMEM((2, 3, DEPTH, CHANNELS), BF16)
    turned = pltpu.VMEM((CHANNELS, 2 * TALL), BF16)
    field = pltpu.VMEM((ROWS, CHANNELS), F32)
    fields = pltpu.VMEM((2, ROWS, CHANNELS), F32)
    board = pltpu.VMEM((ITEMS, 4, 4, 16, 128), BF16)
    boards = pltpu.VMEM((2, ITEMS, 4, 4, 16, 128), BF16)
    early, late = (8, 32, 128), (8, 24, 128)
    return pl.pallas_call(
        window_kernel,
        out_shape=[jax.ShapeDtypeStruct(early, BF16), jax.ShapeDtypeStruct(late, BF16)],
        in_specs=[smem] * 3 + [hbm] * 5,
        out_specs=[vmem, vmem],
        scratch_shapes=[pltpu.VMEM(p.shape, F32) for p in params]
        + [
            pltpu.VMEM(hidden_state.shape, BF16),
            pltpu.VMEM((48, 128), F32),
            pltpu.VMEM((2, 8, 24, 128), BF16),
            pltpu.VMEM((2, 192, 128), F32),
            boards,
            boards,
            board,
            board,
            pltpu.VMEM((4, 12, 4, 16, 128), BF16),
            pltpu.VMEM((4, 12, 4, 16, 128), BF16),
            pltpu.VMEM((12, 4, 16, 128), BF16),
            pltpu.VMEM((12, 4, 16, 128), BF16),
            pltpu.VMEM((4, 12, 16, 128), BF16),
            pltpu.VMEM((4, 12, 16, 128), BF16),
            pltpu.VMEM((384, 128), F32),
            pltpu.VMEM(early, BF16),
            pltpu.VMEM(late, BF16),
            copies,
            copies,
            copies,
            copies,
            turned,
            turned,
            field,
            field,
            fields,
            fields,
            field,
            dma((5,)),
        ]
        + [
            dma(shape)
            for shape in (
                (2, 8), (2, 8), (3, 2, 4), (3, 2, 4), (3, 2, 4, 4), (3, 2, 4), (3, 2, 4), (3, 2, 4),
                (12,), (12,), (12, 4), (12, 4), (12, 4), (12, 4), (2, 8), (2, 8),
            )
        ],
        compiler_params=pltpu.CompilerParams(
            collective_id=0, has_side_effects=True, vmem_limit_bytes=58 << 20
        ),
        name="window",
    )(moves, values, rewards, hidden_state, *params)


def adam(param, grad, mean, square):
    mean_new = beta_one * mean + (1.0 - beta_one) * grad
    square_new = beta_two * square + (1.0 - beta_two) * grad * grad
    param_new = param - step_size * mean_new / (jnp.sqrt(square_new) + eps_adam)
    return param_new, mean_new, square_new, grad


def adam_kernel(*refs):
    given, outs, held, sem = refs[0:14], refs[14:30], refs[30:44], refs[44]
    loads = [pltpu.make_async_copy(src, dst, sem.at[k]) for k, (src, dst) in enumerate(zip(given, held))]
    for load in loads:
        load.start()
    for load in loads:
        load.wait()
    early, late = held[0:2]
    params, means, squares = held[2:6], held[6:10], held[10:14]
    new, mean_new, square_new, grads = outs[0:4], outs[4:8], outs[8:12], outs[12:16]
    totals = []
    for parts in (early, late):
        total = parts[0].astype(F32)
        for piece in range(1, 8):
            total = total + parts[piece].astype(F32)
        totals.append(total)

    def owned(item):
        if item < FIRST:
            return totals[0][2 * item : 2 * item + 2]
        return totals[1][2 * (item - 12) : 2 * (item - 12) + 2]

    for which in range(2):
        for tap in range(9):
            a, b = tap // 3, tap % 3
            grad = owned((FIRST, SECOND)[which] + tap)
            results = adam(params[which][a, b], grad, means[which][a, b], squares[which][a, b])
            for ref, result in zip((new, mean_new, square_new, grads), results):
                ref[which][a, b] = result
    head = jnp.concatenate([owned(HEAD + k) for k in range(5)], axis=1)[:, 0:BUCKETS]
    results = adam(params[2][0], head, means[2][0], squares[2][0])
    for ref, result in zip((new, mean_new, square_new, grads), results):
        ref[2][0] = result
    embed = owned(EMBED)
    embed = jnp.concatenate([embed[0:1, 0:1], embed[1:2, 0:1]], axis=1)
    results = adam(params[3][...], embed, means[3][...], squares[3][...])
    for ref, result in zip((new, mean_new, square_new, grads), results):
        ref[3][...] = result


def updates(early, late, params, means, squares):
    vmem = pl.BlockSpec(memory_space=pltpu.VMEM)
    shapes = [jax.ShapeDtypeStruct(p.shape, F32) for p in params]
    given = (early, late, *params, *means, *squares)
    return pl.pallas_call(
        adam_kernel,
        out_shape=shapes * 4,
        in_specs=[pl.BlockSpec(memory_space=pltpu.HBM)] * 14,
        out_specs=[vmem] * 16,
        scratch_shapes=[pltpu.VMEM(a.shape, a.dtype) for a in given] + [pltpu.SemaphoreType.DMA((14,))],
        compiler_params=pltpu.CompilerParams(vmem_limit_bytes=58 << 20),
        name="adam",
    )(*given)


def local(
    hidden_state,
    actions,
    value_target,
    reward_target,
    kernel_first,
    kernel_second,
    head_weight,
    action_embed,
    first_mean,
    first_square,
    second_mean,
    second_square,
    head_mean,
    head_square,
    embed_mean,
    embed_square,
):
    params = (kernel_first, kernel_second, head_weight, action_embed)
    boards = jnp.transpose(hidden_state, (1, 2, 0, 3))
    early, late = window_grads(actions, value_target, reward_target, boards, params)
    outs = updates(
        early,
        late,
        params,
        (first_mean, second_mean, head_mean, embed_mean),
        (first_square, second_square, head_square, embed_square),
    )
    new, means, squares, sums = outs[0:4], outs[4:8], outs[8:12], outs[12:16]
    moments = [moment for pair in zip(means, squares) for moment in pair]
    return (*new, *moments, *sums)


def solution(mesh):
    torus = Mesh(mesh.devices.reshape(4, 8, 4, mesh.shape["mp"]), ("dp_0", "dp_1", "dp_2", "mp"))
    kernel = P(None, None, DP, "mp")
    head = P("mp", DP, None)
    embed = P("mp", DP)
    rows = P(DP, None)
    placed = (P(DP, None, None, None), rows, rows, rows, kernel, kernel, head, embed)
    moments = (kernel, kernel, kernel, kernel, head, head, embed, embed)
    return jax.shard_map(
        local,
        mesh=torus,
        in_specs=placed + moments,
        out_specs=(kernel, kernel, head, embed) + moments + (kernel, kernel, head, embed),
        check_vma=False,
    )
```

```python
import functools

import jax
import jax.numpy as jnp
from jax import lax
from jax.experimental import pallas as pl
from jax.experimental.pallas import tpu as pltpu
from jax.sharding import Mesh
from jax.sharding import PartitionSpec as P

MESH = pl.DeviceIdType.MESH
CHANNELS = 256
DP = ("dp_0", "dp_1", "dp_2")
SIDE = 19
CELLS = 361
BUCKETS = 601
PITCH = 20
ROWS = 384
GUARD = 24
SHIFTS = tuple(PITCH * (t // 3 - 1) + t % 3 - 1 for t in range(9))
ITEMS = 24
HEAD, SECOND, FIRST, EMBED = 0, 5, 14, 23
CHUNKS = (((0, 2), (2, 3)), ((5, 5), (10, 4)), ((14, 5), (19, 5)))
PIECES = (
    (0, 0, 2, 0), (1, 2, 3, 0),
    (0, 5, 3, 2), (1, 8, 2, 3), (0, 10, 2, 5), (1, 12, 2, 5),
    (0, 14, 2, 7), (1, 16, 2, 7), (0, 18, 2, 9), (1, 20, 2, 9), (0, 22, 1, 11), (1, 23, 1, 11),
)
HALVES = (("dp_2", "dp_0"), ("dp_0", "dp_2"))
ORDER = (1, 3, 2)
SCALE = (9.0 * CHANNELS) ** (-0.5)

head_scale = 4.0
soft_cap = 15.0
eps_norm = 1e-05
beta_one = 0.9
beta_two = 0.999
step_size = 0.1
eps_adam = 1e-08

F32 = jnp.float32
BF16 = jnp.bfloat16


def scoped(method):
    @functools.wraps(method)
    def inner(self, *given):
        tag = "_".join(str(v) for v in given if isinstance(v, int))
        with jax.named_scope(f"{type(self).__name__}_{method.__name__}_{tag}"):
            return method(self, *given)

    return inner


def seats():
    return (
        lax.axis_index("dp_0"),
        lax.axis_index("dp_1"),
        lax.axis_index("dp_2"),
        lax.axis_index("mp"),
    )


def greet_all(y, z, x, c):
    barrier = pltpu.get_barrier_semaphore()
    for step in range(1, 8):
        pl.semaphore_signal(
            barrier, inc=1, device_id={"dp_1": lax.rem(z + step, 8)}, device_id_type=MESH
        )
    for step in range(1, 4):
        for name, here in (("dp_0", y), ("dp_2", x)):
            pl.semaphore_signal(
                barrier, inc=1, device_id={name: lax.rem(here + step, 4)}, device_id_type=MESH
            )
    pl.semaphore_signal(barrier, inc=1, device_id={"mp": 1 - c}, device_id_type=MESH)
    return barrier


def remote(src, dst, send, recv, peer):
    return pltpu.make_async_remote_copy(
        src_ref=src, dst_ref=dst, send_sem=send, recv_sem=recv, device_id=peer, device_id_type=MESH
    )


def arrived(ref, recv, send, peer):
    remote(ref, ref, send, recv, peer).wait_recv()


class Gather:
    def __init__(self, seat, w, stage, wide, sems, started):
        self.y, self.z, self.x, self.c = seat
        self.here = {"dp_0": self.y, "dp_2": self.x}
        self.w, self.stage, self.wide, self.started = w, stage, wide, started
        self.z_send, self.z_recv, self.p_send, self.p_recv = sems[0:4]
        self.q_send, self.q_recv, self.m_send, self.m_recv = sems[4:8]
        self.partner = {"mp": 1 - self.c}

    def launch(self, copy):
        copy.start()
        self.started.append(copy)

    def tile(self, chunk, half, near, far):
        items = pl.ds(*CHUNKS[chunk][half])
        if half == 0:
            return self.w.at[self.c, items, far, near]
        return self.w.at[self.c, items, near, far]

    def slab(self, chunk, half, far, core):
        items = pl.ds(*CHUNKS[chunk][half])
        if half == 0:
            return self.w.at[core, items, far]
        return self.w.at[core, items, :, far]

    @scoped
    def along_z(self):
        z = self.z
        for group in (1, 0):
            ref = self.stage.at[group, z]
            for step in range(1, 8):
                peer = {"dp_1": lax.rem(z + step, 8)}
                self.launch(remote(ref, ref, self.z_send.at[group, step], self.z_recv.at[group, z], peer))

    @scoped
    def unpack(self, group):
        for step in range(1, 8):
            peer = lax.rem(self.z + step, 8)
            sems = self.z_recv.at[group, peer], self.z_send.at[group, 0]
            arrived(self.stage.at[group, peer], *sems, {"dp_1": peer})
        for piece in range(8):
            self.wide[group, 24 * piece : 24 * piece + 24, :] = self.stage[group, piece].astype(F32)

    def to_far(self, chunk, half, turn, near):
        far = HALVES[half][1]
        at = self.here[far]
        ref = self.tile(chunk, half, near, at)
        for step in ORDER:
            self.launch(
                remote(
                    ref, ref, self.q_send.at[chunk, half, turn, step], self.q_recv.at[chunk, half, at],
                    {far: lax.rem(at + step, 4)},
                )
            )

    @scoped
    def near_sends(self, chunk):
        for half, (near, far) in enumerate(HALVES):
            start, count = CHUNKS[chunk][half]
            for item in range(start, start + count):
                group, line = item // 12, 2 * (item % 12)
                slab = self.wide.at[group]
                low = slab[pl.ds(line, 8, stride=24), :]
                high = slab[pl.ds(line + 1, 8, stride=24), :]
                self.w[self.c, item, self.y, self.x] = jnp.concatenate([low, high], axis=0).astype(BF16)
        for step in ORDER:
            for half, (near, far) in enumerate(HALVES):
                at = self.here[near]
                ref = self.tile(chunk, half, at, self.here[far])
                self.launch(
                    remote(
                        ref, ref, self.p_send.at[chunk, half, step], self.p_recv.at[chunk, half, at],
                        {near: lax.rem(at + step, 4)},
                    )
                )

    def own_sends(self, chunk):
        for half, (near, far) in enumerate(HALVES):
            self.to_far(chunk, half, 0, self.here[near])

    def to_partner(self, chunk, half, turn, ref):
        sems = self.m_send.at[chunk, half, turn], self.m_recv.at[chunk, half, turn]
        self.launch(remote(ref, ref, *sems, self.partner))

    @scoped
    def far_sends(self, chunk):
        for step in ORDER:
            for half, (near, far) in enumerate(HALVES):
                peer = lax.rem(self.here[near] + step, 4)
                ref = self.tile(chunk, half, peer, self.here[far])
                arrived(ref, self.p_recv.at[chunk, half, peer], self.p_send.at[chunk, half, 0], {near: peer})
                self.to_far(chunk, half, step, peer)
        for half, (near, far) in enumerate(HALVES):
            self.to_partner(chunk, half, 0, self.slab(chunk, half, self.here[far], self.c))

    @scoped
    def cross(self, chunk):
        for step in ORDER:
            for half, (near, far) in enumerate(HALVES):
                peer = lax.rem(self.here[far] + step, 4)
                ref = self.slab(chunk, half, peer, self.c)
                arrived(ref, self.q_recv.at[chunk, half, peer], self.q_send.at[chunk, half, 0, 0], {far: peer})
                self.to_partner(chunk, half, step, ref)

    @scoped
    def join(self, chunk):
        for half, (near, far) in enumerate(HALVES):
            for turn in range(4):
                ref = self.slab(chunk, half, lax.rem(self.here[far] + turn, 4), 1 - self.c)
                sems = self.m_recv.at[chunk, half, turn], self.m_send.at[chunk, half, turn]
                arrived(ref, *sems, self.partner)


class Scatter:
    def __init__(self, seat, g, buffers, sems, started):
        self.y, self.z, self.x, self.c = seat
        self.here = {"dp_0": self.y, "dp_2": self.x}
        self.g, self.started = g, started
        self.inbox, self.sums, a_in, b_in, a_sum, b_sum, a_last, b_last, self.flat = buffers
        self.arrivals, self.folded, self.last = (a_in, b_in), (a_sum, b_sum), (a_last, b_last)
        self.m_send, self.m_recv, self.p_send, self.p_recv = sems[0:4]
        self.q_send, self.q_recv, self.z_send, self.z_recv = sems[4:8]
        self.partner = {"mp": 1 - self.c}

    def launch(self, copy):
        copy.start()
        self.started.append(copy)

    def across(self, piece):
        half, start, count, _ = PIECES[piece]
        items = pl.ds(start, count)
        return remote(
            self.g.at[1 - self.c, items], self.inbox.at[items], self.m_send.at[piece], self.m_recv.at[piece],
            self.partner,
        )

    def to_partner(self, piece):
        self.launch(self.across(piece))

    @scoped
    def near_sends(self, piece):
        half, start, count, at = PIECES[piece]
        near, far = HALVES[half]
        self.across(piece).wait_recv()
        for item in range(start, start + count):
            total = self.g[self.c, item].astype(F32) + self.inbox[item].astype(F32)
            self.sums[item] = total.astype(BF16)
        items = pl.ds(start, count)
        for step in ORDER:
            peer = lax.rem(self.here[near] + step, 4)
            ref = self.sums.at[items, :, peer] if half == 0 else self.sums.at[items, peer]
            self.launch(
                remote(
                    ref, self.arrivals[half].at[self.here[near], pl.ds(at, count)], self.p_send.at[piece, step],
                    self.p_recv.at[piece, self.here[near]], {near: peer},
                )
            )

    @scoped
    def far_sends(self, piece):
        half, start, count, at = PIECES[piece]
        near, far = HALVES[half]
        peers = [lax.rem(self.here[near] + step, 4) for step in ORDER]
        box, total_of = self.arrivals[half], self.folded[half]
        for peer in peers:
            ref = box.at[peer, pl.ds(at, count)]
            arrived(ref, self.p_recv.at[piece, peer], self.p_send.at[piece, 0], {near: peer})
        for item in range(count):
            own = self.sums[start + item, :, self.x] if half == 0 else self.sums[start + item, self.y]
            total = own.astype(F32)
            for peer in peers:
                total = total + box[peer, at + item].astype(F32)
            total_of[at + item] = total.astype(BF16)
        for step in ORDER:
            peer = lax.rem(self.here[far] + step, 4)
            self.launch(
                remote(
                    total_of.at[pl.ds(at, count), peer], self.last[half].at[self.here[far], pl.ds(at, count)],
                    self.q_send.at[piece, step], self.q_recv.at[piece, self.here[far]], {far: peer},
                )
            )

    @scoped
    def settle(self, piece):
        half, start, count, at = PIECES[piece]
        near, far = HALVES[half]
        peers = [lax.rem(self.here[far] + step, 4) for step in ORDER]
        box, total_of = self.last[half], self.folded[half]
        for peer in peers:
            ref = box.at[peer, pl.ds(at, count)]
            arrived(ref, self.q_recv.at[piece, peer], self.q_send.at[piece, 0], {far: peer})
        for item in range(count):
            total = total_of[at + item, self.here[far]].astype(F32)
            for peer in peers:
                total = total + box[peer, at + item].astype(F32)
            self.flat[16 * (start + item) : 16 * (start + item) + 16, :] = total

    @scoped
    def along_z(self, turn, item, letters, out):
        rows = letters.shape[1]
        for spot in range(8):
            letters[spot] = self.flat[pl.ds(16 * item + spot, rows, stride=8), :].astype(BF16)
        for step in range(1, 8):
            peer = lax.rem(self.z + step, 8)
            self.launch(
                remote(
                    letters.at[peer], out.at[self.z], self.z_send.at[turn, step], self.z_recv.at[turn, self.z],
                    {"dp_1": peer},
                )
            )
        out[self.z] = letters[self.z]

    @scoped
    def collect(self, turn, out):
        for step in range(1, 8):
            peer = lax.rem(self.z + step, 8)
            arrived(out.at[peer], self.z_recv.at[turn, peer], self.z_send.at[turn, 0], {"dp_1": peer})


NN = (((1,), (0,)), ((), ()))
NT = (((1,), (1,)), ((), ()))
TN = (((0,), (0,)), ((), ()))


def dot(a, b, dims=NN):
    return lax.dot_general(a, b, dims, preferred_element_type=F32)


def window_kernel(
    moves_in, values_in, rewards_in, hidden_in, first_in, second_in, head_in, embed_in, early, late,
    first_v, second_v, head_v, embed_v, hidden_v, rows, stage, wide, w, g,
    inbox, sums, a_in, b_in, a_sum, b_sum, a_last, b_last, flat, early_out, late_out,
    xs, hs, bs, zs, xt, bt, state, mixed, pre, summed, saved, slabs, first_t, second_t, moves, values, rewards, local_sem, *sems,
):
    seat = y, z, x, c = seats()
    barrier = greet_all(y, z, x, c)
    pairs = (
        (first_in, first_v), (second_in, second_v), (head_in, head_v), (embed_in, embed_v), (hidden_in, hidden_v),
        (moves_in, moves), (values_in, values), (rewards_in, rewards),
    )
    loads = [pltpu.make_async_copy(src, dst, local_sem.at[k]) for k, (src, dst) in enumerate(pairs)]
    for load in loads:
        load.start()
    started, sent = [], []
    gather = Gather(seat, w, stage, wide, sems[0:8], sent)
    scatter = Scatter(
        seat, g, (inbox, sums, a_in, b_in, a_sum, b_sum, a_last, b_last, flat), sems[8:16], started
    )
    rows[2 * HEAD : 2 * SECOND, :] = jnp.zeros((10, 128), F32)
    for load in loads[0:4]:
        load.wait()
    for tap in range(9):
        at = 2 * (SECOND + tap)
        rows[at : at + 2, :] = second_v[tap // 3, tap % 3]
        at = 2 * (FIRST + tap)
        rows[at : at + 2, :] = first_v[tap // 3, tap % 3]
    for block in range(5):
        width = min(128, BUCKETS - 128 * block)
        at = 2 * (HEAD + block)
        rows[at : at + 2, 0:width] = head_v[0, :, 128 * block : 128 * block + width]
    for r in range(2):
        at = 2 * EMBED + r
        rows[at : at + 1, :] = jnp.broadcast_to(embed_v[:, r : r + 1], (1, 128))
    for group in range(2):
        stage[group, z] = rows[24 * group : 24 * group + 24, :].astype(BF16)
    with jax.named_scope("barrier"):
        pl.semaphore_wait(barrier, 14)
    gather.along_z()

    def phase(run):
        def inner(*given):
            with jax.named_scope(run.__name__):
                return run(*given)

        return inner

    row = lax.broadcasted_iota(jnp.int32, (ROWS, CHANNELS), 0)
    valid = (lax.rem(row, PITCH) < SIDE) & (row < PITCH * SIDE)

    def whole(h, item):
        return w[h, item].reshape(CHANNELS, 128)

    def first(tap):
        return jnp.concatenate([whole(0, FIRST + tap), whole(1, FIRST + tap)], axis=1)

    def second(tap):
        return jnp.concatenate([whole(0, SECOND + tap), whole(1, SECOND + tap)], axis=1)

    def head(h):
        return jnp.concatenate([whole(h, HEAD + k) for k in range(5)], axis=1)

    def halves(lhs, rhs):
        cut = ROWS // 2
        return jnp.concatenate([dot(lhs[:cut], rhs), dot(lhs[cut:], rhs)], axis=0)

    @phase
    def transposes(dest, kernel, flip):
        for tap in range(9):
            turn = kernel(8 - tap if flip else tap).astype(F32).T
            dest[CHANNELS * tap : CHANNELS * tap + CHANNELS, :] = turn.astype(BF16)

    def taps_of(field):
        return jnp.concatenate([field[t] for t in range(9)], axis=1)

    @phase
    def conv_first(field):
        return halves(taps_of(field), jnp.concatenate([first(t) for t in range(9)], axis=0))

    @phase
    def conv_second(field):
        return halves(taps_of(field), second_t[...])

    @phase
    def back_second(field):
        return halves(taps_of(field), jnp.concatenate([second(8 - t) for t in range(9)], axis=0))

    @phase
    def back_first(field):
        return halves(taps_of(field), first_t[...])

    @phase
    def spread(value, dest):
        for h in range(2):
            lanes = slice(128 * h, 128 * h + 128)
            slabs[h, GUARD : GUARD + ROWS, :] = value[:, lanes]
            for t in range(9):
                start = GUARD + SHIFTS[t]
                dest[t, :, lanes] = slabs[h, start : start + ROWS, :].astype(BF16)

    @phase
    def turned(value):
        return value.T.astype(BF16)

    def total(value):
        return jnp.sum(jnp.sum(value, axis=0, keepdims=True), axis=1, keepdims=True)

    def store(h, item, value):
        g[h, item] = value.astype(BF16).reshape(4, 4, 16, 128)

    for h in range(2):
        slabs[h, 0:GUARD, :] = jnp.zeros((GUARD, 128), F32)
        slabs[h, GUARD + ROWS :, :] = jnp.zeros((GUARD, 128), F32)
    flat[16 * FIRST : 16 * FIRST + 32, :] = jnp.zeros((32, 128), F32)

    state[...] = jnp.zeros((ROWS, CHANNELS), F32)
    for load in loads[4:8]:
        load.wait()

    with jax.named_scope("place"):
        for line in range(SIDE):
            cells = hidden_v[line].astype(F32)
            mine = jnp.where(c == 0, cells[:, 0, :], cells[:, 1, :])
            state[PITCH * line : PITCH * line + SIDE, :] = mine
    lane = lax.broadcasted_iota(jnp.int32, (CHANNELS, CHANNELS), 1)
    natural = 64 * (lane // 64) + 8 * (lane % 8) + 2 * ((lane // 16) % 4) + (lane // 8) % 2
    source = lax.broadcasted_iota(jnp.int32, (CHANNELS, CHANNELS), 0)
    permute = jnp.where(source == natural, 1.0, 0.0).astype(BF16)
    state[...] = dot(state[...].astype(BF16), permute)

    gather.unpack(1)
    gather.near_sends(2)
    gather.own_sends(2)
    gather.unpack(0)
    gather.near_sends(1)
    gather.own_sends(1)
    gather.near_sends(0)
    gather.far_sends(2)
    gather.far_sends(1)
    gather.own_sends(0)
    gather.far_sends(0)
    gather.cross(2)
    gather.join(2)

    ones = jnp.ones((16, 128), BF16)
    pick = lax.broadcasted_iota(jnp.int32, (16, 128), 1) == 0
    pick = jnp.where(pick, ones, jnp.zeros_like(ones))
    embed = [dot(pick, whole(e, EMBED), NT)[0:1, :] for e in range(2)]

    kept = []
    pooled_rows = jnp.zeros((16, CHANNELS), F32)
    for k in range(2):
        move = moves[c, k]
        spot = PITCH * lax.div(move, SIDE) + lax.rem(move, SIDE)
        passed = move == CELLS
        added = jnp.where(row == spot, embed[0], 0.0) + jnp.where(passed, 1.0, 0.0) * embed[1]
        now = jnp.where(valid, state[...] + added, 0.0)
        mixed[...] = now
        if k == 1:
            gather.cross(0)
        spread(now, xs.at[k])
        value = SCALE * conv_first(xs.at[k])
        pre[k] = value
        spread(jnp.where(valid, value * jax.nn.sigmoid(value), 0.0), hs.at[k])
        if k == 0:
            gather.cross(1)
        xt[:, ROWS * k : ROWS * k + ROWS] = turned(mixed[...])
        if k == 0:
            transposes(first_t, first, True)
            gather.join(1)
            transposes(second_t, second, False)
        branch = conv_second(hs.at[k])
        value = jnp.where(valid, mixed[...] + SCALE * branch, 0.0)
        summed[k] = value
        factor = lax.rsqrt(total(value * value) / (CELLS * CHANNELS) + eps_norm)
        value = value * factor
        state[...] = value
        pooled = jnp.sum(value, axis=0, keepdims=True) / CELLS
        own_row = lax.broadcasted_iota(jnp.int32, (16, CHANNELS), 0) == k
        pooled_rows = jnp.where(own_row, pooled, pooled_rows)
        kept.append((spot, passed, factor))
    gather.join(0)

    bucket = lax.broadcasted_iota(jnp.int32, (16, 640), 1)
    top_row = lax.broadcasted_iota(jnp.int32, (16, 640), 0) == 0
    pooled = pooled_rows.astype(BF16)
    pooled_grads = jnp.zeros((16, CHANNELS), F32)
    logits = []
    for h, targets in enumerate((values, rewards)):
        raw = head_scale * dot(pooled, head(h))
        squashed = jnp.tanh(raw / soft_cap)
        raised = jnp.where(bucket < BUCKETS, jnp.exp(soft_cap * squashed), 0.0)
        chances = raised / jnp.sum(raised, axis=1, keepdims=True)
        picked = jnp.where(bucket == jnp.where(top_row, targets[c, 0], targets[c, 1]), 1.0, 0.0)
        logit = (chances - picked) * (1.0 - squashed * squashed) / 256.0
        logit = jnp.where(bucket < BUCKETS, logit, 0.0).astype(BF16)
        pooled_grads = pooled_grads + dot(logit, head(h), NT)
        logits.append(logit)
    for h in range(2):
        grad = head_scale * dot(pooled, logits[h], TN)
        for block in range(5):
            store(h, HEAD + block, grad[:, 128 * block : 128 * block + 128])
    for piece in (0, 1):
        scatter.to_partner(piece)

    def window(field, tap):
        return jnp.concatenate([field[k, tap] for k in range(2)], axis=0)

    def second_taps(*taps):
        with jax.named_scope("second_taps"):
            for tap in taps:
                grad = SCALE * dot(bt[...], window(hs, tap))
                store(0, SECOND + tap, grad[:, 0:128])
                store(1, SECOND + tap, grad[:, 128:256])

    def first_taps(*taps):
        with jax.named_scope("first_taps"):
            for tap in taps:
                grad = SCALE * dot(xt[...], window(zs, 8 - tap))
                store(0, FIRST + tap, grad[:, 0:128])
                store(1, FIRST + tap, grad[:, 128:256])

    embed_grad = [jnp.zeros((1, CHANNELS), F32) for _ in range(2)]
    for k in (1, 0):
        spot, passed, factor = kept[k]
        grad = head_scale * pooled_grads[k : k + 1, :] / CELLS
        if k == 0:
            grad = saved[...] + grad
        grad = jnp.where(valid, grad, 0.0)
        value = summed[k]
        slope = total(grad * value) / (CELLS * CHANNELS)
        summed_grad = factor * grad - factor * factor * factor * value * slope
        saved[...] = summed_grad
        spread(summed_grad, bs.at[k])
        bt[:, ROWS * k : ROWS * k + ROWS] = turned(summed_grad)
        if k == 0:
            second_taps(0, 1, 2)
            scatter.to_partner(2)
            second_taps(3, 4)
            scatter.to_partner(3)
            second_taps(5, 6)
            scatter.to_partner(4)
            second_taps(7, 8)
            scatter.to_partner(5)
            scatter.near_sends(2)
            scatter.near_sends(3)
        hidden_grad = SCALE * back_second(bs.at[k])
        if k == 0:
            scatter.near_sends(4)
        value = pre[k]
        sig = jax.nn.sigmoid(value)
        inner = hidden_grad * (sig * (1.0 + value * (1.0 - sig)))
        spread(jnp.where(valid, inner, 0.0), zs.at[k])
        for piece in ((5,), (0, 1))[k]:
            scatter.near_sends(piece)
        if k == 0:
            first_taps(0, 1)
            scatter.to_partner(6)
            first_taps(2, 3)
            scatter.to_partner(7)
            for piece in (0, 1):
                scatter.far_sends(piece)
        carry = saved[...] + SCALE * back_first(zs.at[k])
        if k == 0:
            scatter.near_sends(6)
            scatter.near_sends(7)
        carry = jnp.where(valid, carry, 0.0)
        saved[...] = carry
        embed_grad[0] = embed_grad[0] + jnp.sum(jnp.where(row == spot, carry, 0.0), axis=0, keepdims=True)
        embed_grad[1] = embed_grad[1] + jnp.where(passed, 1.0, 0.0) * jnp.sum(carry, axis=0, keepdims=True)

    for e in range(2):
        lines = jnp.broadcast_to(embed_grad[e], (16, CHANNELS)).astype(BF16)
        top = lax.broadcasted_iota(jnp.int32, (16, 128), 0) == 0
        store(e, EMBED, dot(lines, jnp.where(top, ones, jnp.zeros_like(ones)), TN))
    scatter.to_partner(11)
    first_taps(4, 5)
    scatter.to_partner(8)
    first_taps(6, 7)
    scatter.to_partner(9)
    first_taps(8)
    scatter.to_partner(10)
    for piece in (8, 11, 9, 10):
        scatter.near_sends(piece)
    for piece in (2, 3, 4, 5, 6, 7):
        scatter.far_sends(piece)
    for copy in sent:
        copy.wait_send()
    for piece in (8, 9, 11):
        scatter.far_sends(piece)
    for piece in (0, 1):
        scatter.settle(piece)
    scatter.far_sends(10)
    for piece in (2, 3, 4, 5):
        scatter.settle(piece)
    scatter.along_z(0, 0, early_out, early)
    for piece in (6, 7, 8, 9, 10, 11):
        scatter.settle(piece)
    scatter.along_z(1, 12, late_out, late)
    scatter.collect(0, early)
    scatter.collect(1, late)
    with jax.named_scope("drain"):
        for copy in started:
            copy.wait_send()


def window_grads(moves, values, rewards, hidden_state, params):
    vmem = pl.BlockSpec(memory_space=pltpu.VMEM)
    hbm = pl.BlockSpec(memory_space=pltpu.HBM)
    dma = pltpu.SemaphoreType.DMA
    copies = pltpu.VMEM((2, 9, ROWS, CHANNELS), BF16)
    turned = pltpu.VMEM((CHANNELS, 2 * ROWS), BF16)
    field = pltpu.VMEM((ROWS, CHANNELS), F32)
    fields = pltpu.VMEM((2, ROWS, CHANNELS), F32)
    board = pltpu.VMEM((ITEMS, 4, 4, 16, 128), BF16)
    boards = pltpu.VMEM((2, ITEMS, 4, 4, 16, 128), BF16)
    early, late = (8, 32, 128), (8, 24, 128)
    return pl.pallas_call(
        window_kernel,
        out_shape=[jax.ShapeDtypeStruct(early, BF16), jax.ShapeDtypeStruct(late, BF16)],
        in_specs=[hbm] * 8,
        out_specs=[vmem, vmem],
        scratch_shapes=[pltpu.VMEM(p.shape, F32) for p in params]
        + [
            pltpu.VMEM(hidden_state.shape, BF16),
            pltpu.VMEM((48, 128), F32),
            pltpu.VMEM((2, 8, 24, 128), BF16),
            pltpu.VMEM((2, 192, 128), F32),
            boards,
            boards,
            board,
            board,
            pltpu.VMEM((4, 12, 4, 16, 128), BF16),
            pltpu.VMEM((4, 12, 4, 16, 128), BF16),
            pltpu.VMEM((12, 4, 16, 128), BF16),
            pltpu.VMEM((12, 4, 16, 128), BF16),
            pltpu.VMEM((4, 12, 16, 128), BF16),
            pltpu.VMEM((4, 12, 16, 128), BF16),
            pltpu.VMEM((384, 128), F32),
            pltpu.VMEM(early, BF16),
            pltpu.VMEM(late, BF16),
            copies,
            copies,
            copies,
            copies,
            turned,
            turned,
            field,
            field,
            fields,
            fields,
            field,
            pltpu.VMEM((2, ROWS + 2 * GUARD, 128), F32),
            pltpu.VMEM((9 * CHANNELS, CHANNELS), BF16),
            pltpu.VMEM((9 * CHANNELS, CHANNELS), BF16),
            pltpu.SMEM((2, 2), jnp.int32),
            pltpu.SMEM((2, 2), jnp.int32),
            pltpu.SMEM((2, 2), jnp.int32),
            dma((8,)),
        ]
        + [
            dma(shape)
            for shape in (
                (2, 8), (2, 8), (3, 2, 4), (3, 2, 4), (3, 2, 4, 4), (3, 2, 4), (3, 2, 4), (3, 2, 4),
                (12,), (12,), (12, 4), (12, 4), (12, 4), (12, 4), (2, 8), (2, 8),
            )
        ],
        compiler_params=pltpu.CompilerParams(
            collective_id=0, has_side_effects=True, vmem_limit_bytes=58 << 20
        ),
        name="window",
    )(moves, values, rewards, hidden_state, *params)


def adam(param, grad, mean, square):
    mean_new = beta_one * mean + (1.0 - beta_one) * grad
    square_new = beta_two * square + (1.0 - beta_two) * grad * grad
    param_new = param - step_size * mean_new / (jnp.sqrt(square_new) + eps_adam)
    return param_new, mean_new, square_new, grad


def adam_kernel(*refs):
    given, outs, held, sem = refs[0:14], refs[14:30], refs[30:44], refs[44]
    loads = [pltpu.make_async_copy(src, dst, sem.at[k]) for k, (src, dst) in enumerate(zip(given, held))]
    for load in loads:
        load.start()
    for load in loads:
        load.wait()
    early, late = held[0:2]
    params, means, squares = held[2:6], held[6:10], held[10:14]
    new, mean_new, square_new, grads = outs[0:4], outs[4:8], outs[8:12], outs[12:16]
    totals = []
    for parts in (early, late):
        total = parts[0].astype(F32)
        for piece in range(1, 8):
            total = total + parts[piece].astype(F32)
        totals.append(total)

    def owned(item):
        if item < FIRST:
            return totals[0][2 * item : 2 * item + 2]
        return totals[1][2 * (item - 12) : 2 * (item - 12) + 2]

    for which in range(2):
        for tap in range(9):
            a, b = tap // 3, tap % 3
            grad = owned((FIRST, SECOND)[which] + tap)
            results = adam(params[which][a, b], grad, means[which][a, b], squares[which][a, b])
            for ref, result in zip((new, mean_new, square_new, grads), results):
                ref[which][a, b] = result
    head = jnp.concatenate([owned(HEAD + k) for k in range(5)], axis=1)[:, 0:BUCKETS]
    results = adam(params[2][0], head, means[2][0], squares[2][0])
    for ref, result in zip((new, mean_new, square_new, grads), results):
        ref[2][0] = result
    embed = owned(EMBED)
    embed = jnp.concatenate([embed[0:1, 0:1], embed[1:2, 0:1]], axis=1)
    results = adam(params[3][...], embed, means[3][...], squares[3][...])
    for ref, result in zip((new, mean_new, square_new, grads), results):
        ref[3][...] = result


def updates(early, late, params, means, squares):
    vmem = pl.BlockSpec(memory_space=pltpu.VMEM)
    shapes = [jax.ShapeDtypeStruct(p.shape, F32) for p in params]
    given = (early, late, *params, *means, *squares)
    return pl.pallas_call(
        adam_kernel,
        out_shape=shapes * 4,
        in_specs=[pl.BlockSpec(memory_space=pltpu.HBM)] * 14,
        out_specs=[vmem] * 16,
        scratch_shapes=[pltpu.VMEM(a.shape, a.dtype) for a in given] + [pltpu.SemaphoreType.DMA((14,))],
        compiler_params=pltpu.CompilerParams(vmem_limit_bytes=58 << 20),
        name="adam",
    )(*given)


def local(
    hidden_state,
    actions,
    value_target,
    reward_target,
    kernel_first,
    kernel_second,
    head_weight,
    action_embed,
    first_mean,
    first_square,
    second_mean,
    second_square,
    head_mean,
    head_square,
    embed_mean,
    embed_square,
):
    params = (kernel_first, kernel_second, head_weight, action_embed)
    boards = jnp.transpose(hidden_state, (1, 2, 0, 3))
    early, late = window_grads(actions, value_target, reward_target, boards, params)
    outs = updates(
        early,
        late,
        params,
        (first_mean, second_mean, head_mean, embed_mean),
        (first_square, second_square, head_square, embed_square),
    )
    new, means, squares, sums = outs[0:4], outs[4:8], outs[8:12], outs[12:16]
    moments = [moment for pair in zip(means, squares) for moment in pair]
    return (*new, *moments, *sums)


def solution(mesh):
    torus = Mesh(mesh.devices.reshape(4, 8, 4, mesh.shape["mp"]), ("dp_0", "dp_1", "dp_2", "mp"))
    kernel = P(None, None, DP, "mp")
    head = P("mp", DP, None)
    embed = P("mp", DP)
    rows = P(DP, None)
    placed = (P(DP, None, None, None), rows, rows, rows, kernel, kernel, head, embed)
    moments = (kernel, kernel, kernel, kernel, head, head, embed, embed)
    return jax.shard_map(
        local,
        mesh=torus,
        in_specs=placed + moments,
        out_specs=(kernel, kernel, head, embed) + moments + (kernel, kernel, head, embed),
        check_vma=False,
    )
```

```python
import functools

import jax
import jax.numpy as jnp
from jax import lax
from jax.experimental import pallas as pl
from jax.experimental.pallas import tpu as pltpu
from jax.sharding import Mesh
from jax.sharding import PartitionSpec as P

MESH = pl.DeviceIdType.MESH
CHANNELS = 256
DP = ("dp_0", "dp_1", "dp_2")
SIDE = 19
CELLS = 361
BUCKETS = 601
PITCH = 20
ROWS = 384
GUARD = 24
SHIFTS = tuple(PITCH * (t // 3 - 1) + t % 3 - 1 for t in range(9))
ITEMS = 23
HEAD, SECOND, FIRST, MIX = 0, 4, 13, 22
SPLIT = 11
CHUNKS = ({0: (0, 2), 1: (2, 2)}, {0: (4, 5), 1: (9, 4)}, {0: (13, 4), 1: (17, 5)}, {0: (22, 1)})
PIECES = (
    (0, 0, 2, 0), (1, 2, 2, 0),
    (0, 4, 1, 2), (1, 5, 2, 2), (0, 7, 2, 3), (1, 9, 2, 4), (0, 11, 2, 5),
    (1, 13, 2, 6), (0, 15, 2, 7), (1, 17, 2, 8), (0, 19, 2, 9), (1, 21, 1, 10), (0, 22, 1, 11),
)
HALVES = (("dp_2", "dp_0"), ("dp_0", "dp_2"))
ORDER = (1, 3, 2)
SCALE = (9.0 * CHANNELS) ** (-0.5)

head_scale = 4.0
soft_cap = 15.0
eps_norm = 1e-05
beta_one = 0.9
beta_two = 0.999
step_size = 0.1
eps_adam = 1e-08

F32 = jnp.float32
BF16 = jnp.bfloat16


def scoped(method):
    @functools.wraps(method)
    def inner(self, *given):
        tag = "_".join(str(v) for v in given if isinstance(v, int))
        with jax.named_scope(f"{type(self).__name__}_{method.__name__}_{tag}"):
            return method(self, *given)

    return inner


def seats():
    return (
        lax.axis_index("dp_0"),
        lax.axis_index("dp_1"),
        lax.axis_index("dp_2"),
        lax.axis_index("mp"),
    )


def greet_all(y, z, x, c):
    barrier = pltpu.get_barrier_semaphore()
    for step in range(1, 8):
        pl.semaphore_signal(
            barrier, inc=1, device_id={"dp_1": lax.rem(z + step, 8)}, device_id_type=MESH
        )
    for step in range(1, 4):
        for name, here in (("dp_0", y), ("dp_2", x)):
            pl.semaphore_signal(
                barrier, inc=1, device_id={name: lax.rem(here + step, 4)}, device_id_type=MESH
            )
    pl.semaphore_signal(barrier, inc=1, device_id={"mp": 1 - c}, device_id_type=MESH)
    return barrier


def remote(src, dst, send, recv, peer):
    return pltpu.make_async_remote_copy(
        src_ref=src, dst_ref=dst, send_sem=send, recv_sem=recv, device_id=peer, device_id_type=MESH
    )


def arrived(ref, recv, send, peer):
    remote(ref, ref, send, recv, peer).wait_recv()


def halves_of(chunk):
    return [(half, *HALVES[half]) for half in CHUNKS[chunk]]


class Gather:
    def __init__(self, seat, w, stage, wide, sems, started):
        self.y, self.z, self.x, self.c = seat
        self.here = {"dp_0": self.y, "dp_2": self.x}
        self.w, self.stage, self.wide, self.started = w, stage, wide, started
        self.z_send, self.z_recv, self.p_send, self.p_recv = sems[0:4]
        self.q_send, self.q_recv, self.m_send, self.m_recv = sems[4:8]
        self.partner = {"mp": 1 - self.c}

    def launch(self, copy):
        copy.start()
        self.started.append(copy)

    def tile(self, chunk, half, near, far):
        items = pl.ds(*CHUNKS[chunk][half])
        if half == 0:
            return self.w.at[self.c, items, far, near]
        return self.w.at[self.c, items, near, far]

    def slab(self, chunk, half, far, core):
        items = pl.ds(*CHUNKS[chunk][half])
        if half == 0:
            return self.w.at[core, items, far]
        return self.w.at[core, items, :, far]

    @scoped
    def along_z(self):
        z = self.z
        for group in (1, 0):
            ref = self.stage.at[group, z]
            for step in range(1, 8):
                peer = {"dp_1": lax.rem(z + step, 8)}
                self.launch(remote(ref, ref, self.z_send.at[group, step], self.z_recv.at[group, z], peer))

    @scoped
    def unpack(self, group):
        for step in range(1, 8):
            peer = lax.rem(self.z + step, 8)
            sems = self.z_recv.at[group, peer], self.z_send.at[group, 0]
            arrived(self.stage.at[group, peer], *sems, {"dp_1": peer})
        for piece in range(8):
            self.wide[group, 24 * piece : 24 * piece + 24, :] = self.stage[group, piece].astype(F32)

    def to_far(self, chunk, half, turn, near):
        far = HALVES[half][1]
        at = self.here[far]
        ref = self.tile(chunk, half, near, at)
        for step in ORDER:
            self.launch(
                remote(
                    ref, ref, self.q_send.at[chunk, half, turn, step], self.q_recv.at[chunk, half, at],
                    {far: lax.rem(at + step, 4)},
                )
            )

    @scoped
    def near_sends(self, chunk):
        for half, near, far in halves_of(chunk):
            start, count = CHUNKS[chunk][half]
            for item in range(start, start + count):
                group = int(item >= SPLIT)
                line = 2 * (item - SPLIT * group)
                slab = self.wide.at[group]
                low = slab[pl.ds(line, 8, stride=24), :]
                high = slab[pl.ds(line + 1, 8, stride=24), :]
                self.w[self.c, item, self.y, self.x] = jnp.concatenate([low, high], axis=0).astype(BF16)
        for step in ORDER:
            for half, near, far in halves_of(chunk):
                at = self.here[near]
                ref = self.tile(chunk, half, at, self.here[far])
                self.launch(
                    remote(
                        ref, ref, self.p_send.at[chunk, half, step], self.p_recv.at[chunk, half, at],
                        {near: lax.rem(at + step, 4)},
                    )
                )

    def own_sends(self, chunk):
        for half, near, far in halves_of(chunk):
            self.to_far(chunk, half, 0, self.here[near])

    def to_partner(self, chunk, half, turn, ref):
        sems = self.m_send.at[chunk, half, turn], self.m_recv.at[chunk, half, turn]
        self.launch(remote(ref, ref, *sems, self.partner))

    @scoped
    def far_sends(self, chunk):
        for step in ORDER:
            for half, near, far in halves_of(chunk):
                peer = lax.rem(self.here[near] + step, 4)
                ref = self.tile(chunk, half, peer, self.here[far])
                arrived(ref, self.p_recv.at[chunk, half, peer], self.p_send.at[chunk, half, 0], {near: peer})
                self.to_far(chunk, half, step, peer)
        for half, near, far in halves_of(chunk):
            self.to_partner(chunk, half, 0, self.slab(chunk, half, self.here[far], self.c))

    @scoped
    def cross(self, chunk):
        for step in ORDER:
            for half, near, far in halves_of(chunk):
                peer = lax.rem(self.here[far] + step, 4)
                ref = self.slab(chunk, half, peer, self.c)
                arrived(ref, self.q_recv.at[chunk, half, peer], self.q_send.at[chunk, half, 0, 0], {far: peer})
                self.to_partner(chunk, half, step, ref)

    @scoped
    def join(self, chunk):
        for half, near, far in halves_of(chunk):
            for turn in range(4):
                ref = self.slab(chunk, half, lax.rem(self.here[far] + turn, 4), 1 - self.c)
                sems = self.m_recv.at[chunk, half, turn], self.m_send.at[chunk, half, turn]
                arrived(ref, *sems, self.partner)


class Scatter:
    def __init__(self, seat, g, buffers, sems, started):
        self.y, self.z, self.x, self.c = seat
        self.here = {"dp_0": self.y, "dp_2": self.x}
        self.g, self.started = g, started
        self.inbox, self.sums, a_in, b_in, a_sum, b_sum, a_last, b_last, self.flat = buffers
        self.arrivals, self.folded, self.last = (a_in, b_in), (a_sum, b_sum), (a_last, b_last)
        self.m_send, self.m_recv, self.p_send, self.p_recv = sems[0:4]
        self.q_send, self.q_recv, self.z_send, self.z_recv = sems[4:8]
        self.partner = {"mp": 1 - self.c}

    def launch(self, copy):
        copy.start()
        self.started.append(copy)

    def across(self, piece):
        half, start, count, _ = PIECES[piece]
        items = pl.ds(start, count)
        return remote(
            self.g.at[1 - self.c, items], self.inbox.at[items], self.m_send.at[piece], self.m_recv.at[piece],
            self.partner,
        )

    def to_partner(self, piece):
        self.launch(self.across(piece))

    @scoped
    def near_sends(self, piece):
        half, start, count, at = PIECES[piece]
        near, far = HALVES[half]
        self.across(piece).wait_recv()
        for item in range(start, start + count):
            total = self.g[self.c, item].astype(F32) + self.inbox[item].astype(F32)
            self.sums[item] = total.astype(BF16)
        items = pl.ds(start, count)
        for step in ORDER:
            peer = lax.rem(self.here[near] + step, 4)
            ref = self.sums.at[items, :, peer] if half == 0 else self.sums.at[items, peer]
            self.launch(
                remote(
                    ref, self.arrivals[half].at[self.here[near], pl.ds(at, count)], self.p_send.at[piece, step],
                    self.p_recv.at[piece, self.here[near]], {near: peer},
                )
            )

    @scoped
    def far_sends(self, piece):
        half, start, count, at = PIECES[piece]
        near, far = HALVES[half]
        peers = [lax.rem(self.here[near] + step, 4) for step in ORDER]
        box, total_of = self.arrivals[half], self.folded[half]
        for peer in peers:
            ref = box.at[peer, pl.ds(at, count)]
            arrived(ref, self.p_recv.at[piece, peer], self.p_send.at[piece, 0], {near: peer})
        for item in range(count):
            own = self.sums[start + item, :, self.x] if half == 0 else self.sums[start + item, self.y]
            total = own.astype(F32)
            for peer in peers:
                total = total + box[peer, at + item].astype(F32)
            total_of[at + item] = total.astype(BF16)
        for step in ORDER:
            peer = lax.rem(self.here[far] + step, 4)
            self.launch(
                remote(
                    total_of.at[pl.ds(at, count), peer], self.last[half].at[self.here[far], pl.ds(at, count)],
                    self.q_send.at[piece, step], self.q_recv.at[piece, self.here[far]], {far: peer},
                )
            )

    @scoped
    def settle(self, piece):
        half, start, count, at = PIECES[piece]
        near, far = HALVES[half]
        peers = [lax.rem(self.here[far] + step, 4) for step in ORDER]
        box, total_of = self.last[half], self.folded[half]
        for peer in peers:
            ref = box.at[peer, pl.ds(at, count)]
            arrived(ref, self.q_recv.at[piece, peer], self.q_send.at[piece, 0], {far: peer})
        for item in range(count):
            total = total_of[at + item, self.here[far]].astype(F32)
            for peer in peers:
                total = total + box[peer, at + item].astype(F32)
            self.flat[16 * (start + item) : 16 * (start + item) + 16, :] = total

    @scoped
    def along_z(self, turn, item, letters, out):
        rows = letters.shape[1]
        for spot in range(8):
            letters[spot] = self.flat[pl.ds(16 * item + spot, rows, stride=8), :].astype(BF16)
        for step in range(1, 8):
            peer = lax.rem(self.z + step, 8)
            self.launch(
                remote(
                    letters.at[peer], out.at[self.z], self.z_send.at[turn, step], self.z_recv.at[turn, self.z],
                    {"dp_1": peer},
                )
            )
        out[self.z] = letters[self.z]

    @scoped
    def collect(self, turn, out):
        for step in range(1, 8):
            peer = lax.rem(self.z + step, 8)
            arrived(out.at[peer], self.z_recv.at[turn, peer], self.z_send.at[turn, 0], {"dp_1": peer})


NN = (((1,), (0,)), ((), ()))
NT = (((1,), (1,)), ((), ()))
TN = (((0,), (0,)), ((), ()))


def dot(a, b, dims=NN):
    return lax.dot_general(a, b, dims, preferred_element_type=F32)


def window_kernel(
    moves_in, values_in, rewards_in, hidden_in, first_in, second_in, head_in, embed_in, early, late,
    first_v, second_v, head_v, embed_v, hidden_v, rows, stage, wide, w, g,
    inbox, sums, a_in, b_in, a_sum, b_sum, a_last, b_last, flat, early_out, late_out,
    xs, hs, bs, zs, xt, bt, state, mixed, pre, summed, saved, slabs, first_t, second_t, moves, values, rewards, local_sem, *sems,
):
    seat = y, z, x, c = seats()
    barrier = greet_all(y, z, x, c)
    pairs = (
        (first_in, first_v), (second_in, second_v), (head_in, head_v), (embed_in, embed_v), (hidden_in, hidden_v),
        (moves_in, moves), (values_in, values), (rewards_in, rewards),
    )
    loads = [pltpu.make_async_copy(src, dst, local_sem.at[k]) for k, (src, dst) in enumerate(pairs)]
    for load in loads:
        load.start()
    started, sent = [], []
    gather = Gather(seat, w, stage, wide, sems[0:8], sent)
    scatter = Scatter(
        seat, g, (inbox, sums, a_in, b_in, a_sum, b_sum, a_last, b_last, flat), sems[8:16], started
    )
    rows[2 * MIX : 2 * MIX + 4, :] = jnp.zeros((4, 128), F32)
    for load in loads[0:4]:
        load.wait()
    for tap in range(9):
        at = 2 * (SECOND + tap)
        rows[at : at + 2, :] = second_v[tap // 3, tap % 3]
        at = 2 * (FIRST + tap)
        rows[at : at + 2, :] = first_v[tap // 3, tap % 3]
    for block in range(5):
        width = min(128, BUCKETS - 128 * block)
        at = 2 * (HEAD + block if block < 4 else MIX)
        rows[at : at + 2, 0:width] = head_v[0, :, 128 * block : 128 * block + width]
    for r in range(2):
        at = 2 * MIX + r
        rows[at : at + 1, 127:128] = embed_v[:, r : r + 1]
    stage[0, z] = rows[0:24, :].astype(BF16)
    stage[1, z] = rows[2 * SPLIT : 2 * SPLIT + 24, :].astype(BF16)
    with jax.named_scope("barrier"):
        pl.semaphore_wait(barrier, 14)
    gather.along_z()

    def phase(run):
        def inner(*given):
            with jax.named_scope(run.__name__):
                return run(*given)

        return inner

    row = lax.broadcasted_iota(jnp.int32, (ROWS, CHANNELS), 0)
    valid = (lax.rem(row, PITCH) < SIDE) & (row < PITCH * SIDE)

    def whole(h, item):
        return w[h, item].reshape(CHANNELS, 128)

    def first(tap):
        return jnp.concatenate([whole(0, FIRST + tap), whole(1, FIRST + tap)], axis=1)

    def second(tap):
        return jnp.concatenate([whole(0, SECOND + tap), whole(1, SECOND + tap)], axis=1)

    def head(h):
        last = whole(h, MIX)
        last = jnp.where(lax.broadcasted_iota(jnp.int32, last.shape, 1) < BUCKETS - 512, last, jnp.zeros_like(last))
        return jnp.concatenate([whole(h, HEAD + k) for k in range(4)] + [last], axis=1)

    def halves(lhs, rhs):
        cut = ROWS // 2
        return jnp.concatenate([dot(lhs[:cut], rhs), dot(lhs[cut:], rhs)], axis=0)

    @phase
    def transposes(dest, kernel, flip):
        for tap in range(9):
            turn = kernel(8 - tap if flip else tap).astype(F32).T
            dest[CHANNELS * tap : CHANNELS * tap + CHANNELS, :] = turn.astype(BF16)

    def taps_of(field):
        return jnp.concatenate([field[t] for t in range(9)], axis=1)

    @phase
    def conv_first(field):
        return halves(taps_of(field), jnp.concatenate([first(t) for t in range(9)], axis=0))

    @phase
    def conv_second(field):
        return halves(taps_of(field), second_t[...])

    @phase
    def back_second(field):
        return halves(taps_of(field), jnp.concatenate([second(8 - t) for t in range(9)], axis=0))

    @phase
    def back_first(field):
        return halves(taps_of(field), first_t[...])

    @phase
    def spread(value, dest):
        for h in range(2):
            lanes = slice(128 * h, 128 * h + 128)
            slabs[h, GUARD : GUARD + ROWS, :] = value[:, lanes]
            for t in range(9):
                start = GUARD + SHIFTS[t]
                dest[t, :, lanes] = slabs[h, start : start + ROWS, :].astype(BF16)

    @phase
    def turned(value):
        return value.T.astype(BF16)

    def total(value):
        return jnp.sum(jnp.sum(value, axis=0, keepdims=True), axis=1, keepdims=True)

    def store(h, item, value):
        g[h, item] = value.astype(BF16).reshape(4, 4, 16, 128)

    for h in range(2):
        slabs[h, 0:GUARD, :] = jnp.zeros((GUARD, 128), F32)
        slabs[h, GUARD + ROWS :, :] = jnp.zeros((GUARD, 128), F32)
    flat[16 * FIRST : 16 * FIRST + 48, :] = jnp.zeros((48, 128), F32)

    state[...] = jnp.zeros((ROWS, CHANNELS), F32)
    for load in loads[4:8]:
        load.wait()

    with jax.named_scope("place"):
        for line in range(SIDE):
            cells = hidden_v[line].astype(F32)
            mine = jnp.where(c == 0, cells[:, 0, :], cells[:, 1, :])
            state[PITCH * line : PITCH * line + SIDE, :] = mine
    lane = lax.broadcasted_iota(jnp.int32, (CHANNELS, CHANNELS), 1)
    natural = 64 * (lane // 64) + 8 * (lane % 8) + 2 * ((lane // 16) % 4) + (lane // 8) % 2
    source = lax.broadcasted_iota(jnp.int32, (CHANNELS, CHANNELS), 0)
    permute = jnp.where(source == natural, 1.0, 0.0).astype(BF16)
    state[...] = dot(state[...].astype(BF16), permute)

    gather.unpack(1)
    for chunk in (3, 2):
        gather.near_sends(chunk)
        gather.own_sends(chunk)
    gather.unpack(0)
    for chunk in (1, 0):
        gather.near_sends(chunk)
    for chunk in (3, 2):
        gather.far_sends(chunk)
    for chunk in (1, 0):
        gather.own_sends(chunk)
        gather.far_sends(chunk)
    gather.cross(3)
    gather.cross(2)
    gather.join(3)

    ones = jnp.ones((16, 128), BF16)
    pick = lax.broadcasted_iota(jnp.int32, (16, 128), 1) == 127
    pick = jnp.where(pick, ones, jnp.zeros_like(ones))
    embed = [dot(pick, whole(e, MIX), NT)[0:1, :] for e in range(2)]

    kept = []
    pooled_rows = jnp.zeros((16, CHANNELS), F32)
    for k in range(2):
        move = moves[c, k]
        spot = PITCH * lax.div(move, SIDE) + lax.rem(move, SIDE)
        passed = move == CELLS
        added = jnp.where(row == spot, embed[0], 0.0) + jnp.where(passed, 1.0, 0.0) * embed[1]
        now = jnp.where(valid, state[...] + added, 0.0)
        mixed[...] = now
        if k == 1:
            gather.cross(0)
        spread(now, xs.at[k])
        if k == 0:
            gather.join(2)
        value = SCALE * conv_first(xs.at[k])
        pre[k] = value
        spread(jnp.where(valid, value * jax.nn.sigmoid(value), 0.0), hs.at[k])
        if k == 0:
            gather.cross(1)
            xt[:, 0:ROWS] = turned(mixed[...])
            transposes(first_t, first, True)
            gather.join(1)
            transposes(second_t, second, False)
        branch = conv_second(hs.at[k])
        value = jnp.where(valid, mixed[...] + SCALE * branch, 0.0)
        summed[k] = value
        factor = lax.rsqrt(total(value * value) / (CELLS * CHANNELS) + eps_norm)
        value = value * factor
        state[...] = value
        pooled = jnp.sum(value, axis=0, keepdims=True) / CELLS
        own_row = lax.broadcasted_iota(jnp.int32, (16, CHANNELS), 0) == k
        pooled_rows = jnp.where(own_row, pooled, pooled_rows)
        kept.append((spot, passed, factor))
    gather.join(0)

    bucket = lax.broadcasted_iota(jnp.int32, (16, 640), 1)
    top_row = lax.broadcasted_iota(jnp.int32, (16, 640), 0) == 0
    pooled = pooled_rows.astype(BF16)
    pooled_grads = jnp.zeros((16, CHANNELS), F32)
    logits = []
    for h, targets in enumerate((values, rewards)):
        raw = head_scale * dot(pooled, head(h))
        squashed = jnp.tanh(raw / soft_cap)
        raised = jnp.where(bucket < BUCKETS, jnp.exp(soft_cap * squashed), 0.0)
        chances = raised / jnp.sum(raised, axis=1, keepdims=True)
        picked = jnp.where(bucket == jnp.where(top_row, targets[c, 0], targets[c, 1]), 1.0, 0.0)
        logit = (chances - picked) * (1.0 - squashed * squashed) / 256.0
        logit = jnp.where(bucket < BUCKETS, logit, 0.0).astype(BF16)
        pooled_grads = pooled_grads + dot(logit, head(h), NT)
        logits.append(logit)
    mixed_grads = []
    for h in range(2):
        grad = head_scale * dot(pooled, logits[h], TN)
        for block in range(4):
            store(h, HEAD + block, grad[:, 128 * block : 128 * block + 128])
        mixed_grads.append(grad[:, 512:640])
    for piece in (0, 1):
        scatter.to_partner(piece)

    def window(field, tap):
        return jnp.concatenate([field[k, tap] for k in range(2)], axis=0)

    def second_taps(*taps):
        with jax.named_scope("second_taps"):
            for tap in taps:
                grad = SCALE * dot(bt[...], window(hs, tap))
                store(0, SECOND + tap, grad[:, 0:128])
                store(1, SECOND + tap, grad[:, 128:256])

    def first_taps(*taps):
        with jax.named_scope("first_taps"):
            for tap in taps:
                grad = SCALE * dot(xt[...], window(zs, 8 - tap))
                store(0, FIRST + tap, grad[:, 0:128])
                store(1, FIRST + tap, grad[:, 128:256])

    embed_grad = [jnp.zeros((1, CHANNELS), F32) for _ in range(2)]
    for k in (1, 0):
        spot, passed, factor = kept[k]
        grad = head_scale * pooled_grads[k : k + 1, :] / CELLS
        if k == 0:
            grad = saved[...] + grad
        grad = jnp.where(valid, grad, 0.0)
        value = summed[k]
        slope = total(grad * value) / (CELLS * CHANNELS)
        summed_grad = factor * grad - factor * factor * factor * value * slope
        saved[...] = summed_grad
        spread(summed_grad, bs.at[k])
        bt[:, ROWS * k : ROWS * k + ROWS] = turned(summed_grad)
        if k == 0:
            second_taps(0)
            scatter.to_partner(2)
            second_taps(1, 2)
            scatter.to_partner(3)
            second_taps(3, 4)
            scatter.to_partner(4)
            xt[:, ROWS : 2 * ROWS] = turned(mixed[...])
            scatter.near_sends(2)
            second_taps(5, 6)
            scatter.to_partner(5)
            scatter.near_sends(3)
            second_taps(7, 8)
            scatter.to_partner(6)
            scatter.near_sends(4)
        hidden_grad = SCALE * back_second(bs.at[k])
        if k == 0:
            scatter.near_sends(5)
        value = pre[k]
        sig = jax.nn.sigmoid(value)
        inner = hidden_grad * (sig * (1.0 + value * (1.0 - sig)))
        spread(jnp.where(valid, inner, 0.0), zs.at[k])
        if k == 0:
            scatter.near_sends(6)
            first_taps(0, 1)
            scatter.to_partner(7)
            first_taps(2, 3)
            scatter.to_partner(8)
            for piece in (0, 1):
                scatter.far_sends(piece)
        carry = saved[...] + SCALE * back_first(zs.at[k])
        if k == 0:
            scatter.near_sends(7)
            scatter.near_sends(8)
        else:
            scatter.near_sends(0)
            scatter.near_sends(1)
        carry = jnp.where(valid, carry, 0.0)
        saved[...] = carry
        embed_grad[0] = embed_grad[0] + jnp.sum(jnp.where(row == spot, carry, 0.0), axis=0, keepdims=True)
        embed_grad[1] = embed_grad[1] + jnp.where(passed, 1.0, 0.0) * jnp.sum(carry, axis=0, keepdims=True)

    for e in range(2):
        lines = jnp.broadcast_to(embed_grad[e], (16, CHANNELS)).astype(BF16)
        corner = lax.broadcasted_iota(jnp.int32, (16, 128), 0) * 128 + lax.broadcasted_iota(jnp.int32, (16, 128), 1)
        corner = jnp.where(corner == 127, ones, jnp.zeros_like(ones))
        store(e, MIX, mixed_grads[e] + dot(lines, corner, TN))
    scatter.to_partner(12)
    first_taps(4, 5)
    scatter.to_partner(9)
    first_taps(6, 7)
    scatter.to_partner(10)
    first_taps(8)
    scatter.to_partner(11)
    for piece in (9, 12, 10, 11):
        scatter.near_sends(piece)
    for piece in (2, 3, 4, 5, 6, 7, 8):
        scatter.far_sends(piece)
    for copy in sent:
        copy.wait_send()
    for piece in (9, 12, 10):
        scatter.far_sends(piece)
    for piece in (0, 1):
        scatter.settle(piece)
    scatter.far_sends(11)
    for piece in (2, 3, 4, 5, 6):
        scatter.settle(piece)
    scatter.along_z(0, 0, early_out, early)
    for piece in (7, 8, 9, 12, 10, 11):
        scatter.settle(piece)
    scatter.along_z(1, SPLIT, late_out, late)
    scatter.collect(0, early)
    scatter.collect(1, late)
    with jax.named_scope("drain"):
        for copy in started:
            copy.wait_send()


def window_grads(moves, values, rewards, hidden_state, params):
    vmem = pl.BlockSpec(memory_space=pltpu.VMEM)
    hbm = pl.BlockSpec(memory_space=pltpu.HBM)
    dma = pltpu.SemaphoreType.DMA
    copies = pltpu.VMEM((2, 9, ROWS, CHANNELS), BF16)
    turned = pltpu.VMEM((CHANNELS, 2 * ROWS), BF16)
    field = pltpu.VMEM((ROWS, CHANNELS), F32)
    fields = pltpu.VMEM((2, ROWS, CHANNELS), F32)
    board = pltpu.VMEM((ITEMS, 4, 4, 16, 128), BF16)
    boards = pltpu.VMEM((2, ITEMS, 4, 4, 16, 128), BF16)
    early, late = (8, 32, 128), (8, 24, 128)
    return pl.pallas_call(
        window_kernel,
        out_shape=[jax.ShapeDtypeStruct(early, BF16), jax.ShapeDtypeStruct(late, BF16)],
        in_specs=[hbm] * 8,
        out_specs=[vmem, vmem],
        scratch_shapes=[pltpu.VMEM(p.shape, F32) for p in params]
        + [
            pltpu.VMEM(hidden_state.shape, BF16),
            pltpu.VMEM((48, 128), F32),
            pltpu.VMEM((2, 8, 24, 128), BF16),
            pltpu.VMEM((2, 192, 128), F32),
            boards,
            boards,
            board,
            board,
            pltpu.VMEM((4, 12, 4, 16, 128), BF16),
            pltpu.VMEM((4, 12, 4, 16, 128), BF16),
            pltpu.VMEM((12, 4, 16, 128), BF16),
            pltpu.VMEM((12, 4, 16, 128), BF16),
            pltpu.VMEM((4, 12, 16, 128), BF16),
            pltpu.VMEM((4, 12, 16, 128), BF16),
            pltpu.VMEM((384, 128), F32),
            pltpu.VMEM(early, BF16),
            pltpu.VMEM(late, BF16),
            copies,
            copies,
            copies,
            copies,
            turned,
            turned,
            field,
            field,
            fields,
            fields,
            field,
            pltpu.VMEM((2, ROWS + 2 * GUARD, 128), F32),
            pltpu.VMEM((9 * CHANNELS, CHANNELS), BF16),
            pltpu.VMEM((9 * CHANNELS, CHANNELS), BF16),
            pltpu.SMEM((2, 2), jnp.int32),
            pltpu.SMEM((2, 2), jnp.int32),
            pltpu.SMEM((2, 2), jnp.int32),
            dma((8,)),
        ]
        + [
            dma(shape)
            for shape in (
                (2, 8), (2, 8), (4, 2, 4), (4, 2, 4), (4, 2, 4, 4), (4, 2, 4), (4, 2, 4), (4, 2, 4),
                (13,), (13,), (13, 4), (13, 4), (13, 4), (13, 4), (2, 8), (2, 8),
            )
        ],
        compiler_params=pltpu.CompilerParams(
            collective_id=0, has_side_effects=True, vmem_limit_bytes=58 << 20
        ),
        name="window",
    )(moves, values, rewards, hidden_state, *params)


def adam(param, grad, mean, square):
    mean_new = beta_one * mean + (1.0 - beta_one) * grad
    square_new = beta_two * square + (1.0 - beta_two) * grad * grad
    param_new = param - step_size * mean_new / (jnp.sqrt(square_new) + eps_adam)
    return param_new, mean_new, square_new, grad


def adam_kernel(*refs):
    given, outs, held, sem = refs[0:14], refs[14:30], refs[30:44], refs[44]
    loads = [pltpu.make_async_copy(src, dst, sem.at[k]) for k, (src, dst) in enumerate(zip(given, held))]
    for load in loads:
        load.start()
    for load in loads:
        load.wait()
    early, late = held[0:2]
    params, means, squares = held[2:6], held[6:10], held[10:14]
    new, mean_new, square_new, grads = outs[0:4], outs[4:8], outs[8:12], outs[12:16]
    totals = []
    for parts in (early, late):
        total = parts[0].astype(F32)
        for piece in range(1, 8):
            total = total + parts[piece].astype(F32)
        totals.append(total)

    def owned(item):
        if item < FIRST:
            return totals[0][2 * item : 2 * item + 2]
        return totals[1][2 * (item - SPLIT) : 2 * (item - SPLIT) + 2]

    for which in range(2):
        for tap in range(9):
            a, b = tap // 3, tap % 3
            grad = owned((FIRST, SECOND)[which] + tap)
            results = adam(params[which][a, b], grad, means[which][a, b], squares[which][a, b])
            for ref, result in zip((new, mean_new, square_new, grads), results):
                ref[which][a, b] = result
    head = jnp.concatenate([owned(HEAD + k) for k in range(4)] + [owned(MIX)], axis=1)[:, 0:BUCKETS]
    results = adam(params[2][0], head, means[2][0], squares[2][0])
    for ref, result in zip((new, mean_new, square_new, grads), results):
        ref[2][0] = result
    embed = owned(MIX)
    embed = jnp.concatenate([embed[0:1, 127:128], embed[1:2, 127:128]], axis=1)
    results = adam(params[3][...], embed, means[3][...], squares[3][...])
    for ref, result in zip((new, mean_new, square_new, grads), results):
        ref[3][...] = result


def updates(early, late, params, means, squares):
    vmem = pl.BlockSpec(memory_space=pltpu.VMEM)
    shapes = [jax.ShapeDtypeStruct(p.shape, F32) for p in params]
    given = (early, late, *params, *means, *squares)
    return pl.pallas_call(
        adam_kernel,
        out_shape=shapes * 4,
        in_specs=[pl.BlockSpec(memory_space=pltpu.HBM)] * 14,
        out_specs=[vmem] * 16,
        scratch_shapes=[pltpu.VMEM(a.shape, a.dtype) for a in given] + [pltpu.SemaphoreType.DMA((14,))],
        compiler_params=pltpu.CompilerParams(vmem_limit_bytes=58 << 20),
        name="adam",
    )(*given)


def local(
    hidden_state,
    actions,
    value_target,
    reward_target,
    kernel_first,
    kernel_second,
    head_weight,
    action_embed,
    first_mean,
    first_square,
    second_mean,
    second_square,
    head_mean,
    head_square,
    embed_mean,
    embed_square,
):
    params = (kernel_first, kernel_second, head_weight, action_embed)
    boards = jnp.transpose(hidden_state, (1, 2, 0, 3))
    early, late = window_grads(actions, value_target, reward_target, boards, params)
    outs = updates(
        early,
        late,
        params,
        (first_mean, second_mean, head_mean, embed_mean),
        (first_square, second_square, head_square, embed_square),
    )
    new, means, squares, sums = outs[0:4], outs[4:8], outs[8:12], outs[12:16]
    moments = [moment for pair in zip(means, squares) for moment in pair]
    return (*new, *moments, *sums)


def solution(mesh):
    torus = Mesh(mesh.devices.reshape(4, 8, 4, mesh.shape["mp"]), ("dp_0", "dp_1", "dp_2", "mp"))
    kernel = P(None, None, DP, "mp")
    head = P("mp", DP, None)
    embed = P("mp", DP)
    rows = P(DP, None)
    placed = (P(DP, None, None, None), rows, rows, rows, kernel, kernel, head, embed)
    moments = (kernel, kernel, kernel, kernel, head, head, embed, embed)
    return jax.shard_map(
        local,
        mesh=torus,
        in_specs=placed + moments,
        out_specs=(kernel, kernel, head, embed) + moments + (kernel, kernel, head, embed),
        check_vma=False,
    )
```

```python
import functools

import jax
import jax.numpy as jnp
from jax import lax
from jax.experimental import pallas as pl
from jax.experimental.pallas import tpu as pltpu
from jax.sharding import Mesh
from jax.sharding import PartitionSpec as P

MESH = pl.DeviceIdType.MESH
CHANNELS = 256
DP = ("dp_0", "dp_1", "dp_2")
SIDE = 19
CELLS = 361
BUCKETS = 601
PITCH = 20
ROWS = 384
GUARD = 24
SHIFTS = tuple(PITCH * (t // 3 - 1) + t % 3 - 1 for t in range(9))
ITEMS = 23
HEAD, SECOND, FIRST, MIX = 0, 4, 13, 22
SPLIT = 11
CHUNKS = ({0: (0, 2), 1: (2, 2)}, {0: (4, 5), 1: (9, 4)}, {0: (13, 4), 1: (17, 5)}, {0: (22, 1)})
PIECES = (
    (0, 0, 2, 0), (1, 2, 2, 0),
    (0, 4, 1, 2), (1, 5, 2, 2), (0, 7, 2, 3), (1, 9, 2, 4), (0, 11, 2, 5),
    (1, 13, 2, 6), (0, 15, 2, 7), (1, 17, 2, 8), (0, 19, 2, 9), (1, 21, 1, 10), (0, 22, 1, 11),
)
HALVES = (("dp_2", "dp_0"), ("dp_0", "dp_2"))
ORDER = (1, 3, 2)
SCALE = (9.0 * CHANNELS) ** (-0.5)

head_scale = 4.0
soft_cap = 15.0
eps_norm = 1e-05
beta_one = 0.9
beta_two = 0.999
step_size = 0.1
eps_adam = 1e-08

F32 = jnp.float32
BF16 = jnp.bfloat16


def scoped(method):
    @functools.wraps(method)
    def inner(self, *given):
        tag = "_".join(str(v) for v in given if isinstance(v, int))
        with jax.named_scope(f"{type(self).__name__}_{method.__name__}_{tag}"):
            return method(self, *given)

    return inner


def seats():
    return (
        lax.axis_index("dp_0"),
        lax.axis_index("dp_1"),
        lax.axis_index("dp_2"),
        lax.axis_index("mp"),
    )


def greet_all(y, z, x, c):
    barrier = pltpu.get_barrier_semaphore()
    for step in range(1, 8):
        pl.semaphore_signal(
            barrier, inc=1, device_id={"dp_1": lax.rem(z + step, 8)}, device_id_type=MESH
        )
    for step in range(1, 4):
        for name, here in (("dp_0", y), ("dp_2", x)):
            pl.semaphore_signal(
                barrier, inc=1, device_id={name: lax.rem(here + step, 4)}, device_id_type=MESH
            )
    pl.semaphore_signal(barrier, inc=1, device_id={"mp": 1 - c}, device_id_type=MESH)
    return barrier


def remote(src, dst, send, recv, peer):
    return pltpu.make_async_remote_copy(
        src_ref=src, dst_ref=dst, send_sem=send, recv_sem=recv, device_id=peer, device_id_type=MESH
    )


def arrived(ref, recv, send, peer):
    remote(ref, ref, send, recv, peer).wait_recv()


def halves_of(chunk):
    return [(half, *HALVES[half]) for half in CHUNKS[chunk]]


class Gather:
    def __init__(self, seat, w, stage, wide, sems, started):
        self.y, self.z, self.x, self.c = seat
        self.here = {"dp_0": self.y, "dp_2": self.x}
        self.w, self.stage, self.wide, self.started = w, stage, wide, started
        self.z_send, self.z_recv, self.p_send, self.p_recv = sems[0:4]
        self.q_send, self.q_recv, self.m_send, self.m_recv = sems[4:8]
        self.partner = {"mp": 1 - self.c}

    def launch(self, copy):
        copy.start()
        self.started.append(copy)

    def tile(self, chunk, half, near, far):
        items = pl.ds(*CHUNKS[chunk][half])
        if half == 0:
            return self.w.at[self.c, items, far, near]
        return self.w.at[self.c, items, near, far]

    def slab(self, chunk, half, far, core):
        items = pl.ds(*CHUNKS[chunk][half])
        if half == 0:
            return self.w.at[core, items, far]
        return self.w.at[core, items, :, far]

    @scoped
    def along_z(self):
        z = self.z
        for group in (1, 0):
            ref = self.stage.at[group, z]
            for step in range(1, 8):
                peer = {"dp_1": lax.rem(z + step, 8)}
                self.launch(remote(ref, ref, self.z_send.at[group, step], self.z_recv.at[group, z], peer))

    @scoped
    def unpack(self, group):
        for step in range(1, 8):
            peer = lax.rem(self.z + step, 8)
            sems = self.z_recv.at[group, peer], self.z_send.at[group, 0]
            arrived(self.stage.at[group, peer], *sems, {"dp_1": peer})
        for piece in range(8):
            self.wide[group, 24 * piece : 24 * piece + 24, :] = self.stage[group, piece].astype(F32)

    def to_far(self, chunk, half, turn, near):
        far = HALVES[half][1]
        at = self.here[far]
        ref = self.tile(chunk, half, near, at)
        for step in ORDER:
            self.launch(
                remote(
                    ref, ref, self.q_send.at[chunk, half, turn, step], self.q_recv.at[chunk, half, at],
                    {far: lax.rem(at + step, 4)},
                )
            )

    @scoped
    def near_sends(self, chunk):
        for half, near, far in halves_of(chunk):
            start, count = CHUNKS[chunk][half]
            for item in range(start, start + count):
                group = int(item >= SPLIT)
                line = 2 * (item - SPLIT * group)
                slab = self.wide.at[group]
                low = slab[pl.ds(line, 8, stride=24), :]
                high = slab[pl.ds(line + 1, 8, stride=24), :]
                self.w[self.c, item, self.y, self.x] = jnp.concatenate([low, high], axis=0).astype(BF16)
        for step in ORDER:
            for half, near, far in halves_of(chunk):
                at = self.here[near]
                ref = self.tile(chunk, half, at, self.here[far])
                self.launch(
                    remote(
                        ref, ref, self.p_send.at[chunk, half, step], self.p_recv.at[chunk, half, at],
                        {near: lax.rem(at + step, 4)},
                    )
                )

    def own_sends(self, chunk):
        for half, near, far in halves_of(chunk):
            self.to_far(chunk, half, 0, self.here[near])

    def to_partner(self, chunk, half, turn, ref):
        sems = self.m_send.at[chunk, half, turn], self.m_recv.at[chunk, half, turn]
        self.launch(remote(ref, ref, *sems, self.partner))

    @scoped
    def far_sends(self, chunk):
        for step in ORDER:
            for half, near, far in halves_of(chunk):
                peer = lax.rem(self.here[near] + step, 4)
                ref = self.tile(chunk, half, peer, self.here[far])
                arrived(ref, self.p_recv.at[chunk, half, peer], self.p_send.at[chunk, half, 0], {near: peer})
                self.to_far(chunk, half, step, peer)
        for half, near, far in halves_of(chunk):
            self.to_partner(chunk, half, 0, self.slab(chunk, half, self.here[far], self.c))

    @scoped
    def cross(self, chunk):
        for step in ORDER:
            for half, near, far in halves_of(chunk):
                peer = lax.rem(self.here[far] + step, 4)
                ref = self.slab(chunk, half, peer, self.c)
                arrived(ref, self.q_recv.at[chunk, half, peer], self.q_send.at[chunk, half, 0, 0], {far: peer})
                self.to_partner(chunk, half, step, ref)

    @scoped
    def join(self, chunk):
        for half, near, far in halves_of(chunk):
            for turn in range(4):
                ref = self.slab(chunk, half, lax.rem(self.here[far] + turn, 4), 1 - self.c)
                sems = self.m_recv.at[chunk, half, turn], self.m_send.at[chunk, half, turn]
                arrived(ref, *sems, self.partner)


class Scatter:
    def __init__(self, seat, g, buffers, sems, started):
        self.y, self.z, self.x, self.c = seat
        self.here = {"dp_0": self.y, "dp_2": self.x}
        self.g, self.started = g, started
        self.inbox, self.sums, a_in, b_in, a_sum, b_sum, a_last, b_last, self.flat = buffers
        self.arrivals, self.folded, self.last = (a_in, b_in), (a_sum, b_sum), (a_last, b_last)
        self.m_send, self.m_recv, self.p_send, self.p_recv = sems[0:4]
        self.q_send, self.q_recv, self.z_send, self.z_recv = sems[4:8]
        self.partner = {"mp": 1 - self.c}

    def launch(self, copy):
        copy.start()
        self.started.append(copy)

    def across(self, piece):
        half, start, count, _ = PIECES[piece]
        items = pl.ds(start, count)
        return remote(
            self.g.at[1 - self.c, items], self.inbox.at[items], self.m_send.at[piece], self.m_recv.at[piece],
            self.partner,
        )

    def to_partner(self, piece):
        self.launch(self.across(piece))

    @scoped
    def near_sends(self, piece):
        half, start, count, at = PIECES[piece]
        near, far = HALVES[half]
        self.across(piece).wait_recv()
        for item in range(start, start + count):
            total = self.g[self.c, item].astype(F32) + self.inbox[item].astype(F32)
            self.sums[item] = total.astype(BF16)
        items = pl.ds(start, count)
        for step in ORDER:
            peer = lax.rem(self.here[near] + step, 4)
            ref = self.sums.at[items, :, peer] if half == 0 else self.sums.at[items, peer]
            self.launch(
                remote(
                    ref, self.arrivals[half].at[self.here[near], pl.ds(at, count)], self.p_send.at[piece, step],
                    self.p_recv.at[piece, self.here[near]], {near: peer},
                )
            )

    @scoped
    def far_sends(self, piece):
        half, start, count, at = PIECES[piece]
        near, far = HALVES[half]
        peers = [lax.rem(self.here[near] + step, 4) for step in ORDER]
        box, total_of = self.arrivals[half], self.folded[half]
        for peer in peers:
            ref = box.at[peer, pl.ds(at, count)]
            arrived(ref, self.p_recv.at[piece, peer], self.p_send.at[piece, 0], {near: peer})
        for item in range(count):
            own = self.sums[start + item, :, self.x] if half == 0 else self.sums[start + item, self.y]
            total = own.astype(F32)
            for peer in peers:
                total = total + box[peer, at + item].astype(F32)
            total_of[at + item] = total.astype(BF16)
        for step in ORDER:
            peer = lax.rem(self.here[far] + step, 4)
            self.launch(
                remote(
                    total_of.at[pl.ds(at, count), peer], self.last[half].at[self.here[far], pl.ds(at, count)],
                    self.q_send.at[piece, step], self.q_recv.at[piece, self.here[far]], {far: peer},
                )
            )

    @scoped
    def settle(self, piece):
        half, start, count, at = PIECES[piece]
        near, far = HALVES[half]
        peers = [lax.rem(self.here[far] + step, 4) for step in ORDER]
        box, total_of = self.last[half], self.folded[half]
        for peer in peers:
            ref = box.at[peer, pl.ds(at, count)]
            arrived(ref, self.q_recv.at[piece, peer], self.q_send.at[piece, 0], {far: peer})
        for item in range(count):
            total = total_of[at + item, self.here[far]].astype(F32)
            for peer in peers:
                total = total + box[peer, at + item].astype(F32)
            self.flat[16 * (start + item) : 16 * (start + item) + 16, :] = total

    @scoped
    def along_z(self, turn, item, letters, out):
        rows = letters.shape[1]
        for spot in range(8):
            letters[spot] = self.flat[pl.ds(16 * item + spot, rows, stride=8), :].astype(BF16)
        for step in range(1, 8):
            peer = lax.rem(self.z + step, 8)
            self.launch(
                remote(
                    letters.at[peer], out.at[self.z], self.z_send.at[turn, step], self.z_recv.at[turn, self.z],
                    {"dp_1": peer},
                )
            )
        out[self.z] = letters[self.z]

    @scoped
    def collect(self, turn, out):
        for step in range(1, 8):
            peer = lax.rem(self.z + step, 8)
            arrived(out.at[peer], self.z_recv.at[turn, peer], self.z_send.at[turn, 0], {"dp_1": peer})


NN = (((1,), (0,)), ((), ()))
NT = (((1,), (1,)), ((), ()))
TN = (((0,), (0,)), ((), ()))


def dot(a, b, dims=NN):
    return lax.dot_general(a, b, dims, preferred_element_type=F32)


def window_kernel(
    moves_in, values_in, rewards_in, hidden_in, first_in, second_in, head_in, embed_in, early, late,
    first_v, second_v, head_v, embed_v, hidden_v, rows, stage, wide, w, g,
    inbox, sums, a_in, b_in, a_sum, b_sum, a_last, b_last, flat, early_out, late_out,
    xs, hs, bs, zs, xt, bt, state, mixed, pre, summed, saved, first_t, second_t, moves, values, rewards, local_sem, *sems,
):
    seat = y, z, x, c = seats()
    barrier = greet_all(y, z, x, c)
    pairs = (
        (first_in, first_v), (second_in, second_v), (head_in, head_v), (embed_in, embed_v), (hidden_in, hidden_v),
        (moves_in, moves), (values_in, values), (rewards_in, rewards),
    )
    loads = [pltpu.make_async_copy(src, dst, local_sem.at[k]) for k, (src, dst) in enumerate(pairs)]
    for load in loads:
        load.start()
    started, sent = [], []
    gather = Gather(seat, w, stage, wide, sems[0:8], sent)
    scatter = Scatter(
        seat, g, (inbox, sums, a_in, b_in, a_sum, b_sum, a_last, b_last, flat), sems[8:16], started
    )
    rows[2 * MIX : 2 * MIX + 4, :] = jnp.zeros((4, 128), F32)
    for load in loads[0:4]:
        load.wait()
    for tap in range(9):
        at = 2 * (SECOND + tap)
        rows[at : at + 2, :] = second_v[tap // 3, tap % 3]
        at = 2 * (FIRST + tap)
        rows[at : at + 2, :] = first_v[tap // 3, tap % 3]
    for block in range(5):
        width = min(128, BUCKETS - 128 * block)
        at = 2 * (HEAD + block if block < 4 else MIX)
        rows[at : at + 2, 0:width] = head_v[0, :, 128 * block : 128 * block + width]
    for r in range(2):
        at = 2 * MIX + r
        rows[at : at + 1, 127:128] = embed_v[:, r : r + 1]
    stage[0, z] = rows[0:24, :].astype(BF16)
    stage[1, z] = rows[2 * SPLIT : 2 * SPLIT + 24, :].astype(BF16)
    with jax.named_scope("barrier"):
        pl.semaphore_wait(barrier, 14)
    gather.along_z()

    def phase(run):
        def inner(*given):
            with jax.named_scope(run.__name__):
                return run(*given)

        return inner

    row = lax.broadcasted_iota(jnp.int32, (ROWS, CHANNELS), 0)
    valid = (lax.rem(row, PITCH) < SIDE) & (row < PITCH * SIDE)

    def whole(h, item):
        return w[h, item].reshape(CHANNELS, 128)

    def first(tap):
        return jnp.concatenate([whole(0, FIRST + tap), whole(1, FIRST + tap)], axis=1)

    def second(tap):
        return jnp.concatenate([whole(0, SECOND + tap), whole(1, SECOND + tap)], axis=1)

    def head(h):
        last = whole(h, MIX)
        last = jnp.where(lax.broadcasted_iota(jnp.int32, last.shape, 1) < BUCKETS - 512, last, jnp.zeros_like(last))
        return jnp.concatenate([whole(h, HEAD + k) for k in range(4)] + [last], axis=1)

    def shifted(field, tap):
        start = GUARD + SHIFTS[tap]
        return jnp.concatenate([field[h, start : start + ROWS, :].astype(BF16) for h in range(2)], axis=1)

    def halves(lhs, rhs):
        cut = ROWS // 2
        return jnp.concatenate([dot(lhs[:cut], rhs), dot(lhs[cut:], rhs)], axis=0)

    @phase
    def transposes(dest, kernel, flip):
        for tap in range(9):
            turn = kernel(8 - tap if flip else tap).astype(F32).T
            dest[CHANNELS * tap : CHANNELS * tap + CHANNELS, :] = turn.astype(BF16)

    def taps_of(field):
        return jnp.concatenate([shifted(field, t) for t in range(9)], axis=1)

    @phase
    def conv_first(field):
        return halves(taps_of(field), jnp.concatenate([first(t) for t in range(9)], axis=0))

    @phase
    def conv_second(field):
        return halves(taps_of(field), second_t[...])

    @phase
    def back_second(field):
        return halves(taps_of(field), jnp.concatenate([second(8 - t) for t in range(9)], axis=0))

    @phase
    def back_first(field):
        return halves(taps_of(field), first_t[...])

    @phase
    def spread(value, dest):
        for h in range(2):
            dest[h, GUARD : GUARD + ROWS, :] = value[:, 128 * h : 128 * h + 128]

    @phase
    def turned(value):
        return value.T.astype(BF16)

    def total(value):
        return jnp.sum(jnp.sum(value, axis=0, keepdims=True), axis=1, keepdims=True)

    def store(h, item, value):
        g[h, item] = value.astype(BF16).reshape(4, 4, 16, 128)

    for field in (xs, hs, bs, zs):
        for k in range(2):
            for h in range(2):
                field[k, h, 0:GUARD, :] = jnp.zeros((GUARD, 128), F32)
                field[k, h, GUARD + ROWS :, :] = jnp.zeros((GUARD, 128), F32)
    flat[16 * FIRST : 16 * FIRST + 48, :] = jnp.zeros((48, 128), F32)

    state[...] = jnp.zeros((ROWS, CHANNELS), F32)
    for load in loads[4:8]:
        load.wait()

    with jax.named_scope("place"):
        for line in range(SIDE):
            cells = hidden_v[line].astype(F32)
            mine = jnp.where(c == 0, cells[:, 0, :], cells[:, 1, :])
            state[PITCH * line : PITCH * line + SIDE, :] = mine
    lane = lax.broadcasted_iota(jnp.int32, (CHANNELS, CHANNELS), 1)
    natural = 64 * (lane // 64) + 8 * (lane % 8) + 2 * ((lane // 16) % 4) + (lane // 8) % 2
    source = lax.broadcasted_iota(jnp.int32, (CHANNELS, CHANNELS), 0)
    permute = jnp.where(source == natural, 1.0, 0.0).astype(BF16)
    state[...] = dot(state[...].astype(BF16), permute)

    gather.unpack(1)
    for chunk in (3, 2):
        gather.near_sends(chunk)
        gather.own_sends(chunk)
    gather.unpack(0)
    for chunk in (1, 0):
        gather.near_sends(chunk)
    for chunk in (3, 2):
        gather.far_sends(chunk)
    for chunk in (1, 0):
        gather.own_sends(chunk)
        gather.far_sends(chunk)
    gather.cross(3)
    gather.cross(2)
    gather.join(3)

    ones = jnp.ones((16, 128), BF16)
    pick = lax.broadcasted_iota(jnp.int32, (16, 128), 1) == 127
    pick = jnp.where(pick, ones, jnp.zeros_like(ones))
    embed = [dot(pick, whole(e, MIX), NT)[0:1, :] for e in range(2)]

    kept = []
    pooled_rows = jnp.zeros((16, CHANNELS), F32)
    for k in range(2):
        move = moves[c, k]
        spot = PITCH * lax.div(move, SIDE) + lax.rem(move, SIDE)
        passed = move == CELLS
        added = jnp.where(row == spot, embed[0], 0.0) + jnp.where(passed, 1.0, 0.0) * embed[1]
        now = jnp.where(valid, state[...] + added, 0.0)
        mixed[...] = now
        if k == 1:
            gather.cross(0)
        spread(now, xs.at[k])
        if k == 0:
            gather.join(2)
        value = SCALE * conv_first(xs.at[k])
        pre[k] = value
        spread(jnp.where(valid, value * jax.nn.sigmoid(value), 0.0), hs.at[k])
        if k == 0:
            gather.cross(1)
            xt[:, 0:ROWS] = turned(mixed[...])
            transposes(first_t, first, True)
            gather.join(1)
            transposes(second_t, second, False)
        branch = conv_second(hs.at[k])
        value = jnp.where(valid, mixed[...] + SCALE * branch, 0.0)
        summed[k] = value
        factor = lax.rsqrt(total(value * value) / (CELLS * CHANNELS) + eps_norm)
        value = value * factor
        state[...] = value
        pooled = jnp.sum(value, axis=0, keepdims=True) / CELLS
        own_row = lax.broadcasted_iota(jnp.int32, (16, CHANNELS), 0) == k
        pooled_rows = jnp.where(own_row, pooled, pooled_rows)
        kept.append((spot, passed, factor))
    gather.join(0)

    bucket = lax.broadcasted_iota(jnp.int32, (16, 640), 1)
    top_row = lax.broadcasted_iota(jnp.int32, (16, 640), 0) == 0
    pooled = pooled_rows.astype(BF16)
    pooled_grads = jnp.zeros((16, CHANNELS), F32)
    logits = []
    for h, targets in enumerate((values, rewards)):
        raw = head_scale * dot(pooled, head(h))
        squashed = jnp.tanh(raw / soft_cap)
        raised = jnp.where(bucket < BUCKETS, jnp.exp(soft_cap * squashed), 0.0)
        chances = raised / jnp.sum(raised, axis=1, keepdims=True)
        picked = jnp.where(bucket == jnp.where(top_row, targets[c, 0], targets[c, 1]), 1.0, 0.0)
        logit = (chances - picked) * (1.0 - squashed * squashed) / 256.0
        logit = jnp.where(bucket < BUCKETS, logit, 0.0).astype(BF16)
        pooled_grads = pooled_grads + dot(logit, head(h), NT)
        logits.append(logit)
    mixed_grads = []
    for h in range(2):
        grad = head_scale * dot(pooled, logits[h], TN)
        for block in range(4):
            store(h, HEAD + block, grad[:, 128 * block : 128 * block + 128])
        mixed_grads.append(grad[:, 512:640])
    for piece in (0, 1):
        scatter.to_partner(piece)

    def window(field, tap):
        return jnp.concatenate([shifted(field.at[k], tap) for k in range(2)], axis=0)

    def second_taps(*taps):
        with jax.named_scope("second_taps"):
            for tap in taps:
                grad = SCALE * dot(bt[...], window(hs, tap))
                store(0, SECOND + tap, grad[:, 0:128])
                store(1, SECOND + tap, grad[:, 128:256])

    def first_taps(*taps):
        with jax.named_scope("first_taps"):
            for tap in taps:
                grad = SCALE * dot(xt[...], window(zs, 8 - tap))
                store(0, FIRST + tap, grad[:, 0:128])
                store(1, FIRST + tap, grad[:, 128:256])

    embed_grad = [jnp.zeros((1, CHANNELS), F32) for _ in range(2)]
    for k in (1, 0):
        spot, passed, factor = kept[k]
        grad = head_scale * pooled_grads[k : k + 1, :] / CELLS
        if k == 0:
            grad = saved[...] + grad
        grad = jnp.where(valid, grad, 0.0)
        value = summed[k]
        slope = total(grad * value) / (CELLS * CHANNELS)
        summed_grad = factor * grad - factor * factor * factor * value * slope
        saved[...] = summed_grad
        spread(summed_grad, bs.at[k])
        bt[:, ROWS * k : ROWS * k + ROWS] = turned(summed_grad)
        if k == 0:
            second_taps(0)
            scatter.to_partner(2)
            second_taps(1, 2)
            scatter.to_partner(3)
            second_taps(3, 4)
            scatter.to_partner(4)
            xt[:, ROWS : 2 * ROWS] = turned(mixed[...])
            scatter.near_sends(2)
            second_taps(5, 6)
            scatter.to_partner(5)
            scatter.near_sends(3)
            second_taps(7, 8)
            scatter.to_partner(6)
            scatter.near_sends(4)
        hidden_grad = SCALE * back_second(bs.at[k])
        if k == 0:
            scatter.near_sends(5)
        value = pre[k]
        sig = jax.nn.sigmoid(value)
        inner = hidden_grad * (sig * (1.0 + value * (1.0 - sig)))
        spread(jnp.where(valid, inner, 0.0), zs.at[k])
        if k == 0:
            scatter.near_sends(6)
            first_taps(0, 1)
            scatter.to_partner(7)
            first_taps(2, 3)
            scatter.to_partner(8)
            for piece in (0, 1):
                scatter.far_sends(piece)
        carry = saved[...] + SCALE * back_first(zs.at[k])
        if k == 0:
            scatter.near_sends(7)
            scatter.near_sends(8)
        else:
            scatter.near_sends(0)
            scatter.near_sends(1)
        carry = jnp.where(valid, carry, 0.0)
        saved[...] = carry
        embed_grad[0] = embed_grad[0] + jnp.sum(jnp.where(row == spot, carry, 0.0), axis=0, keepdims=True)
        embed_grad[1] = embed_grad[1] + jnp.where(passed, 1.0, 0.0) * jnp.sum(carry, axis=0, keepdims=True)

    for e in range(2):
        lines = jnp.broadcast_to(embed_grad[e], (16, CHANNELS)).astype(BF16)
        corner = lax.broadcasted_iota(jnp.int32, (16, 128), 0) * 128 + lax.broadcasted_iota(jnp.int32, (16, 128), 1)
        corner = jnp.where(corner == 127, ones, jnp.zeros_like(ones))
        store(e, MIX, mixed_grads[e] + dot(lines, corner, TN))
    scatter.to_partner(12)
    first_taps(4, 5)
    scatter.to_partner(9)
    first_taps(6, 7)
    scatter.to_partner(10)
    first_taps(8)
    scatter.to_partner(11)
    for piece in (9, 12, 10, 11):
        scatter.near_sends(piece)
    for piece in (2, 3, 4, 5, 6, 7, 8):
        scatter.far_sends(piece)
    for copy in sent:
        copy.wait_send()
    for piece in (9, 12, 10):
        scatter.far_sends(piece)
    for piece in (0, 1):
        scatter.settle(piece)
    scatter.far_sends(11)
    for piece in (2, 3, 4, 5, 6):
        scatter.settle(piece)
    scatter.along_z(0, 0, early_out, early)
    for piece in (7, 8, 9, 12, 10, 11):
        scatter.settle(piece)
    scatter.along_z(1, SPLIT, late_out, late)
    scatter.collect(0, early)
    scatter.collect(1, late)
    with jax.named_scope("drain"):
        for copy in started:
            copy.wait_send()


def window_grads(moves, values, rewards, hidden_state, params):
    vmem = pl.BlockSpec(memory_space=pltpu.VMEM)
    hbm = pl.BlockSpec(memory_space=pltpu.HBM)
    dma = pltpu.SemaphoreType.DMA
    copies = pltpu.VMEM((2, 2, ROWS + 2 * GUARD, 128), F32)
    turned = pltpu.VMEM((CHANNELS, 2 * ROWS), BF16)
    field = pltpu.VMEM((ROWS, CHANNELS), F32)
    fields = pltpu.VMEM((2, ROWS, CHANNELS), F32)
    board = pltpu.VMEM((ITEMS, 4, 4, 16, 128), BF16)
    boards = pltpu.VMEM((2, ITEMS, 4, 4, 16, 128), BF16)
    early, late = (8, 32, 128), (8, 24, 128)
    return pl.pallas_call(
        window_kernel,
        out_shape=[jax.ShapeDtypeStruct(early, BF16), jax.ShapeDtypeStruct(late, BF16)],
        in_specs=[hbm] * 8,
        out_specs=[vmem, vmem],
        scratch_shapes=[pltpu.VMEM(p.shape, F32) for p in params]
        + [
            pltpu.VMEM(hidden_state.shape, BF16),
            pltpu.VMEM((48, 128), F32),
            pltpu.VMEM((2, 8, 24, 128), BF16),
            pltpu.VMEM((2, 192, 128), F32),
            boards,
            boards,
            board,
            board,
            pltpu.VMEM((4, 12, 4, 16, 128), BF16),
            pltpu.VMEM((4, 12, 4, 16, 128), BF16),
            pltpu.VMEM((12, 4, 16, 128), BF16),
            pltpu.VMEM((12, 4, 16, 128), BF16),
            pltpu.VMEM((4, 12, 16, 128), BF16),
            pltpu.VMEM((4, 12, 16, 128), BF16),
            pltpu.VMEM((384, 128), F32),
            pltpu.VMEM(early, BF16),
            pltpu.VMEM(late, BF16),
            copies,
            copies,
            copies,
            copies,
            turned,
            turned,
            field,
            field,
            fields,
            fields,
            field,
            pltpu.VMEM((9 * CHANNELS, CHANNELS), BF16),
            pltpu.VMEM((9 * CHANNELS, CHANNELS), BF16),
            pltpu.SMEM((2, 2), jnp.int32),
            pltpu.SMEM((2, 2), jnp.int32),
            pltpu.SMEM((2, 2), jnp.int32),
            dma((8,)),
        ]
        + [
            dma(shape)
            for shape in (
                (2, 8), (2, 8), (4, 2, 4), (4, 2, 4), (4, 2, 4, 4), (4, 2, 4), (4, 2, 4), (4, 2, 4),
                (13,), (13,), (13, 4), (13, 4), (13, 4), (13, 4), (2, 8), (2, 8),
            )
        ],
        compiler_params=pltpu.CompilerParams(
            collective_id=0, has_side_effects=True, vmem_limit_bytes=58 << 20
        ),
        name="window",
    )(moves, values, rewards, hidden_state, *params)


def adam(param, grad, mean, square):
    mean_new = beta_one * mean + (1.0 - beta_one) * grad
    square_new = beta_two * square + (1.0 - beta_two) * grad * grad
    param_new = param - step_size * mean_new / (jnp.sqrt(square_new) + eps_adam)
    return param_new, mean_new, square_new, grad


def adam_kernel(*refs):
    given, outs, held, sem = refs[0:14], refs[14:30], refs[30:44], refs[44]
    loads = [pltpu.make_async_copy(src, dst, sem.at[k]) for k, (src, dst) in enumerate(zip(given, held))]
    for load in loads:
        load.start()
    for load in loads:
        load.wait()
    early, late = held[0:2]
    params, means, squares = held[2:6], held[6:10], held[10:14]
    new, mean_new, square_new, grads = outs[0:4], outs[4:8], outs[8:12], outs[12:16]
    totals = []
    for parts in (early, late):
        total = parts[0].astype(F32)
        for piece in range(1, 8):
            total = total + parts[piece].astype(F32)
        totals.append(total)

    def owned(item):
        if item < FIRST:
            return totals[0][2 * item : 2 * item + 2]
        return totals[1][2 * (item - SPLIT) : 2 * (item - SPLIT) + 2]

    for which in range(2):
        for tap in range(9):
            a, b = tap // 3, tap % 3
            grad = owned((FIRST, SECOND)[which] + tap)
            results = adam(params[which][a, b], grad, means[which][a, b], squares[which][a, b])
            for ref, result in zip((new, mean_new, square_new, grads), results):
                ref[which][a, b] = result
    head = jnp.concatenate([owned(HEAD + k) for k in range(4)] + [owned(MIX)], axis=1)[:, 0:BUCKETS]
    results = adam(params[2][0], head, means[2][0], squares[2][0])
    for ref, result in zip((new, mean_new, square_new, grads), results):
        ref[2][0] = result
    embed = owned(MIX)
    embed = jnp.concatenate([embed[0:1, 127:128], embed[1:2, 127:128]], axis=1)
    results = adam(params[3][...], embed, means[3][...], squares[3][...])
    for ref, result in zip((new, mean_new, square_new, grads), results):
        ref[3][...] = result


def updates(early, late, params, means, squares):
    vmem = pl.BlockSpec(memory_space=pltpu.VMEM)
    shapes = [jax.ShapeDtypeStruct(p.shape, F32) for p in params]
    given = (early, late, *params, *means, *squares)
    return pl.pallas_call(
        adam_kernel,
        out_shape=shapes * 4,
        in_specs=[pl.BlockSpec(memory_space=pltpu.HBM)] * 14,
        out_specs=[vmem] * 16,
        scratch_shapes=[pltpu.VMEM(a.shape, a.dtype) for a in given] + [pltpu.SemaphoreType.DMA((14,))],
        compiler_params=pltpu.CompilerParams(vmem_limit_bytes=58 << 20),
        name="adam",
    )(*given)


def local(
    hidden_state,
    actions,
    value_target,
    reward_target,
    kernel_first,
    kernel_second,
    head_weight,
    action_embed,
    first_mean,
    first_square,
    second_mean,
    second_square,
    head_mean,
    head_square,
    embed_mean,
    embed_square,
):
    params = (kernel_first, kernel_second, head_weight, action_embed)
    boards = jnp.transpose(hidden_state, (1, 2, 0, 3))
    early, late = window_grads(actions, value_target, reward_target, boards, params)
    outs = updates(
        early,
        late,
        params,
        (first_mean, second_mean, head_mean, embed_mean),
        (first_square, second_square, head_square, embed_square),
    )
    new, means, squares, sums = outs[0:4], outs[4:8], outs[8:12], outs[12:16]
    moments = [moment for pair in zip(means, squares) for moment in pair]
    return (*new, *moments, *sums)


def solution(mesh):
    torus = Mesh(mesh.devices.reshape(4, 8, 4, mesh.shape["mp"]), ("dp_0", "dp_1", "dp_2", "mp"))
    kernel = P(None, None, DP, "mp")
    head = P("mp", DP, None)
    embed = P("mp", DP)
    rows = P(DP, None)
    placed = (P(DP, None, None, None), rows, rows, rows, kernel, kernel, head, embed)
    moments = (kernel, kernel, kernel, kernel, head, head, embed, embed)
    return jax.shard_map(
        local,
        mesh=torus,
        in_specs=placed + moments,
        out_specs=(kernel, kernel, head, embed) + moments + (kernel, kernel, head, embed),
        check_vma=False,
    )
```

```python
import functools

import jax
import jax.numpy as jnp
from jax import lax
from jax.experimental import pallas as pl
from jax.experimental.pallas import tpu as pltpu
from jax.sharding import Mesh
from jax.sharding import PartitionSpec as P

MESH = pl.DeviceIdType.MESH
CHANNELS = 256
DP = ("dp_0", "dp_1", "dp_2")
SIDE = 19
CELLS = 361
BUCKETS = 601
PITCH = 20
ROWS = 384
GUARD = 24
SHIFTS = tuple(PITCH * (t // 3 - 1) + t % 3 - 1 for t in range(9))
ITEMS = 23
HEAD, SECOND, FIRST, MIX = 0, 4, 13, 22
SPLIT = 11
CHUNKS = ({0: (0, 2), 1: (2, 2)}, {0: (4, 5), 1: (9, 4)}, {0: (13, 4), 1: (17, 5)}, {0: (22, 1)})
PIECES = (
    (0, 0, 2, 0), (1, 2, 2, 0),
    (0, 4, 1, 2), (1, 5, 2, 2), (0, 7, 2, 3), (1, 9, 2, 4), (0, 11, 2, 5),
    (1, 13, 2, 6), (0, 15, 2, 7), (1, 17, 2, 8), (0, 19, 2, 9), (1, 21, 1, 10), (0, 22, 1, 11),
)
HALVES = (("dp_2", "dp_0"), ("dp_0", "dp_2"))
ORDER = (1, 3, 2)
FARTHEST = (4, 3, 5, 2, 6, 1, 7)
SCALE = (9.0 * CHANNELS) ** (-0.5)

head_scale = 4.0
soft_cap = 15.0
eps_norm = 1e-05
beta_one = 0.9
beta_two = 0.999
step_size = 0.1
eps_adam = 1e-08

F32 = jnp.float32
BF16 = jnp.bfloat16


def scoped(method):
    @functools.wraps(method)
    def inner(self, *given):
        tag = "_".join(str(v) for v in given if isinstance(v, int))
        with jax.named_scope(f"{type(self).__name__}_{method.__name__}_{tag}"):
            return method(self, *given)

    return inner


def seats():
    return (
        lax.axis_index("dp_0"),
        lax.axis_index("dp_1"),
        lax.axis_index("dp_2"),
        lax.axis_index("mp"),
    )


def greet_all(y, z, x, c):
    barrier = pltpu.get_barrier_semaphore()
    for step in range(1, 8):
        pl.semaphore_signal(
            barrier, inc=1, device_id={"dp_1": lax.rem(z + step, 8)}, device_id_type=MESH
        )
    for step in range(1, 4):
        for name, here in (("dp_0", y), ("dp_2", x)):
            pl.semaphore_signal(
                barrier, inc=1, device_id={name: lax.rem(here + step, 4)}, device_id_type=MESH
            )
    pl.semaphore_signal(barrier, inc=1, device_id={"mp": 1 - c}, device_id_type=MESH)
    return barrier


def remote(src, dst, send, recv, peer):
    return pltpu.make_async_remote_copy(
        src_ref=src, dst_ref=dst, send_sem=send, recv_sem=recv, device_id=peer, device_id_type=MESH
    )


def arrived(ref, recv, send, peer):
    remote(ref, ref, send, recv, peer).wait_recv()


def halves_of(chunk):
    return [(half, *HALVES[half]) for half in CHUNKS[chunk]]


class Gather:
    def __init__(self, seat, w, stage, wide, sems, started):
        self.y, self.z, self.x, self.c = seat
        self.here = {"dp_0": self.y, "dp_2": self.x}
        self.w, self.stage, self.wide, self.started = w, stage, wide, started
        self.z_send, self.z_recv, self.p_send, self.p_recv = sems[0:4]
        self.q_send, self.q_recv, self.m_send, self.m_recv = sems[4:8]
        self.partner = {"mp": 1 - self.c}

    def launch(self, copy):
        copy.start()
        self.started.append(copy)

    def tile(self, chunk, half, near, far):
        items = pl.ds(*CHUNKS[chunk][half])
        if half == 0:
            return self.w.at[self.c, items, far, near]
        return self.w.at[self.c, items, near, far]

    def slab(self, chunk, half, far, core):
        items = pl.ds(*CHUNKS[chunk][half])
        if half == 0:
            return self.w.at[core, items, far]
        return self.w.at[core, items, :, far]

    @scoped
    def along_z(self):
        z = self.z
        for group in (1, 0):
            ref = self.stage.at[group, z]
            for step in FARTHEST:
                peer = {"dp_1": lax.rem(z + step, 8)}
                self.launch(remote(ref, ref, self.z_send.at[group, step], self.z_recv.at[group, z], peer))

    @scoped
    def unpack(self, group):
        for step in range(1, 8):
            peer = lax.rem(self.z + step, 8)
            sems = self.z_recv.at[group, peer], self.z_send.at[group, 0]
            arrived(self.stage.at[group, peer], *sems, {"dp_1": peer})
        for piece in range(8):
            self.wide[group, 24 * piece : 24 * piece + 24, :] = self.stage[group, piece].astype(F32)

    def to_far(self, chunk, half, turn, near):
        far = HALVES[half][1]
        at = self.here[far]
        ref = self.tile(chunk, half, near, at)
        for step in ORDER:
            self.launch(
                remote(
                    ref, ref, self.q_send.at[chunk, half, turn, step], self.q_recv.at[chunk, half, at],
                    {far: lax.rem(at + step, 4)},
                )
            )

    @scoped
    def near_sends(self, chunk):
        for half, near, far in halves_of(chunk):
            start, count = CHUNKS[chunk][half]
            for item in range(start, start + count):
                group = int(item >= SPLIT)
                line = 2 * (item - SPLIT * group)
                slab = self.wide.at[group]
                low = slab[pl.ds(line, 8, stride=24), :]
                high = slab[pl.ds(line + 1, 8, stride=24), :]
                self.w[self.c, item, self.y, self.x] = jnp.concatenate([low, high], axis=0).astype(BF16)
        for step in ORDER:
            for half, near, far in halves_of(chunk):
                at = self.here[near]
                ref = self.tile(chunk, half, at, self.here[far])
                self.launch(
                    remote(
                        ref, ref, self.p_send.at[chunk, half, step], self.p_recv.at[chunk, half, at],
                        {near: lax.rem(at + step, 4)},
                    )
                )

    def own_sends(self, chunk):
        for half, near, far in halves_of(chunk):
            self.to_far(chunk, half, 0, self.here[near])

    def to_partner(self, chunk, half, turn, ref):
        sems = self.m_send.at[chunk, half, turn], self.m_recv.at[chunk, half, turn]
        self.launch(remote(ref, ref, *sems, self.partner))

    @scoped
    def far_sends(self, chunk):
        for step in ORDER:
            for half, near, far in halves_of(chunk):
                peer = lax.rem(self.here[near] + step, 4)
                ref = self.tile(chunk, half, peer, self.here[far])
                arrived(ref, self.p_recv.at[chunk, half, peer], self.p_send.at[chunk, half, 0], {near: peer})
                self.to_far(chunk, half, step, peer)
        for half, near, far in halves_of(chunk):
            self.to_partner(chunk, half, 0, self.slab(chunk, half, self.here[far], self.c))

    @scoped
    def cross(self, chunk):
        for step in ORDER:
            for half, near, far in halves_of(chunk):
                peer = lax.rem(self.here[far] + step, 4)
                ref = self.slab(chunk, half, peer, self.c)
                arrived(ref, self.q_recv.at[chunk, half, peer], self.q_send.at[chunk, half, 0, 0], {far: peer})
                self.to_partner(chunk, half, step, ref)

    @scoped
    def join(self, chunk):
        for half, near, far in halves_of(chunk):
            for turn in range(4):
                ref = self.slab(chunk, half, lax.rem(self.here[far] + turn, 4), 1 - self.c)
                sems = self.m_recv.at[chunk, half, turn], self.m_send.at[chunk, half, turn]
                arrived(ref, *sems, self.partner)


class Scatter:
    def __init__(self, seat, g, buffers, sems, started):
        self.y, self.z, self.x, self.c = seat
        self.here = {"dp_0": self.y, "dp_2": self.x}
        self.g, self.started = g, started
        self.inbox, self.sums, a_in, b_in, a_sum, b_sum, a_last, b_last, self.flat = buffers
        self.arrivals, self.folded, self.last = (a_in, b_in), (a_sum, b_sum), (a_last, b_last)
        self.m_send, self.m_recv, self.p_send, self.p_recv = sems[0:4]
        self.q_send, self.q_recv, self.z_send, self.z_recv = sems[4:8]
        self.partner = {"mp": 1 - self.c}

    def launch(self, copy):
        copy.start()
        self.started.append(copy)

    def across(self, piece):
        half, start, count, _ = PIECES[piece]
        items = pl.ds(start, count)
        return remote(
            self.g.at[1 - self.c, items], self.inbox.at[items], self.m_send.at[piece], self.m_recv.at[piece],
            self.partner,
        )

    def to_partner(self, piece):
        self.launch(self.across(piece))

    @scoped
    def near_sends(self, piece):
        half, start, count, at = PIECES[piece]
        near, far = HALVES[half]
        self.across(piece).wait_recv()
        for item in range(start, start + count):
            total = self.g[self.c, item].astype(F32) + self.inbox[item].astype(F32)
            self.sums[item] = total.astype(BF16)
        items = pl.ds(start, count)
        for step in ORDER:
            peer = lax.rem(self.here[near] + step, 4)
            ref = self.sums.at[items, :, peer] if half == 0 else self.sums.at[items, peer]
            self.launch(
                remote(
                    ref, self.arrivals[half].at[self.here[near], pl.ds(at, count)], self.p_send.at[piece, step],
                    self.p_recv.at[piece, self.here[near]], {near: peer},
                )
            )

    @scoped
    def far_sends(self, piece):
        half, start, count, at = PIECES[piece]
        near, far = HALVES[half]
        peers = [lax.rem(self.here[near] + step, 4) for step in ORDER]
        box, total_of = self.arrivals[half], self.folded[half]
        for peer in peers:
            ref = box.at[peer, pl.ds(at, count)]
            arrived(ref, self.p_recv.at[piece, peer], self.p_send.at[piece, 0], {near: peer})
        for item in range(count):
            own = self.sums[start + item, :, self.x] if half == 0 else self.sums[start + item, self.y]
            total = own.astype(F32)
            for peer in peers:
                total = total + box[peer, at + item].astype(F32)
            total_of[at + item] = total.astype(BF16)
        for step in ORDER:
            peer = lax.rem(self.here[far] + step, 4)
            self.launch(
                remote(
                    total_of.at[pl.ds(at, count), peer], self.last[half].at[self.here[far], pl.ds(at, count)],
                    self.q_send.at[piece, step], self.q_recv.at[piece, self.here[far]], {far: peer},
                )
            )

    @scoped
    def settle(self, piece):
        half, start, count, at = PIECES[piece]
        near, far = HALVES[half]
        peers = [lax.rem(self.here[far] + step, 4) for step in ORDER]
        box, total_of = self.last[half], self.folded[half]
        for peer in peers:
            ref = box.at[peer, pl.ds(at, count)]
            arrived(ref, self.q_recv.at[piece, peer], self.q_send.at[piece, 0], {far: peer})
        for item in range(count):
            total = total_of[at + item, self.here[far]].astype(F32)
            for peer in peers:
                total = total + box[peer, at + item].astype(F32)
            self.flat[16 * (start + item) : 16 * (start + item) + 16, :] = total

    @scoped
    def along_z(self, turn, item, letters, out):
        rows = letters.shape[1]
        for spot in range(8):
            letters[spot] = self.flat[pl.ds(16 * item + spot, rows, stride=8), :].astype(BF16)
        for step in FARTHEST:
            peer = lax.rem(self.z + step, 8)
            self.launch(
                remote(
                    letters.at[peer], out.at[self.z], self.z_send.at[turn, step], self.z_recv.at[turn, self.z],
                    {"dp_1": peer},
                )
            )
        out[self.z] = letters[self.z]

    @scoped
    def collect(self, turn, out):
        for step in range(1, 8):
            peer = lax.rem(self.z + step, 8)
            arrived(out.at[peer], self.z_recv.at[turn, peer], self.z_send.at[turn, 0], {"dp_1": peer})


NN = (((1,), (0,)), ((), ()))
NT = (((1,), (1,)), ((), ()))
TN = (((0,), (0,)), ((), ()))


def dot(a, b, dims=NN):
    return lax.dot_general(a, b, dims, preferred_element_type=F32)


def window_kernel(
    moves_in, values_in, rewards_in, hidden_in, first_in, second_in, head_in, embed_in, early, late,
    first_v, second_v, head_v, embed_v, hidden_v, rows, stage, wide, w, g,
    inbox, sums, a_in, b_in, a_sum, b_sum, a_last, b_last, flat, early_out, late_out,
    xs, hs, bs, zs, xt, bt, state, mixed, pre, summed, saved, first_t, second_t, moves, values, rewards, local_sem, *sems,
):
    seat = y, z, x, c = seats()
    barrier = greet_all(y, z, x, c)
    pairs = (
        (first_in, first_v), (second_in, second_v), (head_in, head_v), (embed_in, embed_v), (hidden_in, hidden_v),
        (moves_in, moves), (values_in, values), (rewards_in, rewards),
    )
    loads = [pltpu.make_async_copy(src, dst, local_sem.at[k]) for k, (src, dst) in enumerate(pairs)]
    for load in loads:
        load.start()
    started, sent = [], []
    gather = Gather(seat, w, stage, wide, sems[0:8], sent)
    scatter = Scatter(
        seat, g, (inbox, sums, a_in, b_in, a_sum, b_sum, a_last, b_last, flat), sems[8:16], started
    )
    rows[2 * MIX : 2 * MIX + 4, :] = jnp.zeros((4, 128), F32)
    for load in loads[0:4]:
        load.wait()
    for tap in range(9):
        at = 2 * (SECOND + tap)
        rows[at : at + 2, :] = second_v[tap // 3, tap % 3]
        at = 2 * (FIRST + tap)
        rows[at : at + 2, :] = first_v[tap // 3, tap % 3]
    for block in range(5):
        width = min(128, BUCKETS - 128 * block)
        at = 2 * (HEAD + block if block < 4 else MIX)
        rows[at : at + 2, 0:width] = head_v[0, :, 128 * block : 128 * block + width]
    for r in range(2):
        at = 2 * MIX + r
        rows[at : at + 1, 127:128] = embed_v[:, r : r + 1]
    stage[0, z] = rows[0:24, :].astype(BF16)
    stage[1, z] = rows[2 * SPLIT : 2 * SPLIT + 24, :].astype(BF16)
    with jax.named_scope("barrier"):
        pl.semaphore_wait(barrier, 14)
    gather.along_z()

    def phase(run):
        def inner(*given):
            with jax.named_scope(run.__name__):
                return run(*given)

        return inner

    row = lax.broadcasted_iota(jnp.int32, (ROWS, CHANNELS), 0)
    valid = (lax.rem(row, PITCH) < SIDE) & (row < PITCH * SIDE)

    def whole(h, item):
        return w[h, item].reshape(CHANNELS, 128)

    def first(tap):
        return jnp.concatenate([whole(0, FIRST + tap), whole(1, FIRST + tap)], axis=1)

    def second(tap):
        return jnp.concatenate([whole(0, SECOND + tap), whole(1, SECOND + tap)], axis=1)

    def head(h):
        last = whole(h, MIX)
        last = jnp.where(lax.broadcasted_iota(jnp.int32, last.shape, 1) < BUCKETS - 512, last, jnp.zeros_like(last))
        return jnp.concatenate([whole(h, HEAD + k) for k in range(4)] + [last], axis=1)

    def shifted(field, tap):
        start = GUARD + SHIFTS[tap]
        return jnp.concatenate([field[h, start : start + ROWS, :].astype(BF16) for h in range(2)], axis=1)

    def halves(lhs, rhs):
        cut = ROWS // 2
        return jnp.concatenate([dot(lhs[:cut], rhs), dot(lhs[cut:], rhs)], axis=0)

    @phase
    def transposes(dest, kernel, flip):
        for tap in range(9):
            turn = kernel(8 - tap if flip else tap).astype(F32).T
            dest[CHANNELS * tap : CHANNELS * tap + CHANNELS, :] = turn.astype(BF16)

    def taps_of(field):
        return jnp.concatenate([shifted(field, t) for t in range(9)], axis=1)

    @phase
    def conv_first(field):
        return halves(taps_of(field), jnp.concatenate([first(t) for t in range(9)], axis=0))

    @phase
    def conv_second(field):
        return halves(taps_of(field), second_t[...])

    @phase
    def back_second(field):
        return halves(taps_of(field), jnp.concatenate([second(8 - t) for t in range(9)], axis=0))

    @phase
    def back_first(field):
        return halves(taps_of(field), first_t[...])

    @phase
    def spread(value, dest):
        for h in range(2):
            dest[h, GUARD : GUARD + ROWS, :] = value[:, 128 * h : 128 * h + 128]

    @phase
    def turned(value):
        return value.T.astype(BF16)

    def total(value):
        return jnp.sum(jnp.sum(value, axis=0, keepdims=True), axis=1, keepdims=True)

    def store(h, item, value):
        g[h, item] = value.astype(BF16).reshape(4, 4, 16, 128)

    for field in (xs, hs, bs, zs):
        for k in range(2):
            for h in range(2):
                field[k, h, 0:GUARD, :] = jnp.zeros((GUARD, 128), F32)
                field[k, h, GUARD + ROWS :, :] = jnp.zeros((GUARD, 128), F32)
    flat[16 * FIRST : 16 * FIRST + 48, :] = jnp.zeros((48, 128), F32)

    state[...] = jnp.zeros((ROWS, CHANNELS), F32)
    for load in loads[4:8]:
        load.wait()

    with jax.named_scope("place"):
        for line in range(SIDE):
            cells = hidden_v[line].astype(F32)
            mine = jnp.where(c == 0, cells[:, 0, :], cells[:, 1, :])
            state[PITCH * line : PITCH * line + SIDE, :] = mine
    lane = lax.broadcasted_iota(jnp.int32, (CHANNELS, CHANNELS), 1)
    natural = 64 * (lane // 64) + 8 * (lane % 8) + 2 * ((lane // 16) % 4) + (lane // 8) % 2
    source = lax.broadcasted_iota(jnp.int32, (CHANNELS, CHANNELS), 0)
    permute = jnp.where(source == natural, 1.0, 0.0).astype(BF16)
    state[...] = dot(state[...].astype(BF16), permute)

    gather.unpack(1)
    for chunk in (3, 2):
        gather.near_sends(chunk)
        gather.own_sends(chunk)
    gather.unpack(0)
    for chunk in (1, 0):
        gather.near_sends(chunk)
    for chunk in (3, 2):
        gather.far_sends(chunk)
    for chunk in (1, 0):
        gather.own_sends(chunk)
        gather.far_sends(chunk)
    gather.cross(3)
    gather.cross(2)
    gather.join(3)

    ones = jnp.ones((16, 128), BF16)
    pick = lax.broadcasted_iota(jnp.int32, (16, 128), 1) == 127
    pick = jnp.where(pick, ones, jnp.zeros_like(ones))
    embed = [dot(pick, whole(e, MIX), NT)[0:1, :] for e in range(2)]

    kept = []
    pooled_rows = jnp.zeros((16, CHANNELS), F32)
    for k in range(2):
        move = moves[c, k]
        spot = PITCH * lax.div(move, SIDE) + lax.rem(move, SIDE)
        passed = move == CELLS
        added = jnp.where(row == spot, embed[0], 0.0) + jnp.where(passed, 1.0, 0.0) * embed[1]
        now = jnp.where(valid, state[...] + added, 0.0)
        mixed[...] = now
        if k == 1:
            gather.cross(0)
        spread(now, xs.at[k])
        if k == 0:
            gather.join(2)
        value = SCALE * conv_first(xs.at[k])
        pre[k] = value
        spread(jnp.where(valid, value * jax.nn.sigmoid(value), 0.0), hs.at[k])
        if k == 0:
            gather.cross(1)
            xt[:, 0:ROWS] = turned(mixed[...])
            transposes(first_t, first, True)
            gather.join(1)
            transposes(second_t, second, False)
        branch = conv_second(hs.at[k])
        value = jnp.where(valid, mixed[...] + SCALE * branch, 0.0)
        summed[k] = value
        factor = lax.rsqrt(total(value * value) / (CELLS * CHANNELS) + eps_norm)
        value = value * factor
        state[...] = value
        pooled = jnp.sum(value, axis=0, keepdims=True) / CELLS
        own_row = lax.broadcasted_iota(jnp.int32, (16, CHANNELS), 0) == k
        pooled_rows = jnp.where(own_row, pooled, pooled_rows)
        kept.append((spot, passed, factor))
    gather.join(0)

    bucket = lax.broadcasted_iota(jnp.int32, (16, 640), 1)
    top_row = lax.broadcasted_iota(jnp.int32, (16, 640), 0) == 0
    pooled = pooled_rows.astype(BF16)
    pooled_grads = jnp.zeros((16, CHANNELS), F32)
    logits = []
    for h, targets in enumerate((values, rewards)):
        raw = head_scale * dot(pooled, head(h))
        squashed = jnp.tanh(raw / soft_cap)
        raised = jnp.where(bucket < BUCKETS, jnp.exp(soft_cap * squashed), 0.0)
        chances = raised / jnp.sum(raised, axis=1, keepdims=True)
        picked = jnp.where(bucket == jnp.where(top_row, targets[c, 0], targets[c, 1]), 1.0, 0.0)
        logit = (chances - picked) * (1.0 - squashed * squashed) / 256.0
        logit = jnp.where(bucket < BUCKETS, logit, 0.0).astype(BF16)
        pooled_grads = pooled_grads + dot(logit, head(h), NT)
        logits.append(logit)
    mixed_grads = []
    for h in range(2):
        grad = head_scale * dot(pooled, logits[h], TN)
        for block in range(4):
            store(h, HEAD + block, grad[:, 128 * block : 128 * block + 128])
        mixed_grads.append(grad[:, 512:640])
    for piece in (0, 1):
        scatter.to_partner(piece)

    def window(field, tap):
        return jnp.concatenate([shifted(field.at[k], tap) for k in range(2)], axis=0)

    def second_taps(*taps):
        with jax.named_scope("second_taps"):
            for tap in taps:
                grad = SCALE * dot(bt[...], window(hs, tap))
                store(0, SECOND + tap, grad[:, 0:128])
                store(1, SECOND + tap, grad[:, 128:256])

    def first_taps(*taps):
        with jax.named_scope("first_taps"):
            for tap in taps:
                grad = SCALE * dot(xt[...], window(zs, 8 - tap))
                store(0, FIRST + tap, grad[:, 0:128])
                store(1, FIRST + tap, grad[:, 128:256])

    embed_grad = [jnp.zeros((1, CHANNELS), F32) for _ in range(2)]
    for k in (1, 0):
        spot, passed, factor = kept[k]
        grad = head_scale * pooled_grads[k : k + 1, :] / CELLS
        if k == 0:
            grad = saved[...] + grad
        grad = jnp.where(valid, grad, 0.0)
        value = summed[k]
        slope = total(grad * value) / (CELLS * CHANNELS)
        summed_grad = factor * grad - factor * factor * factor * value * slope
        saved[...] = summed_grad
        spread(summed_grad, bs.at[k])
        bt[:, ROWS * k : ROWS * k + ROWS] = turned(summed_grad)
        if k == 0:
            second_taps(0)
            scatter.to_partner(2)
            second_taps(1, 2)
            scatter.to_partner(3)
            second_taps(3, 4)
            scatter.to_partner(4)
            xt[:, ROWS : 2 * ROWS] = turned(mixed[...])
            scatter.near_sends(2)
            second_taps(5, 6)
            scatter.to_partner(5)
            scatter.near_sends(3)
            second_taps(7, 8)
            scatter.to_partner(6)
            scatter.near_sends(4)
        hidden_grad = SCALE * back_second(bs.at[k])
        if k == 0:
            scatter.near_sends(5)
        value = pre[k]
        sig = jax.nn.sigmoid(value)
        inner = hidden_grad * (sig * (1.0 + value * (1.0 - sig)))
        spread(jnp.where(valid, inner, 0.0), zs.at[k])
        if k == 0:
            scatter.near_sends(6)
            first_taps(0, 1)
            scatter.to_partner(7)
            first_taps(2, 3)
            scatter.to_partner(8)
            for piece in (0, 1):
                scatter.far_sends(piece)
        carry = saved[...] + SCALE * back_first(zs.at[k])
        if k == 0:
            scatter.near_sends(7)
            scatter.near_sends(8)
        else:
            scatter.near_sends(0)
            scatter.near_sends(1)
        carry = jnp.where(valid, carry, 0.0)
        saved[...] = carry
        embed_grad[0] = embed_grad[0] + jnp.sum(jnp.where(row == spot, carry, 0.0), axis=0, keepdims=True)
        embed_grad[1] = embed_grad[1] + jnp.where(passed, 1.0, 0.0) * jnp.sum(carry, axis=0, keepdims=True)

    for e in range(2):
        lines = jnp.broadcast_to(embed_grad[e], (16, CHANNELS)).astype(BF16)
        corner = lax.broadcasted_iota(jnp.int32, (16, 128), 0) * 128 + lax.broadcasted_iota(jnp.int32, (16, 128), 1)
        corner = jnp.where(corner == 127, ones, jnp.zeros_like(ones))
        store(e, MIX, mixed_grads[e] + dot(lines, corner, TN))
    scatter.to_partner(12)
    first_taps(4, 5)
    scatter.to_partner(9)
    first_taps(6, 7)
    scatter.to_partner(10)
    first_taps(8)
    scatter.to_partner(11)
    for piece in (9, 12, 10, 11):
        scatter.near_sends(piece)
    for piece in (2, 3, 4, 5, 6, 7, 8):
        scatter.far_sends(piece)
    for copy in sent:
        copy.wait_send()
    for piece in (9, 12, 10):
        scatter.far_sends(piece)
    for piece in (0, 1):
        scatter.settle(piece)
    scatter.far_sends(11)
    for piece in (2, 3, 4, 5, 6):
        scatter.settle(piece)
    scatter.along_z(0, 0, early_out, early)
    for piece in (7, 8, 9, 12, 10, 11):
        scatter.settle(piece)
    scatter.along_z(1, SPLIT, late_out, late)
    scatter.collect(0, early)
    scatter.collect(1, late)
    with jax.named_scope("drain"):
        for copy in started:
            copy.wait_send()


def window_grads(moves, values, rewards, hidden_state, params):
    vmem = pl.BlockSpec(memory_space=pltpu.VMEM)
    hbm = pl.BlockSpec(memory_space=pltpu.HBM)
    dma = pltpu.SemaphoreType.DMA
    copies = pltpu.VMEM((2, 2, ROWS + 2 * GUARD, 128), F32)
    turned = pltpu.VMEM((CHANNELS, 2 * ROWS), BF16)
    field = pltpu.VMEM((ROWS, CHANNELS), F32)
    fields = pltpu.VMEM((2, ROWS, CHANNELS), F32)
    board = pltpu.VMEM((ITEMS, 4, 4, 16, 128), BF16)
    boards = pltpu.VMEM((2, ITEMS, 4, 4, 16, 128), BF16)
    early, late = (8, 32, 128), (8, 24, 128)
    return pl.pallas_call(
        window_kernel,
        out_shape=[jax.ShapeDtypeStruct(early, BF16), jax.ShapeDtypeStruct(late, BF16)],
        in_specs=[hbm] * 8,
        out_specs=[vmem, vmem],
        scratch_shapes=[pltpu.VMEM(p.shape, F32) for p in params]
        + [
            pltpu.VMEM(hidden_state.shape, BF16),
            pltpu.VMEM((48, 128), F32),
            pltpu.VMEM((2, 8, 24, 128), BF16),
            pltpu.VMEM((2, 192, 128), F32),
            boards,
            boards,
            board,
            board,
            pltpu.VMEM((4, 12, 4, 16, 128), BF16),
            pltpu.VMEM((4, 12, 4, 16, 128), BF16),
            pltpu.VMEM((12, 4, 16, 128), BF16),
            pltpu.VMEM((12, 4, 16, 128), BF16),
            pltpu.VMEM((4, 12, 16, 128), BF16),
            pltpu.VMEM((4, 12, 16, 128), BF16),
            pltpu.VMEM((384, 128), F32),
            pltpu.VMEM(early, BF16),
            pltpu.VMEM(late, BF16),
            copies,
            copies,
            copies,
            copies,
            turned,
            turned,
            field,
            field,
            fields,
            fields,
            field,
            pltpu.VMEM((9 * CHANNELS, CHANNELS), BF16),
            pltpu.VMEM((9 * CHANNELS, CHANNELS), BF16),
            pltpu.SMEM((2, 2), jnp.int32),
            pltpu.SMEM((2, 2), jnp.int32),
            pltpu.SMEM((2, 2), jnp.int32),
            dma((8,)),
        ]
        + [
            dma(shape)
            for shape in (
                (2, 8), (2, 8), (4, 2, 4), (4, 2, 4), (4, 2, 4, 4), (4, 2, 4), (4, 2, 4), (4, 2, 4),
                (13,), (13,), (13, 4), (13, 4), (13, 4), (13, 4), (2, 8), (2, 8),
            )
        ],
        compiler_params=pltpu.CompilerParams(
            collective_id=0, has_side_effects=True, vmem_limit_bytes=58 << 20
        ),
        name="window",
    )(moves, values, rewards, hidden_state, *params)


def adam(param, grad, mean, square):
    mean_new = beta_one * mean + (1.0 - beta_one) * grad
    square_new = beta_two * square + (1.0 - beta_two) * grad * grad
    param_new = param - step_size * mean_new / (jnp.sqrt(square_new) + eps_adam)
    return param_new, mean_new, square_new, grad


def adam_kernel(*refs):
    given, outs, held, sem = refs[0:14], refs[14:30], refs[30:44], refs[44]
    loads = [pltpu.make_async_copy(src, dst, sem.at[k]) for k, (src, dst) in enumerate(zip(given, held))]
    for load in loads:
        load.start()
    for load in loads:
        load.wait()
    early, late = held[0:2]
    params, means, squares = held[2:6], held[6:10], held[10:14]
    new, mean_new, square_new, grads = outs[0:4], outs[4:8], outs[8:12], outs[12:16]
    totals = []
    for parts in (early, late):
        total = parts[0].astype(F32)
        for piece in range(1, 8):
            total = total + parts[piece].astype(F32)
        totals.append(total)

    def owned(item):
        if item < FIRST:
            return totals[0][2 * item : 2 * item + 2]
        return totals[1][2 * (item - SPLIT) : 2 * (item - SPLIT) + 2]

    for which in range(2):
        for tap in range(9):
            a, b = tap // 3, tap % 3
            grad = owned((FIRST, SECOND)[which] + tap)
            results = adam(params[which][a, b], grad, means[which][a, b], squares[which][a, b])
            for ref, result in zip((new, mean_new, square_new, grads), results):
                ref[which][a, b] = result
    head = jnp.concatenate([owned(HEAD + k) for k in range(4)] + [owned(MIX)], axis=1)[:, 0:BUCKETS]
    results = adam(params[2][0], head, means[2][0], squares[2][0])
    for ref, result in zip((new, mean_new, square_new, grads), results):
        ref[2][0] = result
    embed = owned(MIX)
    embed = jnp.concatenate([embed[0:1, 127:128], embed[1:2, 127:128]], axis=1)
    results = adam(params[3][...], embed, means[3][...], squares[3][...])
    for ref, result in zip((new, mean_new, square_new, grads), results):
        ref[3][...] = result


def updates(early, late, params, means, squares):
    vmem = pl.BlockSpec(memory_space=pltpu.VMEM)
    shapes = [jax.ShapeDtypeStruct(p.shape, F32) for p in params]
    given = (early, late, *params, *means, *squares)
    return pl.pallas_call(
        adam_kernel,
        out_shape=shapes * 4,
        in_specs=[pl.BlockSpec(memory_space=pltpu.HBM)] * 14,
        out_specs=[vmem] * 16,
        scratch_shapes=[pltpu.VMEM(a.shape, a.dtype) for a in given] + [pltpu.SemaphoreType.DMA((14,))],
        compiler_params=pltpu.CompilerParams(vmem_limit_bytes=58 << 20),
        name="adam",
    )(*given)


def local(
    hidden_state,
    actions,
    value_target,
    reward_target,
    kernel_first,
    kernel_second,
    head_weight,
    action_embed,
    first_mean,
    first_square,
    second_mean,
    second_square,
    head_mean,
    head_square,
    embed_mean,
    embed_square,
):
    params = (kernel_first, kernel_second, head_weight, action_embed)
    boards = jnp.transpose(hidden_state, (1, 2, 0, 3))
    early, late = window_grads(actions, value_target, reward_target, boards, params)
    outs = updates(
        early,
        late,
        params,
        (first_mean, second_mean, head_mean, embed_mean),
        (first_square, second_square, head_square, embed_square),
    )
    new, means, squares, sums = outs[0:4], outs[4:8], outs[8:12], outs[12:16]
    moments = [moment for pair in zip(means, squares) for moment in pair]
    return (*new, *moments, *sums)


def solution(mesh):
    torus = Mesh(mesh.devices.reshape(4, 8, 4, mesh.shape["mp"]), ("dp_0", "dp_1", "dp_2", "mp"))
    kernel = P(None, None, DP, "mp")
    head = P("mp", DP, None)
    embed = P("mp", DP)
    rows = P(DP, None)
    placed = (P(DP, None, None, None), rows, rows, rows, kernel, kernel, head, embed)
    moments = (kernel, kernel, kernel, kernel, head, head, embed, embed)
    return jax.shard_map(
        local,
        mesh=torus,
        in_specs=placed + moments,
        out_specs=(kernel, kernel, head, embed) + moments + (kernel, kernel, head, embed),
        check_vma=False,
    )
```
